32 devices in a mesh: data: 1 (over z), col: 4 (over y), row: 8 (over x, core).
Axes of the slice: x: 4, y: 4, z: 1, core: 2. Of those that a mesh axis runs over, the one named last changes fastest.
The devices are a block of a 4x4x8 slice.
Arguments:
- x_seq: bfloat16 [24, 32, 4096], P(None, 'data', 'row')
- h_init: float32 [2, 32, 4096], P(None, 'data', 'row')
- wx_l1: bfloat16 [4096, 3, 4096], P('row', None, 'col')
- whru_l1: bfloat16 [4096, 2, 4096], P('row', None, 'col')
- whn_l1: bfloat16 [4096, 4096], P('row', 'col')
- bias_l1: float32 [3, 4096], P(None, 'col')
- wx_l2: bfloat16 [4096, 3, 4096], P('row', None, 'col')
- whru_l2: bfloat16 [4096, 2, 4096], P('row', None, 'col')
- whn_l2: bfloat16 [4096, 4096], P('row', 'col')
- bias_l2: float32 [3, 4096], P(None, 'col')
Outputs:
- output 1: bfloat16 [24, 32, 4096], P(None, 'data', ('col', 'row'))
- output 2: float32 [2, 32, 4096], P(None, 'data', ('col', 'row'))
All inputs are finite; a program needn't handle non-finite values.
Results may differ from the reference program's by a relative error of at most 0.0024724.
Values are sent between devices in bfloat16 or wider.
A program may use at most 768 MiB of HBM per device.

```python
import jax
import jax.numpy as jnp
from jax import lax

SEQ_LEN = 24
BATCH_GROUP = 32
HIDDEN = 4096


def setup_inputs(seed: int = 0, part: int = 0) -> dict:
    part_key = jax.random.fold_in(jax.random.key(seed), part)
    seq_key, state_key = jax.random.split(part_key, 2)
    weight_keys = jax.random.split(jax.random.key(seed + 1), 8)
    w_scale = HIDDEN ** -0.5
    gate_shift = jnp.array([0.0, 1.5, 0.0], jnp.float32)[:, None]

    def draw_weight(key, shape):
        return (w_scale * jax.random.normal(key, shape, jnp.float32)).astype(jnp.bfloat16)

    def draw_bias(key):
        return 0.5 * jax.random.normal(key, (3, HIDDEN), jnp.float32) + gate_shift

    x_seq = jax.random.normal(seq_key, (SEQ_LEN, BATCH_GROUP, HIDDEN), jnp.float32).astype(jnp.bfloat16)
    h_init = 0.8 * jnp.tanh(jax.random.normal(state_key, (2, BATCH_GROUP, HIDDEN), jnp.float32))
    return {
        "x_seq": x_seq,
        "h_init": h_init,
        "wx_l1": draw_weight(weight_keys[0], (HIDDEN, 3, HIDDEN)),
        "whru_l1": draw_weight(weight_keys[1], (HIDDEN, 2, HIDDEN)),
        "whn_l1": draw_weight(weight_keys[2], (HIDDEN, HIDDEN)),
        "bias_l1": draw_bias(weight_keys[3]),
        "wx_l2": draw_weight(weight_keys[4], (HIDDEN, 3, HIDDEN)),
        "whru_l2": draw_weight(weight_keys[5], (HIDDEN, 2, HIDDEN)),
        "whn_l2": draw_weight(weight_keys[6], (HIDDEN, HIDDEN)),
        "bias_l2": draw_bias(weight_keys[7]),
    }


def gru_layer(in_seq, w_x, w_hru, w_hn, gate_bias, h_start):
    batch_rows = in_seq.shape[1]
    wx_flat = w_x.reshape(HIDDEN, 3 * HIDDEN)
    whru_flat = w_hru.reshape(HIDDEN, 2 * HIDDEN)

    def gru_step(h_prev, step_in):
        in_proj = jnp.dot(step_in, wx_flat, preferred_element_type=jnp.float32).reshape(batch_rows, 3, HIDDEN) + gate_bias
        rec_ru = jnp.dot(h_prev.astype(jnp.bfloat16), whru_flat, preferred_element_type=jnp.float32).reshape(batch_rows, 2, HIDDEN)
        reset_gate = jax.nn.sigmoid(in_proj[:, 0] + rec_ru[:, 0])
        update_gate = jax.nn.sigmoid(in_proj[:, 1] + rec_ru[:, 1])
        gated_h = (reset_gate * h_prev).astype(jnp.bfloat16)
        candidate = jnp.tanh(in_proj[:, 2] + jnp.dot(gated_h, w_hn, preferred_element_type=jnp.float32))
        h_next = (1.0 - update_gate) * candidate + update_gate * h_prev
        return h_next, h_next.astype(jnp.bfloat16)

    return lax.scan(gru_step, h_start, in_seq)


def reference(x_seq, h_init, wx_l1, whru_l1, whn_l1, bias_l1, wx_l2, whru_l2, whn_l2, bias_l2):
    h1_last, h1_seq = gru_layer(x_seq, wx_l1, whru_l1, whn_l1, bias_l1, h_init[0])
    h2_last, h2_seq = gru_layer(h1_seq, wx_l2, whru_l2, whn_l2, bias_l2, h_init[1])
    return h2_seq, jnp.stack([h1_last, h2_last])
```

```python
import functools

import jax
import jax.numpy as jnp
from jax import lax
from jax.experimental import pallas as pl
from jax.experimental.pallas import tpu as pltpu
from jax.sharding import PartitionSpec as P

MESH = pl.DeviceIdType.MESH
F32 = jnp.float32
BF16 = jnp.bfloat16
HALVES = 2
CORES = 2
RESET, UPDATE, CAND, REC_RESET, REC_UPDATE, REC_CAND = range(6)
GATES = 6


def ring_distance(offset, count):
    return min(offset, count - offset)


def gru_kernel(
    rows, cols,
    x_ref, h_ref, wx1, wru1, wn1, b1, wx2, wru2, wn2, b2,
    seq_out, last_out,
    weights, relay, xs, x_relay, state_in,
    h1_blocks, r1_blocks, h2_blocks, r2_blocks,
    states, updates, projections, seq_halves, last_halves,
    weight_sem, relay_sem, xs_sem, x_relay_sem, state_sem,
    weight_sent, relay_sent, x_sent, x_relay_sent, state_sent,
    block_sem, block_sent, out_sem, out_sent,
):
    chips = rows // CORES
    steps, batch, half = seq_out.shape
    chunk = HALVES * half
    places = chips * cols
    row, col = lax.axis_index("row"), lax.axis_index("col")
    xpos, core = row // CORES, row % CORES
    layers = ((wx1, wru1, wn1), (wx2, wru2, wn2))

    def device(x, c, y):
        return {"row": CORES * x + c, "col": y}

    def wrap_x(v):
        return lax.rem(v + 2 * chips, chips)

    def wrap_y(v):
        return lax.rem(v + 2 * cols, cols)

    def place_of(x_from, y_from, x_to, y_to):
        return chips * wrap_y(y_from - y_to) + wrap_x(x_from - x_to)

    barrier = pltpu.get_barrier_semaphore()
    for k in range(1, rows * cols):
        other = {"row": lax.rem(row + k % rows, rows), "col": lax.rem(col + k // rows, cols)}
        pl.semaphore_signal(barrier, inc=1, device_id=other, device_id_type=MESH)
    pl.semaphore_wait(barrier, rows * cols - 1)

    def remote(src, dst, send, recv, to):
        return pltpu.make_async_remote_copy(
            src_ref=src, dst_ref=dst, send_sem=send, recv_sem=recv, device_id=to, device_id_type=MESH
        )

    def own_unit(j):
        return HALVES * core + j, xpos

    def weight_pieces(layer, j, x_to, dst):
        wx, wru, wn = layers[layer]
        depth = pl.ds(j * chunk, chunk)
        for s in range(HALVES):
            units = pl.ds(pl.multiple_of(x_to * chunk + s * half, half), half)
            yield wx.at[:, depth, units], dst.at[pl.ds(0, 3), s]
            yield wru.at[:, depth, units], dst.at[pl.ds(3, 2), s]
            yield wn.at[depth, units], dst.at[5, s]

    def x_pieces(j, dst):
        for s in range(HALVES):
            yield x_ref.at[:, :, pl.ds(j * chunk + s * half, half)], dst.at[:, s]

    def send_weights(layer):
        for j, turn in ((0, 1), (1, -1)):
            via, far = wrap_x(xpos + turn), wrap_x(xpos + 2)
            for src, dst in weight_pieces(layer, j, far, relay.at[layer, j, core]):
                remote(src, dst, weight_sent.at[layer, 2, j], relay_sem.at[layer, j, core], device(via, 0, col)).start()
        for turn in (1, chips - 1, 0):
            x_to = wrap_x(xpos + turn)
            for j in range(2):
                place = place_of(*own_unit(j), x_to, col)
                dst_chunk = weights.at[layer, place]

                def remote_pieces():
                    for src, dst in weight_pieces(layer, j, x_to, dst_chunk):
                        remote(src, dst, weight_sent.at[layer, turn, j], weight_sem.at[layer, place], device(x_to, 1, col)).start()

                if turn:
                    remote_pieces()
                else:
                    pl.when(core == 0)(remote_pieces)

                    @pl.when(core == 1)
                    def _():
                        for src, dst in weight_pieces(layer, j, x_to, dst_chunk):
                            pltpu.make_async_copy(src, dst, weight_sem.at[layer, place]).start()

    def send_x():
        for j, turn in ((0, 1), (1, -1)):
            via = wrap_x(xpos + turn)
            for src, dst in x_pieces(j, x_relay.at[j, core]):
                remote(src, dst, x_sent.at[2, j], x_relay_sem.at[j, core], device(via, 0, col)).start()
        for turn in (1, chips - 1, 0):
            x_to = wrap_x(xpos + turn)
            for j in range(2):
                place = place_of(*own_unit(j), x_to, col)

                def remote_pieces():
                    for src, dst in x_pieces(j, xs.at[place]):
                        remote(src, dst, x_sent.at[turn, j], xs_sem.at[place], device(x_to, 1, col)).start()

                if turn:
                    remote_pieces()
                else:
                    pl.when(core == 0)(remote_pieces)

                    @pl.when(core == 1)
                    def _():
                        for src, dst in x_pieces(j, xs.at[place]):
                            pltpu.make_async_copy(src, dst, xs_sem.at[place]).start()

    def pass_on(layer):
        for j, turn in ((0, 1), (1, -1)):
            for c in range(CORES):
                src = relay.at[layer, j, c]
                pltpu.make_async_copy(src, src, relay_sem.at[layer, j, c]).wait()
                x_to = wrap_x(xpos + turn)
                place = place_of(HALVES * c + j, wrap_x(xpos - turn), x_to, col)
                remote(src, weights.at[layer, place], relay_sent.at[layer, j, c], weight_sem.at[layer, place], device(x_to, 1, col)).start()

    def pass_on_x():
        for j, turn in ((0, 1), (1, -1)):
            for c in range(CORES):
                src = x_relay.at[j, c]
                pltpu.make_async_copy(src, src, x_relay_sem.at[j, c]).wait()
                x_to = wrap_x(xpos + turn)
                place = place_of(HALVES * c + j, wrap_x(xpos - turn), x_to, col)
                remote(src, xs.at[place], x_relay_sent.at[j, c], xs_sem.at[place], device(x_to, 1, col)).start()

    @pl.when(xpos == col)
    def _():
        for j in range(2):
            x_to = HALVES * core + j
            for s in range(HALVES):
                src = h_ref.at[:, :, pl.ds(j * chunk + s * half, half)]
                dst = state_in.at[:, s]
                mine = (x_to == xpos) & (core == 1)

                @pl.when(mine)
                def _():
                    pltpu.make_async_copy(src, dst, state_sem.at[s]).start()

                @pl.when(jnp.logical_not(mine))
                def _():
                    copy = remote(src, dst, state_sent.at[j, s], state_sem.at[s], device(x_to, 1, col))
                    copy.start()
                    copy.wait_send()

    send_weights(0)
    send_x()

    @pl.when(core == 0)
    def _():
        pass_on(0)
        pass_on_x()

    send_weights(1)

    @pl.when(core == 0)
    def _():
        pass_on(1)

    def drain_sends():
        piece = weights.at[0, 0]
        for layer in range(2):
            for j in range(2):
                for turn in (1, 2, chips - 1):
                    pltpu.make_async_copy(piece, piece, weight_sent.at[layer, turn, j]).wait()

                @pl.when(core == 0)
                def _():
                    pltpu.make_async_copy(piece, piece, weight_sent.at[layer, 0, j]).wait()
                    for c in range(CORES):
                        pltpu.make_async_copy(piece, piece, relay_sent.at[layer, j, c]).wait()

        part = xs.at[0]
        for j in range(2):
            for turn in (1, 2, chips - 1):
                pltpu.make_async_copy(part, part, x_sent.at[turn, j]).wait()

            @pl.when(core == 0)
            def _():
                pltpu.make_async_copy(part, part, x_sent.at[0, j]).wait()
                for c in range(CORES):
                    pltpu.make_async_copy(part, part, x_relay_sent.at[j, c]).wait()

    offsets = [(dx, dy) for dy in range(cols) for dx in range(chips)]
    distance = [ring_distance(dx, chips) + ring_distance(dy, cols) for dx, dy in offsets]
    far_first = sorted(range(1, places), key=lambda p: -distance[p])
    groups = [
        [p for p in range(places) if distance[p] <= 1],
        [p for p in range(places) if distance[p] == 2],
        [p for p in range(places) if distance[p] > 2],
    ]

    def spread(blocks, kind):
        for p in far_first:
            dx, dy = offsets[p]
            there = chips * ((cols - dy) % cols) + (chips - dx) % chips
            to = device(wrap_x(xpos + dx), 1, wrap_y(col + dy))
            remote(blocks.at[0], blocks.at[there], block_sent.at[kind], block_sem.at[kind, there], to).start()

    def arrived(blocks, kind, group):
        for p in group:
            if p:
                pltpu.make_async_copy(blocks.at[p], blocks.at[p], block_sem.at[kind, p]).wait()

    def all_sent(blocks, kind):
        sent = blocks.at[pl.ds(1, places - 1)]
        pltpu.make_async_copy(sent, sent, block_sent.at[kind]).wait()

    def wide(parts):
        return jnp.concatenate(parts, axis=1)

    def product(lhs_of, layer, gates, total=None, group=None):
        for p in range(places) if group is None else group:
            rhs = wide([weights[layer, p, g, s] for g in gates for s in range(HALVES)])
            lhs = wide([lhs_of(p, s) for s in range(HALVES)])
            term = jnp.dot(lhs, rhs, preferred_element_type=F32)
            total = term if total is None else total + term
        return total

    def gathered(blocks, kind, layer, gates):
        total = None
        for group in groups:
            arrived(blocks, kind, group)
            total = product(lambda p, s: blocks[p, s], layer, gates, total, group)
        return total

    def project(layer, lhs_of, bias):
        total = product(lhs_of, layer, (RESET, UPDATE, CAND))
        for g in range(3):
            for s in range(HALVES):
                n = g * HALVES + s
                here = bias[pl.ds(g, 1), pl.ds(pl.multiple_of(xpos * chunk + s * half, half), half)]
                projections[layer, g, s] = total[:, n * half : (n + 1) * half] + here

    def reset_half(layer, blocks, kind, out_blocks):
        total = gathered(blocks, kind, layer, (REC_RESET, REC_UPDATE))
        for s in range(HALVES):
            reset = jax.nn.sigmoid(projections[layer, RESET, s] + total[:, s * half : (s + 1) * half])
            out_blocks[0, s] = (reset * states[layer, s]).astype(BF16)
        for s in range(HALVES):
            n = HALVES + s
            updates[layer, s] = jax.nn.sigmoid(projections[layer, UPDATE, s] + total[:, n * half : (n + 1) * half])

    def next_half(layer, blocks, kind, emit):
        total = gathered(blocks, kind, layer, (REC_CAND,))
        for s in range(HALVES):
            candidate = jnp.tanh(projections[layer, CAND, s] + total[:, s * half : (s + 1) * half])
            update = updates[layer, s]
            state = (1.0 - update) * candidate + update * states[layer, s]
            states[layer, s] = state
            emit(s, state.astype(BF16))

    H1, R1, H2, R2 = range(4)

    def first_reset(t):
        slot = h1_blocks.at[lax.rem(t, 2)]
        reset_half(0, slot, H1, r1_blocks)
        all_sent(slot, H1)
        spread(r1_blocks, R1)

    def first_next(t):
        slot = h1_blocks.at[lax.rem(t + 1, 2)]

        def emit(s, value):
            slot[0, s] = value

        next_half(0, r1_blocks, R1, emit)
        all_sent(r1_blocks, R1)
        spread(slot, H1)

    def first_inputs(t):
        project(0, lambda p, s: xs[p, t, s], b1)

    def second_inputs(t):
        slot = h1_blocks.at[lax.rem(t, 2)]
        project(1, lambda p, s: slot[p, s], b2)

    def second_reset():
        reset_half(1, h2_blocks, H2, r2_blocks)
        all_sent(h2_blocks, H2)
        spread(r2_blocks, R2)

    def second_next(t, last):
        def emit(s, value):
            seq_halves[s, t] = value
            if not last:
                h2_blocks[0, s] = value

        next_half(1, r2_blocks, R2, emit)
        all_sent(r2_blocks, R2)
        if not last:
            spread(h2_blocks, H2)

    @pl.when(core == 1)
    def _():
        for s in range(HALVES):
            part = state_in.at[:, s]
            pltpu.make_async_copy(part, part, state_sem.at[s]).wait()
        for layer in range(2):
            for s in range(HALVES):
                states[layer, s] = state_in[layer, s]
        for s in range(HALVES):
            h1_blocks[0, 0, s] = state_in[0, s].astype(BF16)
            h2_blocks[0, s] = state_in[1, s].astype(BF16)
        spread(h1_blocks.at[0], H1)
        spread(h2_blocks, H2)
        for p in range(places):
            pltpu.make_async_copy(xs.at[p], xs.at[p], xs_sem.at[p]).wait()
            pltpu.make_async_copy(weights.at[0, p], weights.at[0, p], weight_sem.at[0, p]).wait()
        first_inputs(0)
        first_reset(0)
        first_next(0)
        first_inputs(jnp.minimum(1, steps - 1))
        for p in range(places):
            pltpu.make_async_copy(weights.at[1, p], weights.at[1, p], weight_sem.at[1, p]).wait()

        def step(t, carry):
            first_reset(t)
            second_inputs(t)
            second_reset()
            first_next(t)
            second_next(t - 1, False)
            first_inputs(jnp.minimum(t + 1, steps - 1))
            return carry

        lax.fori_loop(1, steps, step, 0)
        last_slot = h1_blocks.at[steps % 2]
        arrived(last_slot, H1, range(places))
        all_sent(last_slot, H1)
        second_inputs(steps)
        second_reset()
        second_next(steps - 1, True)
        for layer in range(2):
            for s in range(HALVES):
                last_halves[s, layer] = states[layer, s]
        seq_copy = remote(seq_halves.at[0], seq_out, out_sent.at[0], out_sem.at[0], device(xpos, 0, col))
        last_copy = remote(last_halves.at[0], last_out, out_sent.at[1], out_sem.at[1], device(xpos, 0, col))
        seq_copy.start()
        last_copy.start()
        seq_out[...] = seq_halves[1]
        last_out[...] = last_halves[1]
        seq_copy.wait_send()
        last_copy.wait_send()

    @pl.when(core == 0)
    def _():
        pltpu.make_async_copy(seq_out, seq_out, out_sem.at[0]).wait()
        pltpu.make_async_copy(last_out, last_out, out_sem.at[1]).wait()

    drain_sends()


def solution(mesh):
    rows, cols = mesh.shape["row"], mesh.shape["col"]
    chips = rows // CORES
    places = chips * cols

    def device_body(x_rows, h_rows, wx_l1, whru_l1, whn_l1, bias_l1, wx_l2, whru_l2, whn_l2, bias_l2):
        steps, batch, row_block = x_rows.shape
        col_block = wx_l1.shape[2]
        half = col_block // rows
        chunk = HALVES * half
        anywhere = pl.BlockSpec(memory_space=pl.ANY)
        vmem = pl.BlockSpec(memory_space=pltpu.VMEM)
        dma = pltpu.SemaphoreType.DMA
        kinds = 4
        block = (HALVES, batch, half)
        scratch = [
            pltpu.VMEM((2, places, GATES, HALVES, chunk, half), BF16),
            pltpu.VMEM((2, 2, CORES, GATES, HALVES, chunk, half), BF16),
            pltpu.VMEM((places, steps, *block), BF16),
            pltpu.VMEM((2, CORES, steps, *block), BF16),
            pltpu.VMEM((2, *block), F32),
            pltpu.VMEM((2, places, *block), BF16),
            pltpu.VMEM((places, *block), BF16),
            pltpu.VMEM((places, *block), BF16),
            pltpu.VMEM((places, *block), BF16),
            pltpu.VMEM((2, *block), F32),
            pltpu.VMEM((2, *block), F32),
            pltpu.VMEM((2, 3, *block), F32),
            pltpu.VMEM((HALVES, steps, batch, half), BF16),
            pltpu.VMEM((HALVES, 2, batch, half), F32),
            dma((2, places)),
            dma((2, 2, CORES)),
            dma((places,)),
            dma((2, CORES)),
            dma((HALVES,)),
            dma((2, chips, 2)),
            dma((2, 2, CORES)),
            dma((chips, 2)),
            dma((2, CORES)),
            dma((2, HALVES)),
            dma((kinds, places)),
            dma((kinds,)),
            dma((2,)),
            dma((2,)),
        ]
        return pl.pallas_call(
            functools.partial(gru_kernel, rows, cols),
            name="gru",
            out_shape=(
                jax.ShapeDtypeStruct((steps, batch, half), BF16),
                jax.ShapeDtypeStruct((2, batch, half), F32),
            ),
            in_specs=[anywhere, anywhere, anywhere, anywhere, anywhere, vmem, anywhere, anywhere, anywhere, vmem],
            out_specs=(vmem, vmem),
            scratch_shapes=scratch,
            compiler_params=pltpu.CompilerParams(
                collective_id=0, has_side_effects=True, vmem_limit_bytes=60 * 1024 * 1024
            ),
        )(
            x_rows, h_rows,
            jnp.transpose(wx_l1, (1, 0, 2)), jnp.transpose(whru_l1, (1, 0, 2)), whn_l1, bias_l1,
            jnp.transpose(wx_l2, (1, 0, 2)), jnp.transpose(whru_l2, (1, 0, 2)), whn_l2, bias_l2,
        )

    seq_spec = P(None, "data", "row")
    out_spec = P(None, "data", ("col", "row"))
    wide_spec = P("row", None, "col")
    square_spec = P("row", "col")
    bias_spec = P(None, "col")
    return jax.shard_map(
        device_body,
        mesh=mesh,
        in_specs=(seq_spec, seq_spec, wide_spec, wide_spec, square_spec, bias_spec, wide_spec, wide_spec, square_spec, bias_spec),
        out_specs=(out_spec, out_spec),
        check_vma=False,
    )
```

```python
import functools

import jax
import jax.numpy as jnp
from jax import lax
from jax.experimental import pallas as pl
from jax.experimental.pallas import tpu as pltpu
from jax.sharding import PartitionSpec as P

MESH = pl.DeviceIdType.MESH
F32 = jnp.float32
BF16 = jnp.bfloat16
HALVES = 2
CORES = 2
RESET, UPDATE, CAND, REC_RESET, REC_UPDATE, REC_CAND = range(6)
GATES = 6


def ring_distance(offset, count):
    return min(offset, count - offset)


def gru_kernel(
    rows, cols,
    x_ref, h_ref, wx1, wru1, wn1, b1, wx2, wru2, wn2, b2,
    seq_out, last_out,
    weights, xs, state_in,
    h1_blocks, r1_blocks, h2_blocks, r2_blocks,
    states, updates, projections, seq_halves, last_halves,
    weight_sem, hand_sem, x_sem, xs_sem, state_sem,
    weight_sent, handed_sent, x_sent, x_passed, state_sent,
    block_sem, block_sent, out_sem, out_sent,
):
    chips = rows // CORES
    steps, batch, half = seq_out.shape
    chunk = HALVES * half
    places = chips * cols
    row, col = lax.axis_index("row"), lax.axis_index("col")
    xpos, core = row // CORES, row % CORES
    layers = ((wx1, wru1, wn1), (wx2, wru2, wn2))

    def device(x, c, y):
        return {"row": CORES * x + c, "col": y}

    def wrap_x(v):
        return lax.rem(v + 2 * chips, chips)

    def wrap_y(v):
        return lax.rem(v + 2 * cols, cols)

    def place_of(x_from, y_from, x_to, y_to):
        return chips * wrap_y(y_from - y_to) + wrap_x(x_from - x_to)

    barrier = pltpu.get_barrier_semaphore()
    for k in range(1, rows * cols):
        other = {"row": lax.rem(row + k % rows, rows), "col": lax.rem(col + k // rows, cols)}
        pl.semaphore_signal(barrier, inc=1, device_id=other, device_id_type=MESH)
    pl.semaphore_wait(barrier, rows * cols - 1)

    def remote(src, dst, send, recv, to):
        return pltpu.make_async_remote_copy(
            src_ref=src, dst_ref=dst, send_sem=send, recv_sem=recv, device_id=to, device_id_type=MESH
        )

    def chunk_place(c, j, x_from, x_to, y_to):
        return place_of(HALVES * c + j, x_from, x_to, y_to)

    def weight_pieces(layer, j, x_to, dst):
        wx, wru, wn = layers[layer]
        depth = pl.ds(j * chunk, chunk)
        for s in range(HALVES):
            units = pl.ds(pl.multiple_of(x_to * chunk + s * half, half), half)
            yield wx.at[:, depth, units], dst.at[pl.ds(0, 3), s]
            yield wru.at[:, depth, units], dst.at[pl.ds(3, 2), s]
            yield wn.at[depth, units], dst.at[5, s]

    def send_weights(layer, turns):
        for turn in turns:
            x_to = wrap_x(xpos + turn)
            for j in range(2):
                place = chunk_place(core, j, xpos, x_to, col)
                for src, dst in weight_pieces(layer, j, x_to, weights.at[layer, place]):
                    remote(src, dst, weight_sent.at[layer, turn, j], weight_sem.at[layer, place], device(x_to, 1, col)).start()

    def keep_weights(layer):
        for j in range(2):
            place = chunk_place(1, j, xpos, xpos, col)
            for src, dst in weight_pieces(layer, j, xpos, weights.at[layer, place]):
                pltpu.make_async_copy(src, dst, weight_sem.at[layer, place]).start()

    def hand_over():
        for turn in far_turns:
            x_to = wrap_x(xpos + turn)
            for j in range(2):
                for src, dst in weight_pieces(1, j, x_to, weights.at[1, 2 * turn + j]):
                    remote(src, dst, weight_sent.at[1, turn, j], hand_sem.at[turn, j], device(xpos, 0, col)).start()

    def send_handed():
        for turn in far_turns:
            x_to = wrap_x(xpos + turn)
            for j in range(2):
                src = weights.at[1, 2 * turn + j]
                pltpu.make_async_copy(src, src, hand_sem.at[turn, j]).wait()
                place = chunk_place(1, j, xpos, x_to, col)
                remote(src, weights.at[1, place], handed_sent.at[turn, j], weight_sem.at[1, place], device(x_to, 1, col)).start()

    share = steps // cols
    my_share = pl.ds(pl.multiple_of(col * share, share), share)

    def x_pieces(j, dst):
        for s in range(HALVES):
            yield x_ref.at[my_share, :, pl.ds(j * chunk + s * half, half)], dst.at[my_share, s]

    def send_x(turns):
        for turn in turns:
            x_to = wrap_x(xpos + turn)
            for j in range(2):
                place = chunk_place(core, j, xpos, x_to, col)
                for src, dst in x_pieces(j, xs.at[place]):
                    remote(src, dst, x_sent.at[turn, j], x_sem.at[place], device(x_to, 0, col)).start()

    def keep_x():
        for j in range(2):
            place = chunk_place(0, j, xpos, xpos, col)
            for src, dst in x_pieces(j, xs.at[place]):
                pltpu.make_async_copy(src, dst, x_sem.at[place]).start()

    def pass_x_on():
        for p in range(places):
            part = xs.at[p, my_share]
            pltpu.make_async_copy(part, part, x_sem.at[p]).wait()
        for k in range(cols):
            for dy in range(cols):
                src = xs.at[pl.ds(chips * dy, chips), my_share]
                dst = xs.at[pl.ds(chips * ((dy - k) % cols), chips), my_share]
                remote(src, dst, x_passed.at[k], xs_sem.at[col], device(xpos, 1, wrap_y(col + k))).start()

    far_turns = (2, 1, chips - 1)

    @pl.when(xpos == col)
    def _():
        for j in range(2):
            x_to = HALVES * core + j
            for s in range(HALVES):
                src = h_ref.at[:, :, pl.ds(j * chunk + s * half, half)]
                dst = state_in.at[:, s]
                mine = (x_to == xpos) & (core == 1)

                @pl.when(mine)
                def _():
                    pltpu.make_async_copy(src, dst, state_sem.at[s]).start()

                @pl.when(jnp.logical_not(mine))
                def _():
                    copy = remote(src, dst, state_sent.at[j, s], state_sem.at[s], device(x_to, 1, col))
                    copy.start()
                    copy.wait_send()

    send_x(far_turns)
    pl.when(core == 1)(lambda: send_x((0,)))
    pl.when(core == 0)(keep_x)
    send_weights(0, far_turns)

    @pl.when(core == 1)
    def _():
        keep_weights(0)
        hand_over()
        keep_weights(1)

    @pl.when(core == 0)
    def _():
        send_weights(0, (0,))
        pass_x_on()
        send_weights(1, far_turns)
        send_weights(1, (0,))
        send_handed()

    def drain_sends():
        piece = weights.at[0, 0]
        for layer in range(2):
            for j in range(2):
                for turn in far_turns:
                    pltpu.make_async_copy(piece, piece, weight_sent.at[layer, turn, j]).wait()

                @pl.when(core == 0)
                def _():
                    pltpu.make_async_copy(piece, piece, weight_sent.at[layer, 0, j]).wait()
        part = xs.at[0, my_share]
        for j in range(2):
            for turn in far_turns:
                pltpu.make_async_copy(part, part, x_sent.at[turn, j]).wait()

        @pl.when(core == 0)
        def _():
            for j in range(2):
                for turn in far_turns:
                    pltpu.make_async_copy(piece, piece, handed_sent.at[turn, j]).wait()
            whole = xs.at[:, my_share]
            for k in range(cols):
                pltpu.make_async_copy(whole, whole, x_passed.at[k]).wait()

        @pl.when(core == 1)
        def _():
            for j in range(2):
                pltpu.make_async_copy(part, part, x_sent.at[0, j]).wait()

    offsets = [(dx, dy) for dy in range(cols) for dx in range(chips)]
    distance = [ring_distance(dx, chips) + ring_distance(dy, cols) for dx, dy in offsets]
    far_first = sorted(range(1, places), key=lambda p: -distance[p])
    groups = [
        [p for p in range(places) if distance[p] <= 1],
        [p for p in range(places) if distance[p] == 2],
        [p for p in range(places) if distance[p] > 2],
    ]

    def spread(blocks, kind):
        for p in far_first:
            dx, dy = offsets[p]
            there = chips * ((cols - dy) % cols) + (chips - dx) % chips
            to = device(wrap_x(xpos + dx), 1, wrap_y(col + dy))
            remote(blocks.at[0], blocks.at[there], block_sent.at[kind], block_sem.at[kind, there], to).start()

    def arrived(blocks, kind, group):
        for p in group:
            if p:
                pltpu.make_async_copy(blocks.at[p], blocks.at[p], block_sem.at[kind, p]).wait()

    def all_sent(blocks, kind):
        sent = blocks.at[pl.ds(1, places - 1)]
        pltpu.make_async_copy(sent, sent, block_sent.at[kind]).wait()

    def wide(parts):
        return jnp.concatenate(parts, axis=1)

    def product(lhs_of, layer, gates, total=None, group=None):
        for p in range(places) if group is None else group:
            rhs = wide([weights[layer, p, g, s] for g in gates for s in range(HALVES)])
            lhs = wide([lhs_of(p, s) for s in range(HALVES)])
            term = jnp.dot(lhs, rhs, preferred_element_type=F32)
            total = term if total is None else total + term
        return total

    def gathered(blocks, kind, layer, gates):
        total = None
        for group in groups:
            arrived(blocks, kind, group)
            total = product(lambda p, s: blocks[p, s], layer, gates, total, group)
        return total

    def project(layer, lhs_of, bias):
        total = product(lhs_of, layer, (RESET, UPDATE, CAND))
        for g in range(3):
            for s in range(HALVES):
                n = g * HALVES + s
                here = bias[pl.ds(g, 1), pl.ds(pl.multiple_of(xpos * chunk + s * half, half), half)]
                projections[layer, g, s] = total[:, n * half : (n + 1) * half] + here

    def reset_half(layer, blocks, kind, out_blocks, send):
        total = gathered(blocks, kind, layer, (REC_RESET, REC_UPDATE))
        for s in range(HALVES):
            reset = jax.nn.sigmoid(projections[layer, RESET, s] + total[:, s * half : (s + 1) * half])
            out_blocks[0, s] = (reset * states[layer, s]).astype(BF16)
        send()
        for s in range(HALVES):
            n = HALVES + s
            updates[layer, s] = jax.nn.sigmoid(projections[layer, UPDATE, s] + total[:, n * half : (n + 1) * half])

    def next_half(layer, blocks, kind, emit):
        total = gathered(blocks, kind, layer, (REC_CAND,))
        for s in range(HALVES):
            candidate = jnp.tanh(projections[layer, CAND, s] + total[:, s * half : (s + 1) * half])
            update = updates[layer, s]
            state = (1.0 - update) * candidate + update * states[layer, s]
            states[layer, s] = state
            emit(s, state.astype(BF16))

    H1, R1, H2, R2 = range(4)

    def first_reset(t):
        slot = h1_blocks.at[lax.rem(t, 2)]
        reset_half(0, slot, H1, r1_blocks, lambda: spread(r1_blocks, R1))
        all_sent(slot, H1)

    def first_next(t):
        slot = h1_blocks.at[lax.rem(t + 1, 2)]

        def emit(s, value):
            slot[0, s] = value

        next_half(0, r1_blocks, R1, emit)
        all_sent(r1_blocks, R1)
        spread(slot, H1)

    def first_inputs(t):
        project(0, lambda p, s: xs[p, t, s], b1)

    def second_inputs(t):
        slot = h1_blocks.at[lax.rem(t, 2)]
        project(1, lambda p, s: slot[p, s], b2)

    def second_reset():
        reset_half(1, h2_blocks, H2, r2_blocks, lambda: spread(r2_blocks, R2))
        all_sent(h2_blocks, H2)

    def second_next(t, last):
        def emit(s, value):
            seq_halves[s, t] = value
            if not last:
                h2_blocks[0, s] = value

        next_half(1, r2_blocks, R2, emit)
        all_sent(r2_blocks, R2)
        if not last:
            spread(h2_blocks, H2)

    @pl.when(core == 1)
    def _():
        for s in range(HALVES):
            part = state_in.at[:, s]
            pltpu.make_async_copy(part, part, state_sem.at[s]).wait()
        for layer in range(2):
            for s in range(HALVES):
                states[layer, s] = state_in[layer, s]
        for s in range(HALVES):
            h1_blocks[0, 0, s] = state_in[0, s].astype(BF16)
            h2_blocks[0, s] = state_in[1, s].astype(BF16)
        spread(h1_blocks.at[0], H1)
        spread(h2_blocks, H2)
        for y in range(cols):
            part = xs.at[:, pl.ds(y * share, share)]
            pltpu.make_async_copy(part, part, xs_sem.at[y]).wait()
        for p in range(places):
            pltpu.make_async_copy(weights.at[0, p], weights.at[0, p], weight_sem.at[0, p]).wait()
        first_inputs(0)
        first_reset(0)
        first_next(0)
        first_inputs(jnp.minimum(1, steps - 1))
        for p in range(places):
            pltpu.make_async_copy(weights.at[1, p], weights.at[1, p], weight_sem.at[1, p]).wait()

        def step(t, carry):
            first_reset(t)
            second_inputs(t)
            second_reset()
            first_next(t)
            second_next(t - 1, False)
            first_inputs(jnp.minimum(t + 1, steps - 1))
            return carry

        lax.fori_loop(1, steps, step, 0)
        last_slot = h1_blocks.at[steps % 2]
        arrived(last_slot, H1, range(places))
        all_sent(last_slot, H1)
        second_inputs(steps)
        second_reset()
        second_next(steps - 1, True)
        for layer in range(2):
            for s in range(HALVES):
                last_halves[s, layer] = states[layer, s]
        seq_copy = remote(seq_halves.at[0], seq_out, out_sent.at[0], out_sem.at[0], device(xpos, 0, col))
        last_copy = remote(last_halves.at[0], last_out, out_sent.at[1], out_sem.at[1], device(xpos, 0, col))
        seq_copy.start()
        last_copy.start()
        seq_out[...] = seq_halves[1]
        last_out[...] = last_halves[1]
        seq_copy.wait_send()
        last_copy.wait_send()

    @pl.when(core == 0)
    def _():
        pltpu.make_async_copy(seq_out, seq_out, out_sem.at[0]).wait()
        pltpu.make_async_copy(last_out, last_out, out_sem.at[1]).wait()

    drain_sends()


def solution(mesh):
    rows, cols = mesh.shape["row"], mesh.shape["col"]
    chips = rows // CORES
    places = chips * cols

    def device_body(x_rows, h_rows, wx_l1, whru_l1, whn_l1, bias_l1, wx_l2, whru_l2, whn_l2, bias_l2):
        steps, batch, row_block = x_rows.shape
        col_block = wx_l1.shape[2]
        half = col_block // rows
        chunk = HALVES * half
        anywhere = pl.BlockSpec(memory_space=pl.ANY)
        vmem = pl.BlockSpec(memory_space=pltpu.VMEM)
        dma = pltpu.SemaphoreType.DMA
        kinds = 4
        block = (HALVES, batch, half)
        scratch = [
            pltpu.VMEM((2, places, GATES, HALVES, chunk, half), BF16),
            pltpu.VMEM((places, steps, *block), BF16),
            pltpu.VMEM((2, *block), F32),
            pltpu.VMEM((2, places, *block), BF16),
            pltpu.VMEM((places, *block), BF16),
            pltpu.VMEM((places, *block), BF16),
            pltpu.VMEM((places, *block), BF16),
            pltpu.VMEM((2, *block), F32),
            pltpu.VMEM((2, *block), F32),
            pltpu.VMEM((2, 3, *block), F32),
            pltpu.VMEM((HALVES, steps, batch, half), BF16),
            pltpu.VMEM((HALVES, 2, batch, half), F32),
            dma((2, places)),
            dma((chips, 2)),
            dma((places,)),
            dma((cols,)),
            dma((HALVES,)),
            dma((2, chips, 2)),
            dma((chips, 2)),
            dma((chips, 2)),
            dma((cols,)),
            dma((2, HALVES)),
            dma((kinds, places)),
            dma((kinds,)),
            dma((2,)),
            dma((2,)),
        ]
        return pl.pallas_call(
            functools.partial(gru_kernel, rows, cols),
            name="gru",
            out_shape=(
                jax.ShapeDtypeStruct((steps, batch, half), BF16),
                jax.ShapeDtypeStruct((2, batch, half), F32),
            ),
            in_specs=[anywhere, anywhere, anywhere, anywhere, anywhere, vmem, anywhere, anywhere, anywhere, vmem],
            out_specs=(vmem, vmem),
            scratch_shapes=scratch,
            compiler_params=pltpu.CompilerParams(
                collective_id=0, has_side_effects=True, vmem_limit_bytes=60 * 1024 * 1024
            ),
        )(
            x_rows, h_rows,
            jnp.transpose(wx_l1, (1, 0, 2)), jnp.transpose(whru_l1, (1, 0, 2)), whn_l1, bias_l1,
            jnp.transpose(wx_l2, (1, 0, 2)), jnp.transpose(whru_l2, (1, 0, 2)), whn_l2, bias_l2,
        )

    seq_spec = P(None, "data", "row")
    out_spec = P(None, "data", ("col", "row"))
    wide_spec = P("row", None, "col")
    square_spec = P("row", "col")
    bias_spec = P(None, "col")
    return jax.shard_map(
        device_body,
        mesh=mesh,
        in_specs=(seq_spec, seq_spec, wide_spec, wide_spec, square_spec, bias_spec, wide_spec, wide_spec, square_spec, bias_spec),
        out_specs=(out_spec, out_spec),
        check_vma=False,
    )
```

```python
import functools

import jax
import jax.numpy as jnp
from jax import lax
from jax.experimental import pallas as pl
from jax.experimental.pallas import tpu as pltpu
from jax.sharding import PartitionSpec as P

MESH = pl.DeviceIdType.MESH
F32 = jnp.float32
BF16 = jnp.bfloat16
HALVES = 2
CORES = 2
RESET, UPDATE, CAND, REC_RESET, REC_UPDATE, REC_CAND = range(6)
GATES = 6


def ring_distance(offset, count):
    return min(offset, count - offset)


def gru_kernel(
    rows, cols,
    x_ref, h_ref, wx1, wru1, wn1, b1, wx2, wru2, wn2, b2,
    seq_out, last_out,
    weights, xs, state_in,
    h1_blocks, r1_blocks, h2_blocks, r2_blocks,
    states, updates, projections, seq_halves, last_halves,
    weight_sem, hand_sem, x_sem, xs_sem, state_sem,
    weight_sent, handed_sent, x_sent, x_passed, state_sent,
    block_sem, block_sent, out_sem, out_sent,
):
    chips = rows // CORES
    steps, batch, half = seq_out.shape
    chunk = HALVES * half
    places = chips * cols
    row, col = lax.axis_index("row"), lax.axis_index("col")
    xpos, core = row // CORES, row % CORES
    layers = ((wx1, wru1, wn1), (wx2, wru2, wn2))

    def device(x, c, y):
        return {"row": CORES * x + c, "col": y}

    def wrap_x(v):
        return lax.rem(v + 2 * chips, chips)

    def wrap_y(v):
        return lax.rem(v + 2 * cols, cols)

    def place_of(x_from, y_from, x_to, y_to):
        return chips * wrap_y(y_from - y_to) + wrap_x(x_from - x_to)

    barrier = pltpu.get_barrier_semaphore()
    for k in range(1, rows * cols):
        other = {"row": lax.rem(row + k % rows, rows), "col": lax.rem(col + k // rows, cols)}
        pl.semaphore_signal(barrier, inc=1, device_id=other, device_id_type=MESH)
    pl.semaphore_wait(barrier, rows * cols - 1)

    def remote(src, dst, send, recv, to):
        return pltpu.make_async_remote_copy(
            src_ref=src, dst_ref=dst, send_sem=send, recv_sem=recv, device_id=to, device_id_type=MESH
        )

    def chunk_place(c, j, x_from, x_to, y_to):
        return place_of(HALVES * c + j, x_from, x_to, y_to)

    def weight_pieces(layer, j, x_to, dst):
        wx, wru, wn = layers[layer]
        depth = pl.ds(j * chunk, chunk)
        for s in range(HALVES):
            units = pl.ds(pl.multiple_of(x_to * chunk + s * half, half), half)
            yield wx.at[:, depth, units], dst.at[pl.ds(0, 3), s]
            yield wru.at[:, depth, units], dst.at[pl.ds(3, 2), s]
            yield wn.at[depth, units], dst.at[5, s]

    def send_weights(layer, turns):
        for turn in turns:
            x_to = wrap_x(xpos + turn)
            for j in range(2):
                place = chunk_place(core, j, xpos, x_to, col)
                for src, dst in weight_pieces(layer, j, x_to, weights.at[layer, place]):
                    remote(src, dst, weight_sent.at[layer, turn, j], weight_sem.at[layer, place], device(x_to, 1, col)).start()

    def keep_weights(layer):
        for j in range(2):
            place = chunk_place(1, j, xpos, xpos, col)
            for src, dst in weight_pieces(layer, j, xpos, weights.at[layer, place]):
                pltpu.make_async_copy(src, dst, weight_sem.at[layer, place]).start()

    def hand_over():
        for turn in far_turns:
            x_to = wrap_x(xpos + turn)
            for j in range(2):
                for src, dst in weight_pieces(1, j, x_to, weights.at[1, 2 * turn + j]):
                    remote(src, dst, weight_sent.at[1, turn, j], hand_sem.at[turn, j], device(xpos, 0, col)).start()

    def send_handed():
        for turn in far_turns:
            x_to = wrap_x(xpos + turn)
            for j in range(2):
                src = weights.at[1, 2 * turn + j]
                pltpu.make_async_copy(src, src, hand_sem.at[turn, j]).wait()
                place = chunk_place(1, j, xpos, x_to, col)
                remote(src, weights.at[1, place], handed_sent.at[turn, j], weight_sem.at[1, place], device(x_to, 1, col)).start()

    share = steps // cols
    my_share = pl.ds(pl.multiple_of(col * share, share), share)

    def x_pieces(j, dst):
        for s in range(HALVES):
            yield x_ref.at[my_share, :, pl.ds(j * chunk + s * half, half)], dst.at[my_share, s]

    def send_x(turns):
        for turn in turns:
            x_to = wrap_x(xpos + turn)
            for j in range(2):
                place = chunk_place(core, j, xpos, x_to, col)
                for src, dst in x_pieces(j, xs.at[place]):
                    remote(src, dst, x_sent.at[turn, j], x_sem.at[place], device(x_to, 0, col)).start()

    def keep_x():
        for j in range(2):
            place = chunk_place(0, j, xpos, xpos, col)
            for src, dst in x_pieces(j, xs.at[place]):
                pltpu.make_async_copy(src, dst, x_sem.at[place]).start()

    def pass_x_on():
        for p in range(places):
            part = xs.at[p, my_share]
            pltpu.make_async_copy(part, part, x_sem.at[p]).wait()
        for k in range(cols):
            for dy in range(cols):
                src = xs.at[pl.ds(chips * dy, chips), my_share]
                dst = xs.at[pl.ds(chips * ((dy - k) % cols), chips), my_share]
                remote(src, dst, x_passed.at[k], xs_sem.at[col], device(xpos, 1, wrap_y(col + k))).start()

    far_turns = (2, 1, chips - 1)

    @pl.when(xpos == col)
    def _():
        for j in range(2):
            x_to = HALVES * core + j
            for s in range(HALVES):
                src = h_ref.at[:, :, pl.ds(j * chunk + s * half, half)]
                dst = state_in.at[:, s]
                mine = (x_to == xpos) & (core == 1)

                @pl.when(mine)
                def _():
                    pltpu.make_async_copy(src, dst, state_sem.at[s]).start()

                @pl.when(jnp.logical_not(mine))
                def _():
                    copy = remote(src, dst, state_sent.at[j, s], state_sem.at[s], device(x_to, 1, col))
                    copy.start()
                    copy.wait_send()

    send_x(far_turns)
    pl.when(core == 1)(lambda: send_x((0,)))
    pl.when(core == 0)(keep_x)
    send_weights(0, far_turns)

    @pl.when(core == 1)
    def _():
        keep_weights(0)
        hand_over()
        keep_weights(1)

    @pl.when(core == 0)
    def _():
        send_weights(0, (0,))
        pass_x_on()
        send_weights(1, far_turns)
        send_weights(1, (0,))
        send_handed()

    def drain_sends():
        piece = weights.at[0, 0]
        for layer in range(2):
            for j in range(2):
                for turn in far_turns:
                    pltpu.make_async_copy(piece, piece, weight_sent.at[layer, turn, j]).wait()

                @pl.when(core == 0)
                def _():
                    pltpu.make_async_copy(piece, piece, weight_sent.at[layer, 0, j]).wait()
        part = xs.at[0, my_share]
        for j in range(2):
            for turn in far_turns:
                pltpu.make_async_copy(part, part, x_sent.at[turn, j]).wait()

        @pl.when(core == 0)
        def _():
            for j in range(2):
                for turn in far_turns:
                    pltpu.make_async_copy(piece, piece, handed_sent.at[turn, j]).wait()
            whole = xs.at[:, my_share]
            for k in range(cols):
                pltpu.make_async_copy(whole, whole, x_passed.at[k]).wait()

        @pl.when(core == 1)
        def _():
            for j in range(2):
                pltpu.make_async_copy(part, part, x_sent.at[0, j]).wait()

    offsets = [(dx, dy) for dy in range(cols) for dx in range(chips)]
    distance = [ring_distance(dx, chips) + ring_distance(dy, cols) for dx, dy in offsets]
    far_first = sorted(range(1, places), key=lambda p: -distance[p])
    by_arrival = sorted(range(places), key=lambda p: (distance[p], ring_distance(offsets[p][0], chips)))

    def spread(blocks, kind):
        for p in far_first:
            dx, dy = offsets[p]
            there = chips * ((cols - dy) % cols) + (chips - dx) % chips
            to = device(wrap_x(xpos + dx), 1, wrap_y(col + dy))
            remote(blocks.at[0], blocks.at[there], block_sent.at[kind], block_sem.at[kind, there], to).start()

    def arrived(blocks, kind, p):
        pltpu.make_async_copy(blocks.at[p], blocks.at[p], block_sem.at[kind, p]).wait()

    def all_sent(blocks, kind):
        sent = blocks.at[pl.ds(1, places - 1)]
        pltpu.make_async_copy(sent, sent, block_sent.at[kind]).wait()

    def wide(parts):
        return jnp.concatenate(parts, axis=1)

    def product(lhs_of, layer, gates, order, before=None):
        total = None
        for p in order:
            if before is not None and p:
                before(p)
            rhs = wide([weights[layer, p, g, s] for g in gates for s in range(HALVES)])
            lhs = wide([lhs_of(p, s) for s in range(HALVES)])
            term = jnp.dot(lhs, rhs, preferred_element_type=F32)
            total = term if total is None else total + term
        return total

    def gathered(blocks, kind, layer, gate):
        return product(lambda p, s: blocks[p, s], layer, (gate,), by_arrival, lambda p: arrived(blocks, kind, p))

    def project(layer, lhs_of, bias):
        total = product(lhs_of, layer, (RESET, UPDATE, CAND), range(places))
        for g in range(3):
            for s in range(HALVES):
                n = g * HALVES + s
                here = bias[pl.ds(g, 1), pl.ds(pl.multiple_of(xpos * chunk + s * half, half), half)]
                projections[layer, g, s] = total[:, n * half : (n + 1) * half] + here

    def reset_half(layer, blocks, kind, out_blocks, send):
        total = gathered(blocks, kind, layer, REC_RESET)
        for s in range(HALVES):
            reset = jax.nn.sigmoid(projections[layer, RESET, s] + total[:, s * half : (s + 1) * half])
            out_blocks[0, s] = (reset * states[layer, s]).astype(BF16)
        send()
        total = product(lambda p, s: blocks[p, s], layer, (REC_UPDATE,), range(places))
        for s in range(HALVES):
            updates[layer, s] = jax.nn.sigmoid(projections[layer, UPDATE, s] + total[:, s * half : (s + 1) * half])

    def next_half(layer, blocks, kind, emit):
        total = gathered(blocks, kind, layer, REC_CAND)
        for s in range(HALVES):
            candidate = jnp.tanh(projections[layer, CAND, s] + total[:, s * half : (s + 1) * half])
            update = updates[layer, s]
            state = (1.0 - update) * candidate + update * states[layer, s]
            emit(s, state.astype(BF16))
            states[layer, s] = state

    H1, R1, H2, R2 = range(4)

    def first_reset(t):
        slot = h1_blocks.at[lax.rem(t, 2)]
        reset_half(0, slot, H1, r1_blocks, lambda: spread(r1_blocks, R1))
        all_sent(slot, H1)

    def first_next(t):
        slot = h1_blocks.at[lax.rem(t + 1, 2)]

        def emit(s, value):
            slot[0, s] = value

        next_half(0, r1_blocks, R1, emit)
        all_sent(r1_blocks, R1)
        spread(slot, H1)

    def first_inputs(t):
        project(0, lambda p, s: xs[p, t, s], b1)

    def second_inputs(t):
        slot = h1_blocks.at[lax.rem(t, 2)]
        project(1, lambda p, s: slot[p, s], b2)

    def second_reset(t):
        slot = h2_blocks.at[lax.rem(t, 2)]
        reset_half(1, slot, H2, r2_blocks, lambda: spread(r2_blocks, R2))
        all_sent(slot, H2)

    def second_next(t, last):
        slot = h2_blocks.at[lax.rem(t + 1, 2)]

        def emit(s, value):
            seq_halves[s, t] = value
            if not last:
                slot[0, s] = value

        next_half(1, r2_blocks, R2, emit)
        all_sent(r2_blocks, R2)
        if not last:
            spread(slot, H2)

    @pl.when(core == 1)
    def _():
        for s in range(HALVES):
            part = state_in.at[:, s]
            pltpu.make_async_copy(part, part, state_sem.at[s]).wait()
        for layer in range(2):
            for s in range(HALVES):
                states[layer, s] = state_in[layer, s]
        for s in range(HALVES):
            h1_blocks[0, 0, s] = state_in[0, s].astype(BF16)
            h2_blocks[0, 0, s] = state_in[1, s].astype(BF16)
        spread(h1_blocks.at[0], H1)
        spread(h2_blocks.at[0], H2)
        for y in range(cols):
            part = xs.at[:, pl.ds(y * share, share)]
            pltpu.make_async_copy(part, part, xs_sem.at[y]).wait()
        for p in range(places):
            pltpu.make_async_copy(weights.at[0, p], weights.at[0, p], weight_sem.at[0, p]).wait()
        first_inputs(0)
        first_reset(0)
        first_next(0)
        first_inputs(jnp.minimum(1, steps - 1))
        for p in range(places):
            pltpu.make_async_copy(weights.at[1, p], weights.at[1, p], weight_sem.at[1, p]).wait()

        def step(t, carry):
            first_reset(t)
            second_inputs(t)
            second_reset(t - 1)
            first_next(t)
            second_next(t - 1, False)
            first_inputs(jnp.minimum(t + 1, steps - 1))
            return carry

        lax.fori_loop(1, steps, step, 0)
        last_slot = h1_blocks.at[steps % 2]
        for p in range(1, places):
            arrived(last_slot, H1, p)
        all_sent(last_slot, H1)
        second_inputs(steps)
        second_reset(steps - 1)
        second_next(steps - 1, True)
        for layer in range(2):
            for s in range(HALVES):
                last_halves[s, layer] = states[layer, s]
        seq_copy = remote(seq_halves.at[0], seq_out, out_sent.at[0], out_sem.at[0], device(xpos, 0, col))
        last_copy = remote(last_halves.at[0], last_out, out_sent.at[1], out_sem.at[1], device(xpos, 0, col))
        seq_copy.start()
        last_copy.start()
        seq_out[...] = seq_halves[1]
        last_out[...] = last_halves[1]
        seq_copy.wait_send()
        last_copy.wait_send()

    @pl.when(core == 0)
    def _():
        pltpu.make_async_copy(seq_out, seq_out, out_sem.at[0]).wait()
        pltpu.make_async_copy(last_out, last_out, out_sem.at[1]).wait()

    drain_sends()


def solution(mesh):
    rows, cols = mesh.shape["row"], mesh.shape["col"]
    chips = rows // CORES
    places = chips * cols

    def device_body(x_rows, h_rows, wx_l1, whru_l1, whn_l1, bias_l1, wx_l2, whru_l2, whn_l2, bias_l2):
        steps, batch, row_block = x_rows.shape
        col_block = wx_l1.shape[2]
        half = col_block // rows
        chunk = HALVES * half
        anywhere = pl.BlockSpec(memory_space=pl.ANY)
        vmem = pl.BlockSpec(memory_space=pltpu.VMEM)
        dma = pltpu.SemaphoreType.DMA
        kinds = 4
        block = (HALVES, batch, half)
        scratch = [
            pltpu.VMEM((2, places, GATES, HALVES, chunk, half), BF16),
            pltpu.VMEM((places, steps, *block), BF16),
            pltpu.VMEM((2, *block), F32),
            pltpu.VMEM((2, places, *block), BF16),
            pltpu.VMEM((places, *block), BF16),
            pltpu.VMEM((2, places, *block), BF16),
            pltpu.VMEM((places, *block), BF16),
            pltpu.VMEM((2, *block), F32),
            pltpu.VMEM((2, *block), F32),
            pltpu.VMEM((2, 3, *block), F32),
            pltpu.VMEM((HALVES, steps, batch, half), BF16),
            pltpu.VMEM((HALVES, 2, batch, half), F32),
            dma((2, places)),
            dma((chips, 2)),
            dma((places,)),
            dma((cols,)),
            dma((HALVES,)),
            dma((2, chips, 2)),
            dma((chips, 2)),
            dma((chips, 2)),
            dma((cols,)),
            dma((2, HALVES)),
            dma((kinds, places)),
            dma((kinds,)),
            dma((2,)),
            dma((2,)),
        ]
        return pl.pallas_call(
            functools.partial(gru_kernel, rows, cols),
            name="gru",
            out_shape=(
                jax.ShapeDtypeStruct((steps, batch, half), BF16),
                jax.ShapeDtypeStruct((2, batch, half), F32),
            ),
            in_specs=[anywhere, anywhere, anywhere, anywhere, anywhere, vmem, anywhere, anywhere, anywhere, vmem],
            out_specs=(vmem, vmem),
            scratch_shapes=scratch,
            compiler_params=pltpu.CompilerParams(
                collective_id=0, has_side_effects=True, vmem_limit_bytes=60 * 1024 * 1024
            ),
        )(
            x_rows, h_rows,
            jnp.transpose(wx_l1, (1, 0, 2)), jnp.transpose(whru_l1, (1, 0, 2)), whn_l1, bias_l1,
            jnp.transpose(wx_l2, (1, 0, 2)), jnp.transpose(whru_l2, (1, 0, 2)), whn_l2, bias_l2,
        )

    seq_spec = P(None, "data", "row")
    out_spec = P(None, "data", ("col", "row"))
    wide_spec = P("row", None, "col")
    square_spec = P("row", "col")
    bias_spec = P(None, "col")
    return jax.shard_map(
        device_body,
        mesh=mesh,
        in_specs=(seq_spec, seq_spec, wide_spec, wide_spec, square_spec, bias_spec, wide_spec, wide_spec, square_spec, bias_spec),
        out_specs=(out_spec, out_spec),
        check_vma=False,
    )
```

```python
import functools

import jax
import jax.numpy as jnp
from jax import lax
from jax.experimental import pallas as pl
from jax.experimental.pallas import tpu as pltpu
from jax.sharding import PartitionSpec as P

MESH = pl.DeviceIdType.MESH
F32 = jnp.float32
BF16 = jnp.bfloat16
HALVES = 2
CORES = 2
RESET, UPDATE, CAND = range(3)
GATES = 3


def ring_distance(offset, count):
    return min(offset, count - offset)


def gru_kernel(
    rows, cols,
    x_ref, h_ref, wx1, wru1, wn1, b1, wx2, wru2, wn2, b2,
    seq_out, last_out,
    recurrent, inputs, xs, state_in, h1_here,
    h1_blocks, r1_blocks, h2_blocks, r2_blocks,
    first_p, second_p, first_made, second_made,
    states, updates, seq_halves, last_halves,
    recurrent_sem, inputs_sem, hand_sem, x_sem, xs_sem, state_sem,
    recurrent_sent, inputs_sent, handed_sent, x_sent, x_passed, state_sent,
    block_sem, block_sent, h1_sem, h1_sent, first_sem, first_sent, second_sem, second_sent,
    out_sem, out_sent,
):
    chips = rows // CORES
    steps, batch, half = seq_out.shape
    chunk = HALVES * half
    places = chips * cols
    row, col = lax.axis_index("row"), lax.axis_index("col")
    xpos, core = row // CORES, row % CORES
    layers = ((wx1, wru1, wn1), (wx2, wru2, wn2))
    turns = (2, 1, chips - 1)

    def device(x, c, y):
        return {"row": CORES * x + c, "col": y}

    def wrap_x(v):
        return lax.rem(v + 2 * chips, chips)

    def wrap_y(v):
        return lax.rem(v + 2 * cols, cols)

    barrier = pltpu.get_barrier_semaphore()
    for k in range(1, rows * cols):
        other = {"row": lax.rem(row + k % rows, rows), "col": lax.rem(col + k // rows, cols)}
        pl.semaphore_signal(barrier, inc=1, device_id=other, device_id_type=MESH)
    pl.semaphore_wait(barrier, rows * cols - 1)

    def remote(src, dst, send, recv, to):
        return pltpu.make_async_remote_copy(
            src_ref=src, dst_ref=dst, send_sem=send, recv_sem=recv, device_id=to, device_id_type=MESH
        )

    def local(src, dst, sem):
        return pltpu.make_async_copy(src, dst, sem)

    def wait_for(ref, sem):
        pltpu.make_async_copy(ref, ref, sem).wait()

    def chunk_place(c, j, x_from, x_to, y_to):
        return chips * wrap_y(x_from - y_to) + wrap_x(HALVES * c + j - x_to)

    def recurrent_pieces(layer, j, x_to, dst):
        _, wru, wn = layers[layer]
        depth = pl.ds(j * chunk, chunk)
        for s in range(HALVES):
            units = pl.ds(pl.multiple_of(x_to * chunk + s * half, half), half)
            yield wru.at[:, depth, units], dst.at[pl.ds(0, 2), s]
            yield wn.at[depth, units], dst.at[2, s]

    def inputs_pieces(layer, j, x_to, dst):
        depth = pl.ds(j * chunk, chunk)
        for s in range(HALVES):
            units = pl.ds(pl.multiple_of(x_to * chunk + s * half, half), half)
            yield layers[layer][0].at[:, depth, units], dst.at[:, s]

    parts = (
        (recurrent_pieces, recurrent, recurrent_sem, recurrent_sent, 1),
        (inputs_pieces, inputs, inputs_sem, inputs_sent, 0),
    )

    def send_part(part, layer, turn):
        pieces, kept, sem, sent, to_core = part
        x_to = wrap_x(xpos + turn)
        for j in range(2):
            place = chunk_place(core, j, xpos, x_to, col)
            for src, dst in pieces(layer, j, x_to, kept.at[layer, place]):
                remote(src, dst, sent.at[layer, turn, j], sem.at[layer, place], device(x_to, to_core, col)).start()

    def keep_part(part, layer):
        pieces, kept, sem, _, c = part
        for j in range(2):
            place = chunk_place(c, j, xpos, xpos, col)
            for src, dst in pieces(layer, j, xpos, kept.at[layer, place]):
                local(src, dst, sem.at[layer, place]).start()

    def send_weights(layer):
        for turn in turns:
            for part in parts:
                send_part(part, layer, turn)

    def share_in_chip(layer):
        for part in parts:
            here = core == part[4]
            pl.when(here)(functools.partial(keep_part, part, layer))
            pl.when(jnp.logical_not(here))(functools.partial(send_part, part, layer, 0))

    def hand_over():
        for turn in turns:
            x_to = wrap_x(xpos + turn)
            for n, (pieces, _, _, sent, _) in enumerate(parts):
                for j in range(2):
                    for src, dst in pieces(1, j, x_to, recurrent.at[n, 2 * turn + j]):
                        remote(src, dst, sent.at[1, turn, j], hand_sem.at[n, turn, j], device(xpos, 0, col)).start()

    def send_handed():
        for turn in turns:
            x_to = wrap_x(xpos + turn)
            for n, (_, kept, sem, _, to_core) in enumerate(parts):
                for j in range(2):
                    src = recurrent.at[n, 2 * turn + j]
                    wait_for(src, hand_sem.at[n, turn, j])
                    place = chunk_place(1, j, xpos, x_to, col)
                    remote(src, kept.at[1, place], handed_sent.at[n, turn, j], sem.at[1, place], device(x_to, to_core, col)).start()

    share = steps // cols

    def share_of(y):
        return pl.ds(pl.multiple_of(y * share, share), share)

    my_share = share_of(col)

    def x_pieces(j, dst):
        for s in range(HALVES):
            yield x_ref.at[my_share, :, pl.ds(j * chunk + s * half, half)], dst.at[my_share, s]

    def send_x(turn):
        x_to = wrap_x(xpos + turn)
        for j in range(2):
            place = chunk_place(core, j, xpos, x_to, col)
            for src, dst in x_pieces(j, xs.at[place]):
                remote(src, dst, x_sent.at[turn, j], x_sem.at[place], device(x_to, 0, col)).start()

    def keep_x():
        for j in range(2):
            place = chunk_place(0, j, xpos, xpos, col)
            for src, dst in x_pieces(j, xs.at[place]):
                local(src, dst, x_sem.at[place]).start()

    def pass_x_on():
        for p in range(places):
            wait_for(xs.at[p, my_share], x_sem.at[p])
        for k in range(1, cols):
            for dy in range(cols):
                src = xs.at[pl.ds(chips * dy, chips), my_share]
                dst = xs.at[pl.ds(chips * ((dy - k) % cols), chips), my_share]
                remote(src, dst, x_passed.at[k], xs_sem.at[k], device(xpos, 0, wrap_y(col + k))).start()

    @pl.when(xpos == col)
    def _():
        for j in range(2):
            x_to = HALVES * core + j
            for s in range(HALVES):
                src = h_ref.at[:, :, pl.ds(j * chunk + s * half, half)]
                dst = state_in.at[:, s]
                mine = (x_to == xpos) & (core == 1)

                @pl.when(mine)
                def _():
                    local(src, dst, state_sem.at[s]).start()

                @pl.when(jnp.logical_not(mine))
                def _():
                    copy = remote(src, dst, state_sent.at[j, s], state_sem.at[s], device(x_to, 1, col))
                    copy.start()
                    copy.wait_send()

    for turn in turns:
        send_x(turn)
    pl.when(core == 1)(lambda: send_x(0))
    pl.when(core == 0)(keep_x)
    send_weights(0)
    share_in_chip(0)

    @pl.when(core == 1)
    def _():
        hand_over()

    @pl.when(core == 0)
    def _():
        pass_x_on()
        send_weights(1)

    share_in_chip(1)
    pl.when(core == 0)(send_handed)

    def drain_sends():
        piece = recurrent.at[0, 0]
        for layer in range(2):
            for j in range(2):
                for n, (_, _, _, sent, to_core) in enumerate(parts):
                    for turn in turns:
                        wait_for(piece, sent.at[layer, turn, j])

                    @pl.when(core != to_core)
                    def _():
                        wait_for(piece, sent.at[layer, 0, j])

        part = xs.at[0, my_share]
        for j in range(2):
            for turn in turns:
                wait_for(part, x_sent.at[turn, j])

        @pl.when(core == 0)
        def _():
            for n in range(len(parts)):
                for j in range(2):
                    for turn in turns:
                        wait_for(piece, handed_sent.at[n, turn, j])
            for k in range(1, cols):
                wait_for(xs.at[:, my_share], x_passed.at[k])

        @pl.when(core == 1)
        def _():
            for j in range(2):
                wait_for(part, x_sent.at[0, j])

    offsets = [(dx, dy) for dy in range(cols) for dx in range(chips)]
    distance = [ring_distance(dx, chips) + ring_distance(dy, cols) for dx, dy in offsets]
    far_first = sorted(range(1, places), key=lambda p: -distance[p])
    by_arrival = sorted(range(places), key=lambda p: (distance[p], ring_distance(offsets[p][0], chips)))

    def spread(blocks, kind):
        for p in far_first:
            dx, dy = offsets[p]
            there = chips * ((cols - dy) % cols) + (chips - dx) % chips
            to = device(wrap_x(xpos + dx), 1, wrap_y(col + dy))
            remote(blocks.at[0], blocks.at[there], block_sent.at[kind], block_sem.at[kind, there], to).start()

    def arrived(blocks, kind, p):
        wait_for(blocks.at[p], block_sem.at[kind, p])

    def all_sent(blocks, kind):
        wait_for(blocks.at[pl.ds(1, places - 1)], block_sent.at[kind])

    def wide(pieces):
        return jnp.concatenate(pieces, axis=1)

    def product(lhs_of, kept, layer, gates, order, before=None):
        total = None
        for p in order:
            if before is not None and p:
                before(p)
            rhs = wide([kept[layer, p, g, s] for g in gates for s in range(HALVES)])
            lhs = wide([lhs_of(p, s) for s in range(HALVES)])
            term = jnp.dot(lhs, rhs, preferred_element_type=F32)
            total = term if total is None else total + term
        return total

    def gathered(blocks, kind, layer, gate):
        return product(lambda p, s: blocks[p, s], recurrent, layer, (gate,), by_arrival, lambda p: arrived(blocks, kind, p))

    def halves_of(total, n=0):
        return [total[:, (n * HALVES + s) * half : (n * HALVES + s + 1) * half] for s in range(HALVES)]

    H1, R1, H2, R2 = range(4)

    def project(layer, lhs_of, bias, made):
        total = product(lhs_of, inputs, layer, (RESET, UPDATE, CAND), range(places))
        for g in range(3):
            for s, value in enumerate(halves_of(total, g)):
                here = bias[pl.ds(g, 1), pl.ds(pl.multiple_of(xpos * chunk + s * half, half), half)]
                made[g, s] = value + here

    def make_first(t, again):
        slot = lax.rem(t, 2)
        if again:
            wait_for(first_made.at[slot], first_sent.at[slot])
        project(0, lambda p, s: xs[p, t, s], b1, first_made.at[slot])
        remote(first_made.at[slot], first_p.at[slot], first_sent.at[slot], first_sem.at[slot], device(xpos, 1, col)).start()

    def make_second(again):
        if again:
            wait_for(second_made, second_sent)
        wait_for(h1_here, h1_sem)
        project(1, lambda p, s: h1_here[p, s], b2, second_made)
        remote(second_made, second_p, second_sent, second_sem, device(xpos, 1, col)).start()

    def reset_half(layer, blocks, kind, out_blocks, p_ref, before_send, after_send):
        total = gathered(blocks, kind, layer, RESET)
        before_send()
        for s, value in enumerate(halves_of(total)):
            reset = jax.nn.sigmoid(p_ref[RESET, s] + value)
            out_blocks[0, s] = (reset * states[layer, s]).astype(BF16)
        after_send()
        total = product(lambda p, s: blocks[p, s], recurrent, layer, (UPDATE,), range(places))
        for s, value in enumerate(halves_of(total)):
            updates[layer, s] = jax.nn.sigmoid(p_ref[UPDATE, s] + value)
        all_sent(blocks, kind)

    def next_half(layer, blocks, kind, p_ref, emit):
        total = gathered(blocks, kind, layer, CAND)
        for s, value in enumerate(halves_of(total)):
            candidate = jnp.tanh(p_ref[CAND, s] + value)
            update = updates[layer, s]
            state = (1.0 - update) * candidate + update * states[layer, s]
            emit(s, state.astype(BF16))
            states[layer, s] = state
        all_sent(blocks, kind)

    def hand_state(slot):
        remote(slot, h1_here, h1_sent, h1_sem, device(xpos, 0, col)).start()

    def first_reset(t, hand, handed):
        slot = h1_blocks.at[lax.rem(t, 2)]

        def before_send():
            wait_for(first_p.at[lax.rem(t, 2)], first_sem.at[lax.rem(t, 2)])
            if handed:
                wait_for(slot, h1_sent)

        def after_send():
            spread(r1_blocks, R1)
            if hand:
                hand_state(slot)

        reset_half(0, slot, H1, r1_blocks, first_p.at[lax.rem(t, 2)], before_send, after_send)

    def first_next(t):
        slot = h1_blocks.at[lax.rem(t + 1, 2)]

        def emit(s, value):
            slot[0, s] = value

        next_half(0, r1_blocks, R1, first_p.at[lax.rem(t, 2)], emit)
        spread(slot, H1)

    def second_reset(t):
        slot = h2_blocks.at[lax.rem(t, 2)]
        reset_half(
            1, slot, H2, r2_blocks, second_p, lambda: wait_for(second_p, second_sem), lambda: spread(r2_blocks, R2)
        )

    def second_next(t, last):
        slot = h2_blocks.at[lax.rem(t + 1, 2)]

        def emit(s, value):
            seq_halves[s, t] = value
            if not last:
                slot[0, s] = value

        next_half(1, r2_blocks, R2, second_p, emit)
        if not last:
            spread(slot, H2)

    def weights_here(kept, sem, layer):
        for p in range(places):
            wait_for(kept.at[layer, p], sem.at[layer, p])

    @pl.when(core == 1)
    def _():
        for s in range(HALVES):
            wait_for(state_in.at[:, s], state_sem.at[s])
        for layer in range(2):
            for s in range(HALVES):
                states[layer, s] = state_in[layer, s]
        for s in range(HALVES):
            h1_blocks[0, 0, s] = state_in[0, s].astype(BF16)
            h2_blocks[0, 0, s] = state_in[1, s].astype(BF16)
        spread(h1_blocks.at[0], H1)
        spread(h2_blocks.at[0], H2)
        weights_here(recurrent, recurrent_sem, 0)
        first_reset(0, False, False)
        first_next(0)
        weights_here(recurrent, recurrent_sem, 1)

        def step(t, handed):
            first_reset(t, True, handed)
            second_reset(t - 1)
            first_next(t)
            second_next(t - 1, False)

        def later_step(t, carry):
            step(t, True)
            return carry

        step(1, False)
        lax.fori_loop(2, steps, later_step, 0)
        last_slot = h1_blocks.at[steps % 2]
        for p in range(1, places):
            arrived(last_slot, H1, p)
        wait_for(last_slot, h1_sent)
        hand_state(last_slot)
        all_sent(last_slot, H1)
        second_reset(steps - 1)
        second_next(steps - 1, True)
        wait_for(last_slot, h1_sent)
        for layer in range(2):
            for s in range(HALVES):
                last_halves[s, layer] = states[layer, s]
        seq_copy = remote(seq_halves.at[0], seq_out, out_sent.at[0], out_sem.at[0], device(xpos, 0, col))
        last_copy = remote(last_halves.at[0], last_out, out_sent.at[1], out_sem.at[1], device(xpos, 0, col))
        seq_copy.start()
        last_copy.start()
        seq_out[...] = seq_halves[1]
        last_out[...] = last_halves[1]
        seq_copy.wait_send()
        last_copy.wait_send()

    @pl.when(core == 0)
    def _():
        for k in range(1, cols):
            wait_for(xs.at[:, share_of(wrap_y(col - k))], xs_sem.at[k])
        weights_here(inputs, inputs_sem, 0)
        make_first(0, False)
        make_first(1, False)
        weights_here(inputs, inputs_sem, 1)
        make_second(False)
        make_first(2, True)

        def later_step(t, carry):
            make_second(True)
            make_first(t + 1, True)
            return carry

        lax.fori_loop(2, steps - 1, later_step, 0)
        make_second(True)
        make_second(True)
        for slot in range(2):
            wait_for(first_made.at[slot], first_sent.at[slot])
        wait_for(second_made, second_sent)
        wait_for(seq_out, out_sem.at[0])
        wait_for(last_out, out_sem.at[1])

    drain_sends()


def solution(mesh):
    rows, cols = mesh.shape["row"], mesh.shape["col"]
    chips = rows // CORES
    places = chips * cols

    def device_body(x_rows, h_rows, wx_l1, whru_l1, whn_l1, bias_l1, wx_l2, whru_l2, whn_l2, bias_l2):
        steps, batch, row_block = x_rows.shape
        col_block = wx_l1.shape[2]
        half = col_block // rows
        chunk = HALVES * half
        anywhere = pl.BlockSpec(memory_space=pl.ANY)
        vmem = pl.BlockSpec(memory_space=pltpu.VMEM)
        dma = pltpu.SemaphoreType.DMA
        kinds = 4
        block = (HALVES, batch, half)
        scratch = [
            pltpu.VMEM((2, places, GATES, HALVES, chunk, half), BF16),
            pltpu.VMEM((2, places, GATES, HALVES, chunk, half), BF16),
            pltpu.VMEM((places, steps, *block), BF16),
            pltpu.VMEM((2, *block), F32),
            pltpu.VMEM((places, *block), BF16),
            pltpu.VMEM((2, places, *block), BF16),
            pltpu.VMEM((places, *block), BF16),
            pltpu.VMEM((2, places, *block), BF16),
            pltpu.VMEM((places, *block), BF16),
            pltpu.VMEM((2, GATES, *block), F32),
            pltpu.VMEM((GATES, *block), F32),
            pltpu.VMEM((2, GATES, *block), F32),
            pltpu.VMEM((GATES, *block), F32),
            pltpu.VMEM((2, *block), F32),
            pltpu.VMEM((2, *block), F32),
            pltpu.VMEM((HALVES, steps, batch, half), BF16),
            pltpu.VMEM((HALVES, 2, batch, half), F32),
            dma((2, places)),
            dma((2, places)),
            dma((2, chips, 2)),
            dma((places,)),
            dma((cols,)),
            dma((HALVES,)),
            dma((2, chips, 2)),
            dma((2, chips, 2)),
            dma((2, chips, 2)),
            dma((chips, 2)),
            dma((cols,)),
            dma((2, HALVES)),
            dma((kinds, places)),
            dma((kinds,)),
            dma,
            dma,
            dma((2,)),
            dma((2,)),
            dma,
            dma,
            dma((2,)),
            dma((2,)),
        ]
        return pl.pallas_call(
            functools.partial(gru_kernel, rows, cols),
            name="gru",
            out_shape=(
                jax.ShapeDtypeStruct((steps, batch, half), BF16),
                jax.ShapeDtypeStruct((2, batch, half), F32),
            ),
            in_specs=[anywhere, anywhere, anywhere, anywhere, anywhere, vmem, anywhere, anywhere, anywhere, vmem],
            out_specs=(vmem, vmem),
            scratch_shapes=scratch,
            compiler_params=pltpu.CompilerParams(
                collective_id=0, has_side_effects=True, vmem_limit_bytes=60 * 1024 * 1024
            ),
        )(
            x_rows, h_rows,
            jnp.transpose(wx_l1, (1, 0, 2)), jnp.transpose(whru_l1, (1, 0, 2)), whn_l1, bias_l1,
            jnp.transpose(wx_l2, (1, 0, 2)), jnp.transpose(whru_l2, (1, 0, 2)), whn_l2, bias_l2,
        )

    seq_spec = P(None, "data", "row")
    out_spec = P(None, "data", ("col", "row"))
    wide_spec = P("row", None, "col")
    square_spec = P("row", "col")
    bias_spec = P(None, "col")
    return jax.shard_map(
        device_body,
        mesh=mesh,
        in_specs=(seq_spec, seq_spec, wide_spec, wide_spec, square_spec, bias_spec, wide_spec, wide_spec, square_spec, bias_spec),
        out_specs=(out_spec, out_spec),
        check_vma=False,
    )
```

```python
import functools

import jax
import jax.numpy as jnp
from jax import lax
from jax.experimental import pallas as pl
from jax.experimental.pallas import tpu as pltpu
from jax.sharding import PartitionSpec as P

MESH = pl.DeviceIdType.MESH
F32 = jnp.float32
BF16 = jnp.bfloat16
HALVES = 2
CORES = 2
RESET, UPDATE, CAND, REC_RESET, REC_UPDATE, REC_CAND = range(6)
GATES = 6


def ring_distance(offset, count):
    return min(offset, count - offset)


def gru_kernel(
    rows, cols,
    x_ref, h_ref, wx1, wru1, wn1, b1, wx2, wru2, wn2, b2,
    seq_out, last_out,
    weights, xs, state_in,
    h1_blocks, r1_blocks, h2_blocks, r2_blocks,
    states, updates, projections, seq_halves, last_halves,
    weight_sem, hand_sem, x_sem, xs_sem, state_sem,
    weight_sent, handed_sent, x_sent, x_passed, state_sent,
    block_sem, block_sent, out_sem, out_sent,
):
    chips = rows // CORES
    steps, batch, half = seq_out.shape
    chunk = HALVES * half
    places = chips * cols
    row, col = lax.axis_index("row"), lax.axis_index("col")
    xpos, core = row // CORES, row % CORES
    layers = ((wx1, wru1, wn1), (wx2, wru2, wn2))

    def device(x, c, y):
        return {"row": CORES * x + c, "col": y}

    def wrap_x(v):
        return lax.rem(v + 2 * chips, chips)

    def wrap_y(v):
        return lax.rem(v + 2 * cols, cols)

    def place_of(x_from, y_from, x_to, y_to):
        return chips * wrap_y(y_from - y_to) + wrap_x(x_from - x_to)

    barrier = pltpu.get_barrier_semaphore()
    for k in range(1, rows * cols):
        other = {"row": lax.rem(row + k % rows, rows), "col": lax.rem(col + k // rows, cols)}
        pl.semaphore_signal(barrier, inc=1, device_id=other, device_id_type=MESH)
    pl.semaphore_wait(barrier, rows * cols - 1)

    def remote(src, dst, send, recv, to):
        return pltpu.make_async_remote_copy(
            src_ref=src, dst_ref=dst, send_sem=send, recv_sem=recv, device_id=to, device_id_type=MESH
        )

    def chunk_place(c, j, x_from, x_to, y_to):
        return place_of(HALVES * c + j, x_from, x_to, y_to)

    def weight_pieces(layer, j, x_to, dst):
        wx, wru, wn = layers[layer]
        depth = pl.ds(j * chunk, chunk)
        for s in range(HALVES):
            units = pl.ds(pl.multiple_of(x_to * chunk + s * half, half), half)
            yield wx.at[:, depth, units], dst.at[pl.ds(0, 3), s]
            yield wru.at[:, depth, units], dst.at[pl.ds(3, 2), s]
            yield wn.at[depth, units], dst.at[5, s]

    def send_weights(layer, turns):
        for turn in turns:
            x_to = wrap_x(xpos + turn)
            for j in range(2):
                place = chunk_place(core, j, xpos, x_to, col)
                for src, dst in weight_pieces(layer, j, x_to, weights.at[layer, place]):
                    remote(src, dst, weight_sent.at[layer, turn, j], weight_sem.at[layer, place], device(x_to, 1, col)).start()

    def keep_weights(layer):
        for j in range(2):
            place = chunk_place(1, j, xpos, xpos, col)
            for src, dst in weight_pieces(layer, j, xpos, weights.at[layer, place]):
                pltpu.make_async_copy(src, dst, weight_sem.at[layer, place]).start()

    def hand_over():
        for turn in far_turns:
            x_to = wrap_x(xpos + turn)
            for j in range(2):
                for src, dst in weight_pieces(1, j, x_to, weights.at[1, 2 * turn + j]):
                    remote(src, dst, weight_sent.at[1, turn, j], hand_sem.at[turn, j], device(xpos, 0, col)).start()

    def send_handed():
        for turn in far_turns:
            x_to = wrap_x(xpos + turn)
            for j in range(2):
                src = weights.at[1, 2 * turn + j]
                pltpu.make_async_copy(src, src, hand_sem.at[turn, j]).wait()
                place = chunk_place(1, j, xpos, x_to, col)
                remote(src, weights.at[1, place], handed_sent.at[turn, j], weight_sem.at[1, place], device(x_to, 1, col)).start()

    share = steps // cols
    my_share = pl.ds(pl.multiple_of(col * share, share), share)

    def x_pieces(j, dst):
        for s in range(HALVES):
            yield x_ref.at[my_share, :, pl.ds(j * chunk + s * half, half)], dst.at[my_share, s]

    def send_x(turns):
        for turn in turns:
            x_to = wrap_x(xpos + turn)
            for j in range(2):
                place = chunk_place(core, j, xpos, x_to, col)
                for src, dst in x_pieces(j, xs.at[place]):
                    remote(src, dst, x_sent.at[turn, j], x_sem.at[place], device(x_to, 0, col)).start()

    def keep_x():
        for j in range(2):
            place = chunk_place(0, j, xpos, xpos, col)
            for src, dst in x_pieces(j, xs.at[place]):
                pltpu.make_async_copy(src, dst, x_sem.at[place]).start()

    def pass_x_on():
        for p in range(places):
            part = xs.at[p, my_share]
            pltpu.make_async_copy(part, part, x_sem.at[p]).wait()
        for k in range(cols):
            for dy in range(cols):
                src = xs.at[pl.ds(chips * dy, chips), my_share]
                dst = xs.at[pl.ds(chips * ((dy - k) % cols), chips), my_share]
                remote(src, dst, x_passed.at[k], xs_sem.at[col], device(xpos, 1, wrap_y(col + k))).start()

    far_turns = (2, 1, chips - 1)

    @pl.when(xpos == col)
    def _():
        for j in range(2):
            x_to = HALVES * core + j
            for s in range(HALVES):
                src = h_ref.at[:, :, pl.ds(j * chunk + s * half, half)]
                dst = state_in.at[:, s]
                mine = (x_to == xpos) & (core == 1)

                @pl.when(mine)
                def _():
                    pltpu.make_async_copy(src, dst, state_sem.at[s]).start()

                @pl.when(jnp.logical_not(mine))
                def _():
                    copy = remote(src, dst, state_sent.at[j, s], state_sem.at[s], device(x_to, 1, col))
                    copy.start()
                    copy.wait_send()

    send_x(far_turns)
    pl.when(core == 1)(lambda: send_x((0,)))
    pl.when(core == 0)(keep_x)
    send_weights(0, far_turns)

    @pl.when(core == 1)
    def _():
        keep_weights(0)
        hand_over()
        keep_weights(1)

    @pl.when(core == 0)
    def _():
        send_weights(0, (0,))
        pass_x_on()
        send_weights(1, far_turns)
        send_weights(1, (0,))
        send_handed()

    def drain_sends():
        piece = weights.at[0, 0]
        for layer in range(2):
            for j in range(2):
                for turn in far_turns:
                    pltpu.make_async_copy(piece, piece, weight_sent.at[layer, turn, j]).wait()

                @pl.when(core == 0)
                def _():
                    pltpu.make_async_copy(piece, piece, weight_sent.at[layer, 0, j]).wait()
        part = xs.at[0, my_share]
        for j in range(2):
            for turn in far_turns:
                pltpu.make_async_copy(part, part, x_sent.at[turn, j]).wait()

        @pl.when(core == 0)
        def _():
            for j in range(2):
                for turn in far_turns:
                    pltpu.make_async_copy(piece, piece, handed_sent.at[turn, j]).wait()
            whole = xs.at[:, my_share]
            for k in range(cols):
                pltpu.make_async_copy(whole, whole, x_passed.at[k]).wait()

        @pl.when(core == 1)
        def _():
            for j in range(2):
                pltpu.make_async_copy(part, part, x_sent.at[0, j]).wait()

    offsets = [(dx, dy) for dy in range(cols) for dx in range(chips)]
    distance = [ring_distance(dx, chips) + ring_distance(dy, cols) for dx, dy in offsets]
    far_first = sorted(range(1, places), key=lambda p: -distance[p])
    by_arrival = [0] + far_first

    def spread(blocks, kind):
        for p in far_first:
            dx, dy = offsets[p]
            there = chips * ((cols - dy) % cols) + (chips - dx) % chips
            to = device(wrap_x(xpos + dx), 1, wrap_y(col + dy))
            remote(blocks.at[0], blocks.at[there], block_sent.at[kind], block_sem.at[kind, there], to).start()

    def arrived(blocks, kind, p):
        pltpu.make_async_copy(blocks.at[p], blocks.at[p], block_sem.at[kind, p]).wait()

    def all_sent(blocks, kind):
        sent = blocks.at[pl.ds(1, places - 1)]
        pltpu.make_async_copy(sent, sent, block_sent.at[kind]).wait()

    def wide(parts):
        return jnp.concatenate(parts, axis=1)

    def product(lhs_of, layer, gates, order, before=None):
        total = None
        for p in order:
            if before is not None and p:
                before(p)
            rhs = wide([weights[layer, p, g, s] for g in gates for s in range(HALVES)])
            lhs = wide([lhs_of(p, s) for s in range(HALVES)])
            term = jnp.dot(lhs, rhs, preferred_element_type=F32)
            total = term if total is None else total + term
        return total

    def gathered(blocks, kind, layer, gate):
        return product(lambda p, s: blocks[p, s], layer, (gate,), by_arrival, lambda p: arrived(blocks, kind, p))

    def project(layer, lhs_of, bias):
        total = product(lhs_of, layer, (RESET, UPDATE, CAND), range(places))
        for g in range(3):
            for s in range(HALVES):
                n = g * HALVES + s
                here = bias[pl.ds(g, 1), pl.ds(pl.multiple_of(xpos * chunk + s * half, half), half)]
                projections[layer, g, s] = total[:, n * half : (n + 1) * half] + here

    def reset_half(layer, blocks, kind, out_blocks, send):
        total = gathered(blocks, kind, layer, REC_RESET)
        for s in range(HALVES):
            reset = jax.nn.sigmoid(projections[layer, RESET, s] + total[:, s * half : (s + 1) * half])
            out_blocks[0, s] = (reset * states[layer, s]).astype(BF16)
        send()
        total = product(lambda p, s: blocks[p, s], layer, (REC_UPDATE,), range(places))
        for s in range(HALVES):
            updates[layer, s] = jax.nn.sigmoid(projections[layer, UPDATE, s] + total[:, s * half : (s + 1) * half])

    def next_half(layer, blocks, kind, emit):
        total = gathered(blocks, kind, layer, REC_CAND)
        for s in range(HALVES):
            candidate = jnp.tanh(projections[layer, CAND, s] + total[:, s * half : (s + 1) * half])
            update = updates[layer, s]
            state = (1.0 - update) * candidate + update * states[layer, s]
            emit(s, state.astype(BF16))
            states[layer, s] = state

    H1, R1, H2, R2 = range(4)

    def first_reset(t):
        slot = h1_blocks.at[lax.rem(t, 2)]
        reset_half(0, slot, H1, r1_blocks, lambda: spread(r1_blocks, R1))
        all_sent(slot, H1)

    def first_next(t):
        slot = h1_blocks.at[lax.rem(t + 1, 2)]

        def emit(s, value):
            slot[0, s] = value

        next_half(0, r1_blocks, R1, emit)
        all_sent(r1_blocks, R1)
        spread(slot, H1)

    def first_inputs(t):
        project(0, lambda p, s: xs[p, t, s], b1)

    def second_inputs(t):
        slot = h1_blocks.at[lax.rem(t, 2)]
        project(1, lambda p, s: slot[p, s], b2)

    def second_reset(t):
        slot = h2_blocks.at[lax.rem(t, 2)]
        reset_half(1, slot, H2, r2_blocks, lambda: spread(r2_blocks, R2))
        all_sent(slot, H2)

    def second_next(t, last):
        slot = h2_blocks.at[lax.rem(t + 1, 2)]

        def emit(s, value):
            seq_halves[s, t] = value
            if not last:
                slot[0, s] = value

        next_half(1, r2_blocks, R2, emit)
        all_sent(r2_blocks, R2)
        if not last:
            spread(slot, H2)

    @pl.when(core == 1)
    def _():
        for s in range(HALVES):
            part = state_in.at[:, s]
            pltpu.make_async_copy(part, part, state_sem.at[s]).wait()
        for layer in range(2):
            for s in range(HALVES):
                states[layer, s] = state_in[layer, s]
        for s in range(HALVES):
            h1_blocks[0, 0, s] = state_in[0, s].astype(BF16)
            h2_blocks[0, 0, s] = state_in[1, s].astype(BF16)
        spread(h1_blocks.at[0], H1)
        spread(h2_blocks.at[0], H2)
        for y in range(cols):
            part = xs.at[:, pl.ds(y * share, share)]
            pltpu.make_async_copy(part, part, xs_sem.at[y]).wait()
        for p in range(places):
            pltpu.make_async_copy(weights.at[0, p], weights.at[0, p], weight_sem.at[0, p]).wait()
        first_inputs(0)
        first_reset(0)
        first_next(0)
        first_inputs(jnp.minimum(1, steps - 1))
        for p in range(places):
            pltpu.make_async_copy(weights.at[1, p], weights.at[1, p], weight_sem.at[1, p]).wait()

        def step(t, carry):
            first_reset(t)
            second_inputs(t)
            second_reset(t - 1)
            first_next(t)
            second_next(t - 1, False)
            first_inputs(jnp.minimum(t + 1, steps - 1))
            return carry

        lax.fori_loop(1, steps, step, 0)
        last_slot = h1_blocks.at[steps % 2]
        for p in range(1, places):
            arrived(last_slot, H1, p)
        all_sent(last_slot, H1)
        second_inputs(steps)
        second_reset(steps - 1)
        second_next(steps - 1, True)
        for layer in range(2):
            for s in range(HALVES):
                last_halves[s, layer] = states[layer, s]
        seq_copy = remote(seq_halves.at[0], seq_out, out_sent.at[0], out_sem.at[0], device(xpos, 0, col))
        last_copy = remote(last_halves.at[0], last_out, out_sent.at[1], out_sem.at[1], device(xpos, 0, col))
        seq_copy.start()
        last_copy.start()
        seq_out[...] = seq_halves[1]
        last_out[...] = last_halves[1]
        seq_copy.wait_send()
        last_copy.wait_send()

    @pl.when(core == 0)
    def _():
        pltpu.make_async_copy(seq_out, seq_out, out_sem.at[0]).wait()
        pltpu.make_async_copy(last_out, last_out, out_sem.at[1]).wait()

    drain_sends()


def solution(mesh):
    rows, cols = mesh.shape["row"], mesh.shape["col"]
    chips = rows // CORES
    places = chips * cols

    def device_body(x_rows, h_rows, wx_l1, whru_l1, whn_l1, bias_l1, wx_l2, whru_l2, whn_l2, bias_l2):
        steps, batch, row_block = x_rows.shape
        col_block = wx_l1.shape[2]
        half = col_block // rows
        chunk = HALVES * half
        anywhere = pl.BlockSpec(memory_space=pl.ANY)
        vmem = pl.BlockSpec(memory_space=pltpu.VMEM)
        dma = pltpu.SemaphoreType.DMA
        kinds = 4
        block = (HALVES, batch, half)
        scratch = [
            pltpu.VMEM((2, places, GATES, HALVES, chunk, half), BF16),
            pltpu.VMEM((places, steps, *block), BF16),
            pltpu.VMEM((2, *block), F32),
            pltpu.VMEM((2, places, *block), BF16),
            pltpu.VMEM((places, *block), BF16),
            pltpu.VMEM((2, places, *block), BF16),
            pltpu.VMEM((places, *block), BF16),
            pltpu.VMEM((2, *block), F32),
            pltpu.VMEM((2, *block), F32),
            pltpu.VMEM((2, 3, *block), F32),
            pltpu.VMEM((HALVES, steps, batch, half), BF16),
            pltpu.VMEM((HALVES, 2, batch, half), F32),
            dma((2, places)),
            dma((chips, 2)),
            dma((places,)),
            dma((cols,)),
            dma((HALVES,)),
            dma((2, chips, 2)),
            dma((chips, 2)),
            dma((chips, 2)),
            dma((cols,)),
            dma((2, HALVES)),
            dma((kinds, places)),
            dma((kinds,)),
            dma((2,)),
            dma((2,)),
        ]
        return pl.pallas_call(
            functools.partial(gru_kernel, rows, cols),
            name="gru",
            out_shape=(
                jax.ShapeDtypeStruct((steps, batch, half), BF16),
                jax.ShapeDtypeStruct((2, batch, half), F32),
            ),
            in_specs=[anywhere, anywhere, anywhere, anywhere, anywhere, vmem, anywhere, anywhere, anywhere, vmem],
            out_specs=(vmem, vmem),
            scratch_shapes=scratch,
            compiler_params=pltpu.CompilerParams(
                collective_id=0, has_side_effects=True, vmem_limit_bytes=60 * 1024 * 1024
            ),
        )(
            x_rows, h_rows,
            jnp.transpose(wx_l1, (1, 0, 2)), jnp.transpose(whru_l1, (1, 0, 2)), whn_l1, bias_l1,
            jnp.transpose(wx_l2, (1, 0, 2)), jnp.transpose(whru_l2, (1, 0, 2)), whn_l2, bias_l2,
        )

    seq_spec = P(None, "data", "row")
    out_spec = P(None, "data", ("col", "row"))
    wide_spec = P("row", None, "col")
    square_spec = P("row", "col")
    bias_spec = P(None, "col")
    return jax.shard_map(
        device_body,
        mesh=mesh,
        in_specs=(seq_spec, seq_spec, wide_spec, wide_spec, square_spec, bias_spec, wide_spec, wide_spec, square_spec, bias_spec),
        out_specs=(out_spec, out_spec),
        check_vma=False,
    )
```

```python
import functools

import jax
import jax.numpy as jnp
from jax import lax
from jax.experimental import pallas as pl
from jax.experimental.pallas import tpu as pltpu
from jax.sharding import PartitionSpec as P

MESH = pl.DeviceIdType.MESH
F32 = jnp.float32
BF16 = jnp.bfloat16
HALVES = 2
CORES = 2
RESET, UPDATE, CAND, REC_RESET, REC_UPDATE, REC_CAND = range(6)
GATES = 6
EARLY = 2


def ring_distance(offset, count):
    return min(offset, count - offset)


def gru_kernel(
    rows, cols,
    x_ref, h_ref, wx1, wru1, wn1, b1, wx2, wru2, wn2, b2,
    seq_out, last_out,
    weights, x_here, first_made, first_parts, state_in,
    h1_blocks, r1_blocks, h2_blocks, r2_blocks,
    states, updates, projections, seq_halves, last_halves,
    weight_sem, hand_sem, x_sem, wide_sem, parts_sem, state_sem,
    weight_sent, handed_sent, x_sent, wide_sent, made_sent, state_sent,
    block_sem, block_sent, out_sem, out_sent,
):
    chips = rows // CORES
    steps, batch, half = seq_out.shape
    chunk = HALVES * half
    places = chips * cols
    row, col = lax.axis_index("row"), lax.axis_index("col")
    xpos, core = row // CORES, row % CORES
    layers = ((wx1, wru1, wn1), (wx2, wru2, wn2))

    def device(x, c, y):
        return {"row": CORES * x + c, "col": y}

    def wrap_x(v):
        return lax.rem(v + 2 * chips, chips)

    def wrap_y(v):
        return lax.rem(v + 2 * cols, cols)

    def place_of(x_from, y_from, x_to, y_to):
        return chips * wrap_y(y_from - y_to) + wrap_x(x_from - x_to)

    barrier = pltpu.get_barrier_semaphore()
    for k in range(1, rows * cols):
        other = {"row": lax.rem(row + k % rows, rows), "col": lax.rem(col + k // rows, cols)}
        pl.semaphore_signal(barrier, inc=1, device_id=other, device_id_type=MESH)
    pl.semaphore_wait(barrier, rows * cols - 1)

    def remote(src, dst, send, recv, to):
        return pltpu.make_async_remote_copy(
            src_ref=src, dst_ref=dst, send_sem=send, recv_sem=recv, device_id=to, device_id_type=MESH
        )

    def chunk_place(c, j, x_from, x_to, y_to):
        return place_of(HALVES * c + j, x_from, x_to, y_to)

    def input_pieces(layer, j, x_to, dst):
        depth = pl.ds(j * chunk, chunk)
        for s in range(HALVES):
            units = pl.ds(pl.multiple_of(x_to * chunk + s * half, half), half)
            yield layers[layer][0].at[:, depth, units], dst.at[pl.ds(0, 3), s]

    def recurrent_pieces(layer, j, x_to, dst):
        _, wru, wn = layers[layer]
        depth = pl.ds(j * chunk, chunk)
        for s in range(HALVES):
            units = pl.ds(pl.multiple_of(x_to * chunk + s * half, half), half)
            yield wru.at[:, depth, units], dst.at[pl.ds(3, 2), s]
            yield wn.at[depth, units], dst.at[5, s]

    def weight_pieces(layer, j, x_to, dst):
        if layer:
            yield from input_pieces(layer, j, x_to, dst)
        yield from recurrent_pieces(layer, j, x_to, dst)

    def moved(layer, index):
        return weights.at[1, index] if layer else weights.at[0, index, pl.ds(3, 3)]

    def send_weights(layer, turns):
        for turn in turns:
            x_to = wrap_x(xpos + turn)
            for j in range(2):
                place = chunk_place(core, j, xpos, x_to, col)
                for src, dst in weight_pieces(layer, j, x_to, weights.at[layer, place]):
                    remote(src, dst, weight_sent.at[layer, turn, j], weight_sem.at[layer, place], device(x_to, 1, col)).start()

    def keep_weights(layer):
        for j in range(2):
            place = chunk_place(1, j, xpos, xpos, col)
            for src, dst in weight_pieces(layer, j, xpos, weights.at[layer, place]):
                pltpu.make_async_copy(src, dst, weight_sem.at[layer, place]).start()

    def hand_over():
        for turn in far_turns:
            x_to = wrap_x(xpos + turn)
            for j in range(2):
                for src, dst in weight_pieces(1, j, x_to, weights.at[1, 2 * turn + j]):
                    remote(src, dst, weight_sent.at[1, turn, j], hand_sem.at[turn, j], device(xpos, 0, col)).start()

    def send_handed():
        for turn in far_turns:
            x_to = wrap_x(xpos + turn)
            for j in range(2):
                src = weights.at[1, 2 * turn + j]
                pltpu.make_async_copy(src, src, hand_sem.at[turn, j]).wait()
                place = chunk_place(1, j, xpos, x_to, col)
                remote(src, weights.at[1, place], handed_sent.at[turn, j], weight_sem.at[1, place], device(x_to, 1, col)).start()

    def input_copies():
        for j in range(2):
            n = 2 * core + j
            for s in range(HALVES):
                yield x_ref.at[:, :, pl.ds(j * chunk + s * half, half)], x_here.at[n, :, s], x_sent.at[j], x_sem.at[n]
            for turn in range(chips):
                kept = weights.at[0, 2 * CORES * turn + n]
                for src, dst in input_pieces(0, j, wrap_x(xpos + turn), kept):
                    yield src, dst, wide_sent.at[turn, j], wide_sem.at[turn, n]

    def keep_inputs():
        for src, dst, _, sem in input_copies():
            pltpu.make_async_copy(src, dst, sem).start()

    def hand_inputs():
        for src, dst, sent, sem in input_copies():
            remote(src, dst, sent, sem, device(xpos, 0, col)).start()

    def inputs_here():
        for n in range(2 * CORES):
            pltpu.make_async_copy(x_here.at[n], x_here.at[n], x_sem.at[n]).wait()
            for turn in range(chips):
                kept = weights.at[0, 2 * CORES * turn + n, pl.ds(0, 3)]
                pltpu.make_async_copy(kept, kept, wide_sem.at[turn, n]).wait()

    def wide(parts):
        return jnp.concatenate(parts, axis=1)

    def make_first(t, again):
        slot = lax.rem(t, 2)
        for turn in (2, 1, chips - 1, 0):
            made = first_made.at[slot, turn]
            if again:
                pltpu.make_async_copy(made, made, made_sent.at[slot, turn]).wait()
            total = None
            for n in range(2 * CORES):
                rhs = wide([weights[0, 2 * CORES * turn + n, g, s] for g in range(3) for s in range(HALVES)])
                lhs = wide([x_here[n, t, s] for s in range(HALVES)])
                term = jnp.dot(lhs, rhs, preferred_element_type=F32)
                total = term if total is None else total + term
            for g in range(3):
                for s in range(HALVES):
                    n = g * HALVES + s
                    made[g, s] = total[:, n * half : (n + 1) * half]
            seen = (chips - turn) % chips
            to = device(wrap_x(xpos + turn), 1, col)
            remote(made, first_parts.at[t, seen], made_sent.at[slot, turn], parts_sem.at[t, seen], to).start()

    far_turns = (2, 1, chips - 1)

    @pl.when(xpos == col)
    def _():
        for j in range(2):
            x_to = HALVES * core + j
            for s in range(HALVES):
                src = h_ref.at[:, :, pl.ds(j * chunk + s * half, half)]
                dst = state_in.at[:, s]
                mine = (x_to == xpos) & (core == 1)

                @pl.when(mine)
                def _():
                    pltpu.make_async_copy(src, dst, state_sem.at[s]).start()

                @pl.when(jnp.logical_not(mine))
                def _():
                    copy = remote(src, dst, state_sent.at[j, s], state_sem.at[s], device(x_to, 1, col))
                    copy.start()
                    copy.wait_send()

    send_weights(0, far_turns)

    @pl.when(core == 1)
    def _():
        hand_inputs()
        keep_weights(0)
        hand_over()
        keep_weights(1)

    @pl.when(core == 0)
    def _():
        keep_inputs()
        send_weights(0, (0,))
        inputs_here()
        for t in range(EARLY):
            make_first(t, False)
        send_weights(1, far_turns)
        send_weights(1, (0,))
        send_handed()

    def drain_sends():
        for layer in range(2):
            piece = moved(layer, 0)
            for j in range(2):
                for turn in far_turns:
                    pltpu.make_async_copy(piece, piece, weight_sent.at[layer, turn, j]).wait()

                @pl.when(core == 0)
                def _():
                    pltpu.make_async_copy(piece, piece, weight_sent.at[layer, 0, j]).wait()

        @pl.when(core == 0)
        def _():
            piece = moved(1, 0)
            for j in range(2):
                for turn in far_turns:
                    pltpu.make_async_copy(piece, piece, handed_sent.at[turn, j]).wait()
            for slot in range(2):
                for turn in range(chips):
                    made = first_made.at[slot, turn]
                    pltpu.make_async_copy(made, made, made_sent.at[slot, turn]).wait()

        @pl.when(core == 1)
        def _():
            piece = weights.at[0, 0, pl.ds(0, 3)]
            for j in range(2):
                pltpu.make_async_copy(x_here.at[0], x_here.at[0], x_sent.at[j]).wait()
                for turn in range(chips):
                    pltpu.make_async_copy(piece, piece, wide_sent.at[turn, j]).wait()

    offsets = [(dx, dy) for dy in range(cols) for dx in range(chips)]
    distance = [ring_distance(dx, chips) + ring_distance(dy, cols) for dx, dy in offsets]
    far_first = sorted(range(1, places), key=lambda p: -distance[p])
    by_arrival = sorted(range(places), key=lambda p: (distance[p], ring_distance(offsets[p][0], chips)))

    def spread(blocks, kind):
        for p in far_first:
            dx, dy = offsets[p]
            there = chips * ((cols - dy) % cols) + (chips - dx) % chips
            to = device(wrap_x(xpos + dx), 1, wrap_y(col + dy))
            remote(blocks.at[0], blocks.at[there], block_sent.at[kind], block_sem.at[kind, there], to).start()

    def arrived(blocks, kind, p):
        pltpu.make_async_copy(blocks.at[p], blocks.at[p], block_sem.at[kind, p]).wait()

    def all_sent(blocks, kind):
        sent = blocks.at[pl.ds(1, places - 1)]
        pltpu.make_async_copy(sent, sent, block_sent.at[kind]).wait()

    def product(lhs_of, layer, gates, order, before=None):
        total = None
        for p in order:
            if before is not None and p:
                before(p)
            rhs = wide([weights[layer, p, g, s] for g in gates for s in range(HALVES)])
            lhs = wide([lhs_of(p, s) for s in range(HALVES)])
            term = jnp.dot(lhs, rhs, preferred_element_type=F32)
            total = term if total is None else total + term
        return total

    def gathered(blocks, kind, layer, gate):
        return product(lambda p, s: blocks[p, s], layer, (gate,), by_arrival, lambda p: arrived(blocks, kind, p))

    def project(layer, lhs_of, bias):
        total = product(lhs_of, layer, (RESET, UPDATE, CAND), range(places))
        for g in range(3):
            for s in range(HALVES):
                n = g * HALVES + s
                here = bias[pl.ds(g, 1), pl.ds(pl.multiple_of(xpos * chunk + s * half, half), half)]
                projections[layer, g, s] = total[:, n * half : (n + 1) * half] + here

    def reset_half(layer, blocks, kind, out_blocks, send):
        total = gathered(blocks, kind, layer, REC_RESET)
        for s in range(HALVES):
            reset = jax.nn.sigmoid(projections[layer, RESET, s] + total[:, s * half : (s + 1) * half])
            out_blocks[0, s] = (reset * states[layer, s]).astype(BF16)
        send()
        total = product(lambda p, s: blocks[p, s], layer, (REC_UPDATE,), range(places))
        for s in range(HALVES):
            updates[layer, s] = jax.nn.sigmoid(projections[layer, UPDATE, s] + total[:, s * half : (s + 1) * half])

    def next_half(layer, blocks, kind, emit):
        total = gathered(blocks, kind, layer, REC_CAND)
        for s in range(HALVES):
            candidate = jnp.tanh(projections[layer, CAND, s] + total[:, s * half : (s + 1) * half])
            update = updates[layer, s]
            state = (1.0 - update) * candidate + update * states[layer, s]
            emit(s, state.astype(BF16))
            states[layer, s] = state

    H1, R1, H2, R2 = range(4)

    def first_reset(t):
        slot = h1_blocks.at[lax.rem(t, 2)]
        reset_half(0, slot, H1, r1_blocks, lambda: spread(r1_blocks, R1))
        all_sent(slot, H1)

    def first_next(t):
        slot = h1_blocks.at[lax.rem(t + 1, 2)]

        def emit(s, value):
            slot[0, s] = value

        next_half(0, r1_blocks, R1, emit)
        all_sent(r1_blocks, R1)
        spread(slot, H1)

    def first_inputs(t):
        for n in range(chips):
            part = first_parts.at[t, n]
            pltpu.make_async_copy(part, part, parts_sem.at[t, n]).wait()
        for g in range(3):
            for s in range(HALVES):
                here = b1[pl.ds(g, 1), pl.ds(pl.multiple_of(xpos * chunk + s * half, half), half)]
                projections[0, g, s] = sum(first_parts[t, n, g, s] for n in range(chips)) + here

    def second_inputs(t):
        slot = h1_blocks.at[lax.rem(t, 2)]
        project(1, lambda p, s: slot[p, s], b2)

    def second_reset(t):
        slot = h2_blocks.at[lax.rem(t, 2)]
        reset_half(1, slot, H2, r2_blocks, lambda: spread(r2_blocks, R2))
        all_sent(slot, H2)

    def second_next(t, last):
        slot = h2_blocks.at[lax.rem(t + 1, 2)]

        def emit(s, value):
            seq_halves[s, t] = value
            if not last:
                slot[0, s] = value

        next_half(1, r2_blocks, R2, emit)
        all_sent(r2_blocks, R2)
        if not last:
            spread(slot, H2)

    @pl.when(core == 1)
    def _():
        for s in range(HALVES):
            part = state_in.at[:, s]
            pltpu.make_async_copy(part, part, state_sem.at[s]).wait()
        for layer in range(2):
            for s in range(HALVES):
                states[layer, s] = state_in[layer, s]
        for s in range(HALVES):
            h1_blocks[0, 0, s] = state_in[0, s].astype(BF16)
            h2_blocks[0, 0, s] = state_in[1, s].astype(BF16)
        spread(h1_blocks.at[0], H1)
        spread(h2_blocks.at[0], H2)
        for p in range(places):
            pltpu.make_async_copy(moved(0, p), moved(0, p), weight_sem.at[0, p]).wait()
        first_inputs(0)
        first_reset(0)
        first_next(0)
        first_inputs(1)
        for p in range(places):
            pltpu.make_async_copy(weights.at[1, p], weights.at[1, p], weight_sem.at[1, p]).wait()

        def step(t, carry):
            first_reset(t)
            second_inputs(t)
            second_reset(t - 1)
            first_next(t)
            second_next(t - 1, False)
            pl.when(t + 1 < steps)(lambda: first_inputs(t + 1))
            return carry

        lax.fori_loop(1, steps, step, 0)
        last_slot = h1_blocks.at[steps % 2]
        for p in range(1, places):
            arrived(last_slot, H1, p)
        all_sent(last_slot, H1)
        second_inputs(steps)
        second_reset(steps - 1)
        second_next(steps - 1, True)
        for layer in range(2):
            for s in range(HALVES):
                last_halves[s, layer] = states[layer, s]
        seq_copy = remote(seq_halves.at[0], seq_out, out_sent.at[0], out_sem.at[0], device(xpos, 0, col))
        last_copy = remote(last_halves.at[0], last_out, out_sent.at[1], out_sem.at[1], device(xpos, 0, col))
        seq_copy.start()
        last_copy.start()
        seq_out[...] = seq_halves[1]
        last_out[...] = last_halves[1]
        seq_copy.wait_send()
        last_copy.wait_send()

    @pl.when(core == 0)
    def _():
        def later_first(t, carry):
            make_first(t, True)
            return carry

        lax.fori_loop(EARLY, steps, later_first, 0)
        pltpu.make_async_copy(seq_out, seq_out, out_sem.at[0]).wait()
        pltpu.make_async_copy(last_out, last_out, out_sem.at[1]).wait()

    drain_sends()


def solution(mesh):
    rows, cols = mesh.shape["row"], mesh.shape["col"]
    chips = rows // CORES
    places = chips * cols

    def device_body(x_rows, h_rows, wx_l1, whru_l1, whn_l1, bias_l1, wx_l2, whru_l2, whn_l2, bias_l2):
        steps, batch, row_block = x_rows.shape
        col_block = wx_l1.shape[2]
        half = col_block // rows
        chunk = HALVES * half
        anywhere = pl.BlockSpec(memory_space=pl.ANY)
        vmem = pl.BlockSpec(memory_space=pltpu.VMEM)
        dma = pltpu.SemaphoreType.DMA
        kinds = 4
        block = (HALVES, batch, half)
        scratch = [
            pltpu.VMEM((2, places, GATES, HALVES, chunk, half), BF16),
            pltpu.VMEM((2 * CORES, steps, *block), BF16),
            pltpu.VMEM((2, chips, 3, *block), F32),
            pltpu.VMEM((steps, chips, 3, *block), F32),
            pltpu.VMEM((2, *block), F32),
            pltpu.VMEM((2, places, *block), BF16),
            pltpu.VMEM((places, *block), BF16),
            pltpu.VMEM((2, places, *block), BF16),
            pltpu.VMEM((places, *block), BF16),
            pltpu.VMEM((2, *block), F32),
            pltpu.VMEM((2, *block), F32),
            pltpu.VMEM((2, 3, *block), F32),
            pltpu.VMEM((HALVES, steps, batch, half), BF16),
            pltpu.VMEM((HALVES, 2, batch, half), F32),
            dma((2, places)),
            dma((chips, 2)),
            dma((2 * CORES,)),
            dma((chips, 2 * CORES)),
            dma((steps, chips)),
            dma((HALVES,)),
            dma((2, chips, 2)),
            dma((chips, 2)),
            dma((2,)),
            dma((chips, 2)),
            dma((2, chips)),
            dma((2, HALVES)),
            dma((kinds, places)),
            dma((kinds,)),
            dma((2,)),
            dma((2,)),
        ]
        return pl.pallas_call(
            functools.partial(gru_kernel, rows, cols),
            name="gru",
            out_shape=(
                jax.ShapeDtypeStruct((steps, batch, half), BF16),
                jax.ShapeDtypeStruct((2, batch, half), F32),
            ),
            in_specs=[anywhere, anywhere, anywhere, anywhere, anywhere, vmem, anywhere, anywhere, anywhere, vmem],
            out_specs=(vmem, vmem),
            scratch_shapes=scratch,
            compiler_params=pltpu.CompilerParams(
                collective_id=0, has_side_effects=True, vmem_limit_bytes=60 * 1024 * 1024
            ),
        )(
            x_rows, h_rows,
            jnp.transpose(wx_l1, (1, 0, 2)), jnp.transpose(whru_l1, (1, 0, 2)), whn_l1, bias_l1,
            jnp.transpose(wx_l2, (1, 0, 2)), jnp.transpose(whru_l2, (1, 0, 2)), whn_l2, bias_l2,
        )

    seq_spec = P(None, "data", "row")
    out_spec = P(None, "data", ("col", "row"))
    wide_spec = P("row", None, "col")
    square_spec = P("row", "col")
    bias_spec = P(None, "col")
    return jax.shard_map(
        device_body,
        mesh=mesh,
        in_specs=(seq_spec, seq_spec, wide_spec, wide_spec, square_spec, bias_spec, wide_spec, wide_spec, square_spec, bias_spec),
        out_specs=(out_spec, out_spec),
        check_vma=False,
    )
```

```python
import functools

import jax
import jax.numpy as jnp
from jax import lax
from jax.experimental import pallas as pl
from jax.experimental.pallas import tpu as pltpu
from jax.sharding import PartitionSpec as P

MESH = pl.DeviceIdType.MESH
F32 = jnp.float32
BF16 = jnp.bfloat16
HALVES = 2
CORES = 2
RESET, UPDATE, CAND, REC_RESET, REC_UPDATE, REC_CAND = range(6)
GATES = 6
EARLY = 2


def ring_distance(offset, count):
    return min(offset, count - offset)


def gru_kernel(
    rows, cols,
    x_ref, h_ref, wx1, wru1, wn1, b1, wx2, wru2, wn2, b2,
    seq_out, last_out,
    weights, x_here, h1_here, first_made, first_parts, second_made, second_parts, state_in,
    h1_blocks, r1_blocks, h2_blocks, r2_blocks,
    states, updates, projections, seq_halves, last_halves,
    weight_sem, hand_sem, x_sem, wide_sem, parts_sem, second_sem, h1_sem, state_sem,
    weight_sent, handed_sent, x_sent, wide_sent, made_sent, second_sent, h1_sent, state_sent,
    block_sem, block_sent, out_sem, out_sent,
):
    chips = rows // CORES
    steps, batch, half = seq_out.shape
    chunk = HALVES * half
    places = chips * cols
    row, col = lax.axis_index("row"), lax.axis_index("col")
    xpos, core = row // CORES, row % CORES
    layers = ((wx1, wru1, wn1), (wx2, wru2, wn2))

    def device(x, c, y):
        return {"row": CORES * x + c, "col": y}

    def wrap_x(v):
        return lax.rem(v + 2 * chips, chips)

    def wrap_y(v):
        return lax.rem(v + 2 * cols, cols)

    def place_of(x_from, y_from, x_to, y_to):
        return chips * wrap_y(y_from - y_to) + wrap_x(x_from - x_to)

    barrier = pltpu.get_barrier_semaphore()
    for k in range(1, rows * cols):
        other = {"row": lax.rem(row + k % rows, rows), "col": lax.rem(col + k // rows, cols)}
        pl.semaphore_signal(barrier, inc=1, device_id=other, device_id_type=MESH)
    pl.semaphore_wait(barrier, rows * cols - 1)

    def remote(src, dst, send, recv, to):
        return pltpu.make_async_remote_copy(
            src_ref=src, dst_ref=dst, send_sem=send, recv_sem=recv, device_id=to, device_id_type=MESH
        )

    def chunk_place(c, j, x_from, x_to, y_to):
        return place_of(HALVES * c + j, x_from, x_to, y_to)

    def input_pieces(layer, j, x_to, dst):
        depth = pl.ds(j * chunk, chunk)
        for s in range(HALVES):
            units = pl.ds(pl.multiple_of(x_to * chunk + s * half, half), half)
            yield layers[layer][0].at[:, depth, units], dst.at[pl.ds(0, 3), s]

    def recurrent_pieces(layer, j, x_to, dst):
        _, wru, wn = layers[layer]
        depth = pl.ds(j * chunk, chunk)
        for s in range(HALVES):
            units = pl.ds(pl.multiple_of(x_to * chunk + s * half, half), half)
            yield wru.at[:, depth, units], dst.at[pl.ds(3, 2), s]
            yield wn.at[depth, units], dst.at[5, s]

    def moved(layer, index):
        return weights.at[layer, index, pl.ds(3, 3)]

    def send_weights(layer, turns):
        for turn in turns:
            x_to = wrap_x(xpos + turn)
            for j in range(2):
                place = chunk_place(core, j, xpos, x_to, col)
                for src, dst in recurrent_pieces(layer, j, x_to, weights.at[layer, place]):
                    remote(src, dst, weight_sent.at[layer, turn, j], weight_sem.at[layer, place], device(x_to, 1, col)).start()

    def keep_weights(layer):
        for j in range(2):
            place = chunk_place(1, j, xpos, xpos, col)
            for src, dst in recurrent_pieces(layer, j, xpos, weights.at[layer, place]):
                pltpu.make_async_copy(src, dst, weight_sem.at[layer, place]).start()

    def hand_over():
        for turn in far_turns:
            x_to = wrap_x(xpos + turn)
            for j in range(2):
                for src, dst in recurrent_pieces(1, j, x_to, weights.at[1, 2 * turn + j]):
                    remote(src, dst, weight_sent.at[1, turn, j], hand_sem.at[turn, j], device(xpos, 0, col)).start()

    def send_handed():
        for turn in far_turns:
            x_to = wrap_x(xpos + turn)
            for j in range(2):
                src = moved(1, 2 * turn + j)
                pltpu.make_async_copy(src, src, hand_sem.at[turn, j]).wait()
                place = chunk_place(1, j, xpos, x_to, col)
                remote(src, moved(1, place), handed_sent.at[turn, j], weight_sem.at[1, place], device(x_to, 1, col)).start()

    def x_copies():
        for j in range(2):
            n = 2 * core + j
            for s in range(HALVES):
                yield x_ref.at[:, :, pl.ds(j * chunk + s * half, half)], x_here.at[n, :, s], x_sent.at[j], x_sem.at[n]

    def input_copies(layer):
        for turn in range(chips):
            for j in range(2):
                n = 2 * core + j
                for src, dst in input_pieces(layer, j, wrap_x(xpos + turn), weights.at[layer, 2 * CORES * turn + n]):
                    yield src, dst, wide_sent.at[layer, turn, j], wide_sem.at[layer, turn, n]

    def keep(copies):
        for src, dst, _, sem in copies:
            pltpu.make_async_copy(src, dst, sem).start()

    def hand(copies):
        for src, dst, sent, sem in copies:
            remote(src, dst, sent, sem, device(xpos, 0, col)).start()

    def x_arrived():
        for n in range(2 * CORES):
            pltpu.make_async_copy(x_here.at[n], x_here.at[n], x_sem.at[n]).wait()

    def inputs_arrived(layer):
        for turn in range(chips):
            for n in range(2 * CORES):
                kept = weights.at[layer, 2 * CORES * turn + n, pl.ds(0, 3)]
                pltpu.make_async_copy(kept, kept, wide_sem.at[layer, turn, n]).wait()

    def wide(parts):
        return jnp.concatenate(parts, axis=1)

    def make(layer, lhs_of, made, sent, parts, sem, again):
        for turn in (2, 1, chips - 1, 0):
            if again:
                pltpu.make_async_copy(made.at[turn], made.at[turn], sent.at[turn]).wait()
            total = None
            for n in range(2 * CORES):
                rhs = wide([weights[layer, 2 * CORES * turn + n, g, s] for g in range(3) for s in range(HALVES)])
                lhs = wide([lhs_of(n, s) for s in range(HALVES)])
                term = jnp.dot(lhs, rhs, preferred_element_type=F32)
                total = term if total is None else total + term
            for g in range(3):
                for s in range(HALVES):
                    n = g * HALVES + s
                    made[turn, g, s] = total[:, n * half : (n + 1) * half]
            seen = (chips - turn) % chips
            remote(made.at[turn], parts.at[seen], sent.at[turn], sem.at[seen], device(wrap_x(xpos + turn), 1, col)).start()

    def make_first(t, again):
        slot = lax.rem(t, 2)
        make(0, lambda n, s: x_here[n, t, s], first_made.at[slot], made_sent.at[slot], first_parts.at[t], parts_sem.at[t], again)

    def make_second(t, again):
        slot = lax.rem(t, 2)
        pltpu.make_async_copy(h1_here, h1_here, h1_sem).wait()
        make(1, lambda n, s: h1_here[wrap_x(n - xpos), s], second_made, second_sent, second_parts.at[slot], second_sem.at[slot], again)

    far_turns = (2, 1, chips - 1)

    @pl.when(xpos == col)
    def _():
        for j in range(2):
            x_to = HALVES * core + j
            for s in range(HALVES):
                src = h_ref.at[:, :, pl.ds(j * chunk + s * half, half)]
                dst = state_in.at[:, s]
                mine = (x_to == xpos) & (core == 1)

                @pl.when(mine)
                def _():
                    pltpu.make_async_copy(src, dst, state_sem.at[s]).start()

                @pl.when(jnp.logical_not(mine))
                def _():
                    copy = remote(src, dst, state_sent.at[j, s], state_sem.at[s], device(x_to, 1, col))
                    copy.start()
                    copy.wait_send()

    send_weights(0, far_turns)

    @pl.when(core == 1)
    def _():
        hand(x_copies())
        hand(input_copies(0))
        keep_weights(0)
        hand_over()
        hand(input_copies(1))
        keep_weights(1)

    @pl.when(core == 0)
    def _():
        keep(x_copies())
        keep(input_copies(0))
        send_weights(0, (0,))
        x_arrived()
        inputs_arrived(0)
        for t in range(EARLY):
            make_first(t, False)
        send_weights(1, far_turns)
        send_weights(1, (0,))
        keep(input_copies(1))
        send_handed()

    def drain_sends():
        piece = moved(0, 0)
        for layer in range(2):
            for j in range(2):
                for turn in far_turns:
                    pltpu.make_async_copy(piece, piece, weight_sent.at[layer, turn, j]).wait()

                @pl.when(core == 0)
                def _():
                    pltpu.make_async_copy(piece, piece, weight_sent.at[layer, 0, j]).wait()

        @pl.when(core == 0)
        def _():
            for j in range(2):
                for turn in far_turns:
                    pltpu.make_async_copy(piece, piece, handed_sent.at[turn, j]).wait()
            for turn in range(chips):
                made = second_made.at[turn]
                pltpu.make_async_copy(made, made, second_sent.at[turn]).wait()
                for slot in range(2):
                    pltpu.make_async_copy(made, made, made_sent.at[slot, turn]).wait()

        @pl.when(core == 1)
        def _():
            for j in range(2):
                pltpu.make_async_copy(x_here.at[0], x_here.at[0], x_sent.at[j]).wait()
                for layer in range(2):
                    for turn in range(chips):
                        pltpu.make_async_copy(piece, piece, wide_sent.at[layer, turn, j]).wait()

    offsets = [(dx, dy) for dy in range(cols) for dx in range(chips)]
    distance = [ring_distance(dx, chips) + ring_distance(dy, cols) for dx, dy in offsets]
    far_first = sorted(range(1, places), key=lambda p: -distance[p])
    by_arrival = sorted(range(places), key=lambda p: (distance[p], ring_distance(offsets[p][0], chips)))

    def spread(blocks, kind):
        for p in far_first:
            dx, dy = offsets[p]
            there = chips * ((cols - dy) % cols) + (chips - dx) % chips
            to = device(wrap_x(xpos + dx), 1, wrap_y(col + dy))
            remote(blocks.at[0], blocks.at[there], block_sent.at[kind], block_sem.at[kind, there], to).start()

    def arrived(blocks, kind, p):
        pltpu.make_async_copy(blocks.at[p], blocks.at[p], block_sem.at[kind, p]).wait()

    def all_sent(blocks, kind):
        sent = blocks.at[pl.ds(1, places - 1)]
        pltpu.make_async_copy(sent, sent, block_sent.at[kind]).wait()

    def product(lhs_of, layer, gates, order, before=None):
        total = None
        for p in order:
            if before is not None and p:
                before(p)
            rhs = wide([weights[layer, p, g, s] for g in gates for s in range(HALVES)])
            lhs = wide([lhs_of(p, s) for s in range(HALVES)])
            term = jnp.dot(lhs, rhs, preferred_element_type=F32)
            total = term if total is None else total + term
        return total

    def gathered(blocks, kind, layer, gate):
        return product(lambda p, s: blocks[p, s], layer, (gate,), by_arrival, lambda p: arrived(blocks, kind, p))

    def add_parts(layer, parts, sem, bias):
        for n in range(chips):
            pltpu.make_async_copy(parts.at[n], parts.at[n], sem.at[n]).wait()
        for g in range(3):
            for s in range(HALVES):
                here = bias[pl.ds(g, 1), pl.ds(pl.multiple_of(xpos * chunk + s * half, half), half)]
                projections[layer, g, s] = sum(parts[n, g, s] for n in range(chips)) + here

    def reset_half(layer, blocks, kind, out_blocks, send):
        total = gathered(blocks, kind, layer, REC_RESET)
        for s in range(HALVES):
            reset = jax.nn.sigmoid(projections[layer, RESET, s] + total[:, s * half : (s + 1) * half])
            out_blocks[0, s] = (reset * states[layer, s]).astype(BF16)
        send()
        total = product(lambda p, s: blocks[p, s], layer, (REC_UPDATE,), range(places))
        for s in range(HALVES):
            updates[layer, s] = jax.nn.sigmoid(projections[layer, UPDATE, s] + total[:, s * half : (s + 1) * half])

    def next_half(layer, blocks, kind, emit):
        total = gathered(blocks, kind, layer, REC_CAND)
        for s in range(HALVES):
            candidate = jnp.tanh(projections[layer, CAND, s] + total[:, s * half : (s + 1) * half])
            update = updates[layer, s]
            state = (1.0 - update) * candidate + update * states[layer, s]
            emit(s, state.astype(BF16))
            states[layer, s] = state

    H1, R1, H2, R2 = range(4)

    def hand_state(slot):
        four = slot.at[pl.ds(chips * wrap_y(xpos - col), chips)]
        return remote(four, h1_here, h1_sent, h1_sem, device(xpos, 0, col))

    def first_reset(t, handed):
        slot = h1_blocks.at[lax.rem(t, 2)]

        def send():
            spread(r1_blocks, R1)
            if handed:
                hand_state(slot).start()

        reset_half(0, slot, H1, r1_blocks, send)
        all_sent(slot, H1)

    def first_next(t):
        slot = h1_blocks.at[lax.rem(t + 1, 2)]

        def emit(s, value):
            slot[0, s] = value

        next_half(0, r1_blocks, R1, emit)
        all_sent(r1_blocks, R1)
        spread(slot, H1)

    def first_inputs(t):
        add_parts(0, first_parts.at[t], parts_sem.at[t], b1)

    def second_inputs(t):
        hand_state(h1_blocks.at[lax.rem(t + 1, 2)]).wait_send()
        slot = lax.rem(t, 2)
        add_parts(1, second_parts.at[slot], second_sem.at[slot], b2)

    def second_reset(t):
        slot = h2_blocks.at[lax.rem(t, 2)]
        reset_half(1, slot, H2, r2_blocks, lambda: spread(r2_blocks, R2))
        all_sent(slot, H2)

    def second_next(t, last):
        slot = h2_blocks.at[lax.rem(t + 1, 2)]

        def emit(s, value):
            seq_halves[s, t] = value
            if not last:
                slot[0, s] = value

        next_half(1, r2_blocks, R2, emit)
        all_sent(r2_blocks, R2)
        if not last:
            spread(slot, H2)

    @pl.when(core == 1)
    def _():
        for s in range(HALVES):
            part = state_in.at[:, s]
            pltpu.make_async_copy(part, part, state_sem.at[s]).wait()
        for layer in range(2):
            for s in range(HALVES):
                states[layer, s] = state_in[layer, s]
        for s in range(HALVES):
            h1_blocks[0, 0, s] = state_in[0, s].astype(BF16)
            h2_blocks[0, 0, s] = state_in[1, s].astype(BF16)
        spread(h1_blocks.at[0], H1)
        spread(h2_blocks.at[0], H2)
        for p in range(places):
            pltpu.make_async_copy(moved(0, p), moved(0, p), weight_sem.at[0, p]).wait()
        first_inputs(0)
        first_reset(0, False)
        first_next(0)
        first_inputs(1)
        first_reset(1, True)
        first_next(1)
        for p in range(places):
            pltpu.make_async_copy(moved(1, p), moved(1, p), weight_sem.at[1, p]).wait()
        second_inputs(0)
        second_reset(0)
        first_inputs(2)

        def step(t, carry):
            first_reset(t, True)
            second_next(t - 2, False)
            first_next(t)
            second_inputs(t - 1)
            second_reset(t - 1)
            pl.when(t + 1 < steps)(lambda: first_inputs(t + 1))
            return carry

        lax.fori_loop(2, steps, step, 0)
        last_slot = h1_blocks.at[steps % 2]
        for p in range(1, places):
            arrived(last_slot, H1, p)
        hand_state(last_slot).start()
        all_sent(last_slot, H1)
        second_next(steps - 2, False)
        second_inputs(steps - 1)
        second_reset(steps - 1)
        second_next(steps - 1, True)
        for layer in range(2):
            for s in range(HALVES):
                last_halves[s, layer] = states[layer, s]
        seq_copy = remote(seq_halves.at[0], seq_out, out_sent.at[0], out_sem.at[0], device(xpos, 0, col))
        last_copy = remote(last_halves.at[0], last_out, out_sent.at[1], out_sem.at[1], device(xpos, 0, col))
        seq_copy.start()
        last_copy.start()
        seq_out[...] = seq_halves[1]
        last_out[...] = last_halves[1]
        seq_copy.wait_send()
        last_copy.wait_send()

    @pl.when(core == 0)
    def _():
        inputs_arrived(1)
        make_first(EARLY, True)
        make_second(0, False)
        make_first(EARLY + 1, True)

        def later(t, carry):
            make_second(t, True)
            pl.when(t + EARLY + 1 < steps)(lambda: make_first(t + EARLY + 1, True))
            return carry

        lax.fori_loop(1, steps, later, 0)
        pltpu.make_async_copy(seq_out, seq_out, out_sem.at[0]).wait()
        pltpu.make_async_copy(last_out, last_out, out_sem.at[1]).wait()

    drain_sends()


def solution(mesh):
    rows, cols = mesh.shape["row"], mesh.shape["col"]
    chips = rows // CORES
    places = chips * cols

    def device_body(x_rows, h_rows, wx_l1, whru_l1, whn_l1, bias_l1, wx_l2, whru_l2, whn_l2, bias_l2):
        steps, batch, row_block = x_rows.shape
        col_block = wx_l1.shape[2]
        half = col_block // rows
        chunk = HALVES * half
        anywhere = pl.BlockSpec(memory_space=pl.ANY)
        vmem = pl.BlockSpec(memory_space=pltpu.VMEM)
        dma = pltpu.SemaphoreType.DMA
        kinds = 4
        block = (HALVES, batch, half)
        scratch = [
            pltpu.VMEM((2, places, GATES, HALVES, chunk, half), BF16),
            pltpu.VMEM((2 * CORES, steps, *block), BF16),
            pltpu.VMEM((chips, *block), BF16),
            pltpu.VMEM((2, chips, 3, *block), F32),
            pltpu.VMEM((steps, chips, 3, *block), F32),
            pltpu.VMEM((chips, 3, *block), F32),
            pltpu.VMEM((2, chips, 3, *block), F32),
            pltpu.VMEM((2, *block), F32),
            pltpu.VMEM((2, places, *block), BF16),
            pltpu.VMEM((places, *block), BF16),
            pltpu.VMEM((2, places, *block), BF16),
            pltpu.VMEM((places, *block), BF16),
            pltpu.VMEM((2, *block), F32),
            pltpu.VMEM((2, *block), F32),
            pltpu.VMEM((2, 3, *block), F32),
            pltpu.VMEM((HALVES, steps, batch, half), BF16),
            pltpu.VMEM((HALVES, 2, batch, half), F32),
            dma((2, places)),
            dma((chips, 2)),
            dma((2 * CORES,)),
            dma((2, chips, 2 * CORES)),
            dma((steps, chips)),
            dma((2, chips)),
            dma,
            dma((HALVES,)),
            dma((2, chips, 2)),
            dma((chips, 2)),
            dma((2,)),
            dma((2, chips, 2)),
            dma((2, chips)),
            dma((chips,)),
            dma,
            dma((2, HALVES)),
            dma((kinds, places)),
            dma((kinds,)),
            dma((2,)),
            dma((2,)),
        ]
        return pl.pallas_call(
            functools.partial(gru_kernel, rows, cols),
            name="gru",
            out_shape=(
                jax.ShapeDtypeStruct((steps, batch, half), BF16),
                jax.ShapeDtypeStruct((2, batch, half), F32),
            ),
            in_specs=[anywhere, anywhere, anywhere, anywhere, anywhere, vmem, anywhere, anywhere, anywhere, vmem],
            out_specs=(vmem, vmem),
            scratch_shapes=scratch,
            compiler_params=pltpu.CompilerParams(
                collective_id=0, has_side_effects=True, vmem_limit_bytes=60 * 1024 * 1024
            ),
        )(
            x_rows, h_rows,
            jnp.transpose(wx_l1, (1, 0, 2)), jnp.transpose(whru_l1, (1, 0, 2)), whn_l1, bias_l1,
            jnp.transpose(wx_l2, (1, 0, 2)), jnp.transpose(whru_l2, (1, 0, 2)), whn_l2, bias_l2,
        )

    seq_spec = P(None, "data", "row")
    out_spec = P(None, "data", ("col", "row"))
    wide_spec = P("row", None, "col")
    square_spec = P("row", "col")
    bias_spec = P(None, "col")
    return jax.shard_map(
        device_body,
        mesh=mesh,
        in_specs=(seq_spec, seq_spec, wide_spec, wide_spec, square_spec, bias_spec, wide_spec, wide_spec, square_spec, bias_spec),
        out_specs=(out_spec, out_spec),
        check_vma=False,
    )
```

```python
import functools

import jax
import jax.numpy as jnp
from jax import lax
from jax.experimental import pallas as pl
from jax.experimental.pallas import tpu as pltpu
from jax.sharding import PartitionSpec as P

MESH = pl.DeviceIdType.MESH
F32 = jnp.float32
BF16 = jnp.bfloat16
HALVES = 2
CORES = 2
RESET, UPDATE, CAND, REC_CAND, REC_RESET, REC_UPDATE = range(6)
GATES = 6
PAIR, WX, WN = range(3)
EARLY = 2


def ring_distance(offset, count):
    return min(offset, count - offset)


def gru_kernel(
    rows, cols,
    x_ref, h_ref, wx1, wru1, wn1, b1, wx2, wru2, wn2, b2,
    seq_out, last_out,
    weights, pairs, x_here, first_made, first_parts, state_in,
    h1_blocks, r1_blocks, h2_blocks, r2_blocks,
    states, updates, projections, seq_halves, last_halves,
    weight_sem, hand_sem, x_sem, wide_sem, parts_sem, state_sem,
    weight_sent, handed_sent, x_sent, wide_sent, made_sent, state_sent,
    block_sem, block_sent, out_sem, out_sent,
):
    chips = rows // CORES
    steps, batch, half = seq_out.shape
    chunk = HALVES * half
    places = chips * cols
    row, col = lax.axis_index("row"), lax.axis_index("col")
    xpos, core = row // CORES, row % CORES
    layers = ((wx1, wru1, wn1), (wx2, wru2, wn2))

    def device(x, c, y):
        return {"row": CORES * x + c, "col": y}

    def wrap_x(v):
        return lax.rem(v + 2 * chips, chips)

    def wrap_y(v):
        return lax.rem(v + 2 * cols, cols)

    def place_of(x_from, y_from, x_to, y_to):
        return chips * wrap_y(y_from - y_to) + wrap_x(x_from - x_to)

    barrier = pltpu.get_barrier_semaphore()
    for k in range(1, rows * cols):
        other = {"row": lax.rem(row + k % rows, rows), "col": lax.rem(col + k // rows, cols)}
        pl.semaphore_signal(barrier, inc=1, device_id=other, device_id_type=MESH)
    pl.semaphore_wait(barrier, rows * cols - 1)

    def remote(src, dst, send, recv, to):
        return pltpu.make_async_remote_copy(
            src_ref=src, dst_ref=dst, send_sem=send, recv_sem=recv, device_id=to, device_id_type=MESH
        )

    def chunk_place(c, j, x_from, x_to, y_to):
        return place_of(HALVES * c + j, x_from, x_to, y_to)

    def room(part, layer, index):
        if part == PAIR:
            return pairs.at[layer, index]
        return weights.at[layer, index, pl.ds(0, 3)] if part == WX else weights.at[layer, index, REC_CAND]

    def pieces(part, layer, j, x_to, index):
        depth = pl.ds(j * chunk, chunk)
        dst = room(part, layer, index)
        wx, wru, wn = layers[layer]
        for s in range(HALVES):
            units = pl.ds(pl.multiple_of(x_to * chunk + s * half, half), half)
            if part == PAIR:
                yield wru.at[depth, :, units], dst.at[s]
            elif part == WX:
                yield wx.at[:, depth, units], dst.at[:, s]
            else:
                yield wn.at[depth, units], dst.at[s]

    moving = ((PAIR, WN), (PAIR, WX, WN))

    def send_part(part, layer, turns):
        for turn in turns:
            x_to = wrap_x(xpos + turn)
            for j in range(2):
                place = chunk_place(core, j, xpos, x_to, col)
                sent, sem = weight_sent.at[layer, part, turn, j], weight_sem.at[layer, part, place]
                for src, dst in pieces(part, layer, j, x_to, place):
                    remote(src, dst, sent, sem, device(x_to, 1, col)).start()

    def keep_weights(layer):
        for part in moving[layer]:
            for j in range(2):
                place = chunk_place(1, j, xpos, xpos, col)
                for src, dst in pieces(part, layer, j, xpos, place):
                    pltpu.make_async_copy(src, dst, weight_sem.at[layer, part, place]).start()

    def hand_over():
        for part in moving[1]:
            for turn in far_turns:
                x_to = wrap_x(xpos + turn)
                for j in range(2):
                    for src, dst in pieces(part, 1, j, x_to, 2 * turn + j):
                        to = device(xpos, 0, col)
                        remote(src, dst, weight_sent.at[1, part, turn, j], hand_sem.at[part, turn, j], to).start()

    def send_handed(part):
        for turn in far_turns:
            x_to = wrap_x(xpos + turn)
            for j in range(2):
                src = room(part, 1, 2 * turn + j)
                pltpu.make_async_copy(src, src, hand_sem.at[part, turn, j]).wait()
                place = chunk_place(1, j, xpos, x_to, col)
                sent, sem = handed_sent.at[part, turn, j], weight_sem.at[1, part, place]
                remote(src, room(part, 1, place), sent, sem, device(x_to, 1, col)).start()

    def weights_arrived(part, layer):
        for p in range(places):
            here = room(part, layer, p)
            pltpu.make_async_copy(here, here, weight_sem.at[layer, part, p]).wait()

    def split_pairs(layer):
        def split(p, carry):
            here = pairs.at[layer, p]
            pltpu.make_async_copy(here, here, weight_sem.at[layer, PAIR, p]).wait()
            for s in range(HALVES):
                both = jnp.swapaxes(here[s], 0, 1)
                weights[layer, p, REC_RESET, s] = both[0]
                weights[layer, p, REC_UPDATE, s] = both[1]
            return carry

        lax.fori_loop(0, places, split, 0)

    def input_copies():
        for j in range(2):
            n = 2 * core + j
            for s in range(HALVES):
                yield x_ref.at[:, :, pl.ds(j * chunk + s * half, half)], x_here.at[n, :, s], x_sent.at[j], x_sem.at[n]
            for turn in range(chips):
                for src, dst in pieces(WX, 0, j, wrap_x(xpos + turn), 2 * CORES * turn + n):
                    yield src, dst, wide_sent.at[turn, j], wide_sem.at[turn, n]

    def keep_inputs():
        for src, dst, _, sem in input_copies():
            pltpu.make_async_copy(src, dst, sem).start()

    def hand_inputs():
        for src, dst, sent, sem in input_copies():
            remote(src, dst, sent, sem, device(xpos, 0, col)).start()

    def inputs_here():
        for n in range(2 * CORES):
            pltpu.make_async_copy(x_here.at[n], x_here.at[n], x_sem.at[n]).wait()
            for turn in range(chips):
                kept = weights.at[0, 2 * CORES * turn + n, pl.ds(0, 3)]
                pltpu.make_async_copy(kept, kept, wide_sem.at[turn, n]).wait()

    def wide(parts):
        return jnp.concatenate(parts, axis=1)

    def make_first(t, again):
        slot = lax.rem(t, 2)
        for turn in (2, 1, chips - 1, 0):
            made = first_made.at[slot, turn]
            if again:
                pltpu.make_async_copy(made, made, made_sent.at[slot, turn]).wait()
            total = None
            for n in range(2 * CORES):
                rhs = wide([weights[0, 2 * CORES * turn + n, g, s] for g in range(3) for s in range(HALVES)])
                lhs = wide([x_here[n, t, s] for s in range(HALVES)])
                term = jnp.dot(lhs, rhs, preferred_element_type=F32)
                total = term if total is None else total + term
            for g in range(3):
                for s in range(HALVES):
                    n = g * HALVES + s
                    made[g, s] = total[:, n * half : (n + 1) * half]
            seen = (chips - turn) % chips
            to = device(wrap_x(xpos + turn), 1, col)
            remote(made, first_parts.at[t, seen], made_sent.at[slot, turn], parts_sem.at[t, seen], to).start()

    far_turns = (2, 1, chips - 1)

    @pl.when(xpos == col)
    def _():
        for j in range(2):
            x_to = HALVES * core + j
            for s in range(HALVES):
                src = h_ref.at[:, :, pl.ds(j * chunk + s * half, half)]
                dst = state_in.at[:, s]
                mine = (x_to == xpos) & (core == 1)

                @pl.when(mine)
                def _():
                    pltpu.make_async_copy(src, dst, state_sem.at[s]).start()

                @pl.when(jnp.logical_not(mine))
                def _():
                    copy = remote(src, dst, state_sent.at[j, s], state_sem.at[s], device(x_to, 1, col))
                    copy.start()
                    copy.wait_send()

    for part in moving[0]:
        send_part(part, 0, far_turns)

    @pl.when(core == 1)
    def _():
        hand_inputs()
        keep_weights(0)
        hand_over()
        keep_weights(1)

    @pl.when(core == 0)
    def _():
        keep_inputs()
        for part in moving[0]:
            send_part(part, 0, (0,))
        inputs_here()
        for t in range(EARLY):
            make_first(t, False)
        for part in moving[1]:
            send_part(part, 1, far_turns)
            send_part(part, 1, (0,))
            send_handed(part)

    def drain_sends():
        for layer in range(2):
            for part in moving[layer]:
                piece = room(part, layer, 0)
                for j in range(2):
                    for turn in far_turns:
                        pltpu.make_async_copy(piece, piece, weight_sent.at[layer, part, turn, j]).wait()

        @pl.when(core == 0)
        def _():
            for layer in range(2):
                for part in moving[layer]:
                    piece = room(part, layer, 0)
                    for j in range(2):
                        pltpu.make_async_copy(piece, piece, weight_sent.at[layer, part, 0, j]).wait()
            for part in moving[1]:
                piece = room(part, 1, 0)
                for j in range(2):
                    for turn in far_turns:
                        pltpu.make_async_copy(piece, piece, handed_sent.at[part, turn, j]).wait()
            for slot in range(2):
                for turn in range(chips):
                    made = first_made.at[slot, turn]
                    pltpu.make_async_copy(made, made, made_sent.at[slot, turn]).wait()

        @pl.when(core == 1)
        def _():
            piece = room(WX, 0, 0)
            for j in range(2):
                pltpu.make_async_copy(x_here.at[0], x_here.at[0], x_sent.at[j]).wait()
                for turn in range(chips):
                    pltpu.make_async_copy(piece, piece, wide_sent.at[turn, j]).wait()

    offsets = [(dx, dy) for dy in range(cols) for dx in range(chips)]
    distance = [ring_distance(dx, chips) + ring_distance(dy, cols) for dx, dy in offsets]
    far_first = sorted(range(1, places), key=lambda p: -distance[p])
    by_arrival = sorted(range(places), key=lambda p: (distance[p], ring_distance(offsets[p][0], chips)))
    groups = [by_arrival[:6], by_arrival[6:10], by_arrival[10:]]

    def spread(blocks, kind):
        for p in far_first:
            dx, dy = offsets[p]
            there = chips * ((cols - dy) % cols) + (chips - dx) % chips
            to = device(wrap_x(xpos + dx), 1, wrap_y(col + dy))
            remote(blocks.at[0], blocks.at[there], block_sent.at[kind], block_sem.at[kind, there], to).start()

    def arrived(blocks, kind, p):
        pltpu.make_async_copy(blocks.at[p], blocks.at[p], block_sem.at[kind, p]).wait()

    def all_sent(blocks, kind):
        sent = blocks.at[pl.ds(1, places - 1)]
        pltpu.make_async_copy(sent, sent, block_sent.at[kind]).wait()

    def product(lhs_of, layer, gates, order, total=None):
        for p in order:
            rhs = wide([weights[layer, p, g, s] for g in gates for s in range(HALVES)])
            lhs = wide([lhs_of(p, s) for s in range(HALVES)])
            term = jnp.dot(lhs, rhs, preferred_element_type=F32)
            total = term if total is None else total + term
        return total

    def gathered(blocks, kind, layer, gate):
        total = None
        for group in groups:
            for p in group:
                if p:
                    arrived(blocks, kind, p)
            total = product(lambda p, s: blocks[p, s], layer, (gate,), group, total)
        return total

    def project(layer, lhs_of, bias):
        total = product(lhs_of, layer, (RESET, UPDATE, CAND), range(places))
        for g in range(3):
            for s in range(HALVES):
                n = g * HALVES + s
                here = bias[pl.ds(g, 1), pl.ds(pl.multiple_of(xpos * chunk + s * half, half), half)]
                projections[layer, g, s] = total[:, n * half : (n + 1) * half] + here

    def reset_half(layer, blocks, kind, out_blocks, send):
        total = gathered(blocks, kind, layer, REC_RESET)
        for s in range(HALVES):
            reset = jax.nn.sigmoid(projections[layer, RESET, s] + total[:, s * half : (s + 1) * half])
            out_blocks[0, s] = (reset * states[layer, s]).astype(BF16)
        send()
        total = product(lambda p, s: blocks[p, s], layer, (REC_UPDATE,), range(places))
        for s in range(HALVES):
            updates[layer, s] = jax.nn.sigmoid(projections[layer, UPDATE, s] + total[:, s * half : (s + 1) * half])

    def next_half(layer, blocks, kind, emit):
        total = gathered(blocks, kind, layer, REC_CAND)
        for s in range(HALVES):
            candidate = jnp.tanh(projections[layer, CAND, s] + total[:, s * half : (s + 1) * half])
            update = updates[layer, s]
            state = (1.0 - update) * candidate + update * states[layer, s]
            emit(s, state.astype(BF16))
            states[layer, s] = state

    H1, R1, H2, R2 = range(4)

    def first_reset(t):
        slot = h1_blocks.at[lax.rem(t, 2)]
        reset_half(0, slot, H1, r1_blocks, lambda: spread(r1_blocks, R1))
        all_sent(slot, H1)

    def first_next(t):
        slot = h1_blocks.at[lax.rem(t + 1, 2)]

        def emit(s, value):
            slot[0, s] = value

        next_half(0, r1_blocks, R1, emit)
        spread(slot, H1)
        all_sent(r1_blocks, R1)

    def first_inputs(t):
        for n in range(chips):
            part = first_parts.at[t, n]
            pltpu.make_async_copy(part, part, parts_sem.at[t, n]).wait()
        for g in range(3):
            for s in range(HALVES):
                here = b1[pl.ds(g, 1), pl.ds(pl.multiple_of(xpos * chunk + s * half, half), half)]
                projections[0, g, s] = sum(first_parts[t, n, g, s] for n in range(chips)) + here

    def second_inputs(t):
        slot = h1_blocks.at[lax.rem(t, 2)]
        project(1, lambda p, s: slot[p, s], b2)

    def second_reset(t):
        slot = h2_blocks.at[lax.rem(t, 2)]
        reset_half(1, slot, H2, r2_blocks, lambda: spread(r2_blocks, R2))
        all_sent(slot, H2)

    def second_next(t, last):
        slot = h2_blocks.at[lax.rem(t + 1, 2)]

        def emit(s, value):
            seq_halves[s, t] = value
            if not last:
                slot[0, s] = value

        next_half(1, r2_blocks, R2, emit)
        if not last:
            spread(slot, H2)
        all_sent(r2_blocks, R2)

    @pl.when(core == 1)
    def _():
        for s in range(HALVES):
            part = state_in.at[:, s]
            pltpu.make_async_copy(part, part, state_sem.at[s]).wait()
        for layer in range(2):
            for s in range(HALVES):
                states[layer, s] = state_in[layer, s]
        for s in range(HALVES):
            h1_blocks[0, 0, s] = state_in[0, s].astype(BF16)
            h2_blocks[0, 0, s] = state_in[1, s].astype(BF16)
        spread(h1_blocks.at[0], H1)
        spread(h2_blocks.at[0], H2)
        split_pairs(0)
        weights_arrived(WN, 0)
        first_inputs(0)
        first_reset(0)
        first_next(0)
        first_inputs(1)
        split_pairs(1)
        weights_arrived(WX, 1)

        def step(t, first):
            first_reset(t)
            second_inputs(t)
            second_reset(t - 1)
            first_next(t)
            if first:
                weights_arrived(WN, 1)
            second_next(t - 1, False)
            pl.when(t + 1 < steps)(lambda: first_inputs(t + 1))

        def later_step(t, carry):
            step(t, False)
            return carry

        step(1, True)
        lax.fori_loop(2, steps, later_step, 0)
        last_slot = h1_blocks.at[steps % 2]
        for p in range(1, places):
            arrived(last_slot, H1, p)
        all_sent(last_slot, H1)
        second_inputs(steps)
        second_reset(steps - 1)
        second_next(steps - 1, True)
        for layer in range(2):
            for s in range(HALVES):
                last_halves[s, layer] = states[layer, s]
        seq_copy = remote(seq_halves.at[0], seq_out, out_sent.at[0], out_sem.at[0], device(xpos, 0, col))
        last_copy = remote(last_halves.at[0], last_out, out_sent.at[1], out_sem.at[1], device(xpos, 0, col))
        seq_copy.start()
        last_copy.start()
        seq_out[...] = seq_halves[1]
        last_out[...] = last_halves[1]
        seq_copy.wait_send()
        last_copy.wait_send()

    @pl.when(core == 0)
    def _():
        def later_first(t, carry):
            make_first(t, True)
            return carry

        lax.fori_loop(EARLY, steps, later_first, 0)
        pltpu.make_async_copy(seq_out, seq_out, out_sem.at[0]).wait()
        pltpu.make_async_copy(last_out, last_out, out_sem.at[1]).wait()

    drain_sends()


def solution(mesh):
    rows, cols = mesh.shape["row"], mesh.shape["col"]
    chips = rows // CORES
    places = chips * cols

    def device_body(x_rows, h_rows, wx_l1, whru_l1, whn_l1, bias_l1, wx_l2, whru_l2, whn_l2, bias_l2):
        steps, batch, row_block = x_rows.shape
        col_block = wx_l1.shape[2]
        half = col_block // rows
        chunk = HALVES * half
        anywhere = pl.BlockSpec(memory_space=pl.ANY)
        vmem = pl.BlockSpec(memory_space=pltpu.VMEM)
        dma = pltpu.SemaphoreType.DMA
        kinds = 4
        block = (HALVES, batch, half)
        scratch = [
            pltpu.VMEM((2, places, GATES, HALVES, chunk, half), BF16),
            pltpu.VMEM((2, places, HALVES, chunk, 2, half), BF16),
            pltpu.VMEM((2 * CORES, steps, *block), BF16),
            pltpu.VMEM((2, chips, 3, *block), F32),
            pltpu.VMEM((steps, chips, 3, *block), F32),
            pltpu.VMEM((2, *block), F32),
            pltpu.VMEM((2, places, *block), BF16),
            pltpu.VMEM((places, *block), BF16),
            pltpu.VMEM((2, places, *block), BF16),
            pltpu.VMEM((places, *block), BF16),
            pltpu.VMEM((2, *block), F32),
            pltpu.VMEM((2, *block), F32),
            pltpu.VMEM((2, 3, *block), F32),
            pltpu.VMEM((HALVES, steps, batch, half), BF16),
            pltpu.VMEM((HALVES, 2, batch, half), F32),
            dma((2, 3, places)),
            dma((3, chips, 2)),
            dma((2 * CORES,)),
            dma((chips, 2 * CORES)),
            dma((steps, chips)),
            dma((HALVES,)),
            dma((2, 3, chips, 2)),
            dma((3, chips, 2)),
            dma((2,)),
            dma((chips, 2)),
            dma((2, chips)),
            dma((2, HALVES)),
            dma((kinds, places)),
            dma((kinds,)),
            dma((2,)),
            dma((2,)),
        ]
        return pl.pallas_call(
            functools.partial(gru_kernel, rows, cols),
            name="gru",
            out_shape=(
                jax.ShapeDtypeStruct((steps, batch, half), BF16),
                jax.ShapeDtypeStruct((2, batch, half), F32),
            ),
            in_specs=[anywhere, anywhere, anywhere, anywhere, anywhere, vmem, anywhere, anywhere, anywhere, vmem],
            out_specs=(vmem, vmem),
            scratch_shapes=scratch,
            compiler_params=pltpu.CompilerParams(
                collective_id=0, has_side_effects=True, vmem_limit_bytes=60 * 1024 * 1024
            ),
        )(
            x_rows, h_rows,
            jnp.transpose(wx_l1, (1, 0, 2)), whru_l1, whn_l1, bias_l1,
            jnp.transpose(wx_l2, (1, 0, 2)), whru_l2, whn_l2, bias_l2,
        )

    seq_spec = P(None, "data", "row")
    out_spec = P(None, "data", ("col", "row"))
    wide_spec = P("row", None, "col")
    square_spec = P("row", "col")
    bias_spec = P(None, "col")
    return jax.shard_map(
        device_body,
        mesh=mesh,
        in_specs=(seq_spec, seq_spec, wide_spec, wide_spec, square_spec, bias_spec, wide_spec, wide_spec, square_spec, bias_spec),
        out_specs=(out_spec, out_spec),
        check_vma=False,
    )
```

```python
import functools

import jax
import jax.numpy as jnp
from jax import lax
from jax.experimental import pallas as pl
from jax.experimental.pallas import tpu as pltpu
from jax.sharding import PartitionSpec as P

MESH = pl.DeviceIdType.MESH
F32 = jnp.float32
BF16 = jnp.bfloat16
HALVES = 2
CORES = 2
RESET, UPDATE, CAND, REC_CAND, REC_RESET, REC_UPDATE = range(6)
GATES = 6
PAIR, WX, WN = range(3)
EARLY = 2


def ring_distance(offset, count):
    return min(offset, count - offset)


def gru_kernel(
    rows, cols,
    x_ref, h_ref, wx1, wru1, wn1, b1, wx2, wru2, wn2, b2,
    seq_out, last_out,
    weights, pairs, x_here, first_made, first_parts, state_in,
    h1_blocks, r1_blocks, h2_blocks, r2_blocks,
    states, updates, projections, seq_halves, last_halves,
    weight_sem, hand_sem, x_sem, wide_sem, parts_sem, state_sem,
    weight_sent, handed_sent, x_sent, wide_sent, made_sent, state_sent,
    block_sem, block_sent, out_sem, out_sent, go_sem,
):
    chips = rows // CORES
    steps, batch, half = seq_out.shape
    chunk = HALVES * half
    places = chips * cols
    row, col = lax.axis_index("row"), lax.axis_index("col")
    xpos, core = row // CORES, row % CORES
    layers = ((wx1, wru1, wn1), (wx2, wru2, wn2))

    def device(x, c, y):
        return {"row": CORES * x + c, "col": y}

    def wrap_x(v):
        return lax.rem(v + 2 * chips, chips)

    def wrap_y(v):
        return lax.rem(v + 2 * cols, cols)

    def place_of(x_from, y_from, x_to, y_to):
        return chips * wrap_y(y_from - y_to) + wrap_x(x_from - x_to)

    barrier = pltpu.get_barrier_semaphore()
    for k in range(1, rows * cols):
        other = {"row": lax.rem(row + k % rows, rows), "col": lax.rem(col + k // rows, cols)}
        pl.semaphore_signal(barrier, inc=1, device_id=other, device_id_type=MESH)
    pl.semaphore_wait(barrier, rows * cols - 1)

    def remote(src, dst, send, recv, to):
        return pltpu.make_async_remote_copy(
            src_ref=src, dst_ref=dst, send_sem=send, recv_sem=recv, device_id=to, device_id_type=MESH
        )

    def chunk_place(c, j, x_from, x_to, y_to):
        return place_of(HALVES * c + j, x_from, x_to, y_to)

    def room(part, layer, index):
        if part == PAIR:
            return pairs.at[layer, index]
        return weights.at[layer, index, pl.ds(0, 3)] if part == WX else weights.at[layer, index, REC_CAND]

    def pieces(part, layer, j, x_to, index):
        depth = pl.ds(j * chunk, chunk)
        dst = room(part, layer, index)
        wx, wru, wn = layers[layer]
        for s in range(HALVES):
            units = pl.ds(pl.multiple_of(x_to * chunk + s * half, half), half)
            if part == PAIR:
                yield wru.at[depth, :, units], dst.at[s]
            elif part == WX:
                yield wx.at[:, depth, units], dst.at[:, s]
            else:
                yield wn.at[depth, units], dst.at[s]

    moving = ((PAIR, WN), (PAIR, WX, WN))

    def send_part(part, layer, turns):
        for turn in turns:
            x_to = wrap_x(xpos + turn)
            for j in range(2):
                place = chunk_place(core, j, xpos, x_to, col)
                sent, sem = weight_sent.at[layer, part, turn, j], weight_sem.at[layer, part, place]
                for src, dst in pieces(part, layer, j, x_to, place):
                    remote(src, dst, sent, sem, device(x_to, 1, col)).start()

    def keep_weights(layer):
        for part in moving[layer]:
            for j in range(2):
                place = chunk_place(1, j, xpos, xpos, col)
                for src, dst in pieces(part, layer, j, xpos, place):
                    pltpu.make_async_copy(src, dst, weight_sem.at[layer, part, place]).start()

    def hand_over():
        for part in moving[1]:
            for turn in far_turns:
                x_to = wrap_x(xpos + turn)
                for j in range(2):
                    for src, dst in pieces(part, 1, j, x_to, 2 * turn + j):
                        to = device(xpos, 0, col)
                        remote(src, dst, weight_sent.at[1, part, turn, j], hand_sem.at[part, turn, j], to).start()

    def send_handed(part):
        for turn in far_turns:
            x_to = wrap_x(xpos + turn)
            for j in range(2):
                src = room(part, 1, 2 * turn + j)
                pltpu.make_async_copy(src, src, hand_sem.at[part, turn, j]).wait()
                place = chunk_place(1, j, xpos, x_to, col)
                sent, sem = handed_sent.at[part, turn, j], weight_sem.at[1, part, place]
                remote(src, room(part, 1, place), sent, sem, device(x_to, 1, col)).start()

    def weights_arrived(part, layer):
        for p in range(places):
            here = room(part, layer, p)
            pltpu.make_async_copy(here, here, weight_sem.at[layer, part, p]).wait()

    def split_pairs(layer):
        def split(p, carry):
            here = pairs.at[layer, p]
            pltpu.make_async_copy(here, here, weight_sem.at[layer, PAIR, p]).wait()
            for s in range(HALVES):
                both = jnp.swapaxes(here[s], 0, 1)
                weights[layer, p, REC_RESET, s] = both[0]
                weights[layer, p, REC_UPDATE, s] = both[1]
            return carry

        lax.fori_loop(0, places, split, 0)

    def input_copies():
        for j in range(2):
            n = 2 * core + j
            for s in range(HALVES):
                yield x_ref.at[:, :, pl.ds(j * chunk + s * half, half)], x_here.at[n, :, s], x_sent.at[j], x_sem.at[n]
            for turn in range(chips):
                for src, dst in pieces(WX, 0, j, wrap_x(xpos + turn), 2 * CORES * turn + n):
                    yield src, dst, wide_sent.at[turn, j], wide_sem.at[turn, n]

    def keep_inputs():
        for src, dst, _, sem in input_copies():
            pltpu.make_async_copy(src, dst, sem).start()

    def hand_inputs():
        for src, dst, sent, sem in input_copies():
            remote(src, dst, sent, sem, device(xpos, 0, col)).start()

    def inputs_here():
        for n in range(2 * CORES):
            pltpu.make_async_copy(x_here.at[n], x_here.at[n], x_sem.at[n]).wait()
            for turn in range(chips):
                kept = weights.at[0, 2 * CORES * turn + n, pl.ds(0, 3)]
                pltpu.make_async_copy(kept, kept, wide_sem.at[turn, n]).wait()

    def wide(parts):
        return jnp.concatenate(parts, axis=1)

    def make_first(t, again, turns=None):
        slot = lax.rem(t, 2)
        for turn in turns or (2, 1, chips - 1, 0):
            made = first_made.at[slot, turn]
            if again:
                pltpu.make_async_copy(made, made, made_sent.at[slot, turn]).wait()
            total = None
            for n in range(2 * CORES):
                rhs = wide([weights[0, 2 * CORES * turn + n, g, s] for g in range(3) for s in range(HALVES)])
                lhs = wide([x_here[n, t, s] for s in range(HALVES)])
                term = jnp.dot(lhs, rhs, preferred_element_type=F32)
                total = term if total is None else total + term
            for g in range(3):
                for s in range(HALVES):
                    n = g * HALVES + s
                    made[g, s] = total[:, n * half : (n + 1) * half]
            seen = (chips - turn) % chips
            to = device(wrap_x(xpos + turn), 1, col)
            remote(made, first_parts.at[t, seen], made_sent.at[slot, turn], parts_sem.at[t, seen], to).start()

    far_turns = (2, 1, chips - 1)

    @pl.when(xpos == col)
    def _():
        for j in range(2):
            x_to = HALVES * core + j
            for s in range(HALVES):
                src = h_ref.at[:, :, pl.ds(j * chunk + s * half, half)]
                dst = state_in.at[:, s]
                mine = (x_to == xpos) & (core == 1)

                @pl.when(mine)
                def _():
                    pltpu.make_async_copy(src, dst, state_sem.at[s]).start()

                @pl.when(jnp.logical_not(mine))
                def _():
                    copy = remote(src, dst, state_sent.at[j, s], state_sem.at[s], device(x_to, 1, col))
                    copy.start()
                    copy.wait_send()

    for part in moving[0]:
        send_part(part, 0, far_turns)

    @pl.when(core == 1)
    def _():
        hand_inputs()
        keep_weights(0)
        hand_over()
        keep_weights(1)

    @pl.when(core == 0)
    def _():
        keep_inputs()
        for part in moving[0]:
            send_part(part, 0, (0,))
        inputs_here()
        for t in range(EARLY):
            make_first(t, False)
        for part in moving[1]:
            send_part(part, 1, far_turns)
            send_part(part, 1, (0,))
            send_handed(part)

    def drain_sends():
        for layer in range(2):
            for part in moving[layer]:
                piece = room(part, layer, 0)
                for j in range(2):
                    for turn in far_turns:
                        pltpu.make_async_copy(piece, piece, weight_sent.at[layer, part, turn, j]).wait()

        @pl.when(core == 0)
        def _():
            for layer in range(2):
                for part in moving[layer]:
                    piece = room(part, layer, 0)
                    for j in range(2):
                        pltpu.make_async_copy(piece, piece, weight_sent.at[layer, part, 0, j]).wait()
            for part in moving[1]:
                piece = room(part, 1, 0)
                for j in range(2):
                    for turn in far_turns:
                        pltpu.make_async_copy(piece, piece, handed_sent.at[part, turn, j]).wait()
            for slot in range(2):
                for turn in range(chips):
                    made = first_made.at[slot, turn]
                    pltpu.make_async_copy(made, made, made_sent.at[slot, turn]).wait()

        @pl.when(core == 1)
        def _():
            piece = room(WX, 0, 0)
            for j in range(2):
                pltpu.make_async_copy(x_here.at[0], x_here.at[0], x_sent.at[j]).wait()
                for turn in range(chips):
                    pltpu.make_async_copy(piece, piece, wide_sent.at[turn, j]).wait()

    offsets = [(dx, dy) for dy in range(cols) for dx in range(chips)]
    distance = [ring_distance(dx, chips) + ring_distance(dy, cols) for dx, dy in offsets]
    far_first = sorted(range(1, places), key=lambda p: -distance[p])
    by_arrival = sorted(range(places), key=lambda p: (distance[p], ring_distance(offsets[p][0], chips)))
    groups = [by_arrival[:6], by_arrival[6:10], by_arrival[10:]]

    def spread(blocks, kind):
        for p in far_first:
            dx, dy = offsets[p]
            there = chips * ((cols - dy) % cols) + (chips - dx) % chips
            to = device(wrap_x(xpos + dx), 1, wrap_y(col + dy))
            remote(blocks.at[0], blocks.at[there], block_sent.at[kind], block_sem.at[kind, there], to).start()

    def arrived(blocks, kind, p):
        pltpu.make_async_copy(blocks.at[p], blocks.at[p], block_sem.at[kind, p]).wait()

    def all_sent(blocks, kind):
        sent = blocks.at[pl.ds(1, places - 1)]
        pltpu.make_async_copy(sent, sent, block_sent.at[kind]).wait()

    def product(lhs_of, layer, gates, order, total=None):
        for p in order:
            rhs = wide([weights[layer, p, g, s] for g in gates for s in range(HALVES)])
            lhs = wide([lhs_of(p, s) for s in range(HALVES)])
            term = jnp.dot(lhs, rhs, preferred_element_type=F32)
            total = term if total is None else total + term
        return total

    def gathered(blocks, kind, layer, gate):
        total = None
        for group in groups:
            for p in group:
                if p:
                    arrived(blocks, kind, p)
            total = product(lambda p, s: blocks[p, s], layer, (gate,), group, total)
        return total

    def project(layer, lhs_of, bias):
        total = product(lhs_of, layer, (RESET, UPDATE, CAND), range(places))
        for g in range(3):
            for s in range(HALVES):
                n = g * HALVES + s
                here = bias[pl.ds(g, 1), pl.ds(pl.multiple_of(xpos * chunk + s * half, half), half)]
                projections[layer, g, s] = total[:, n * half : (n + 1) * half] + here

    def reset_half(layer, blocks, kind, out_blocks, send):
        total = gathered(blocks, kind, layer, REC_RESET)
        for s in range(HALVES):
            reset = jax.nn.sigmoid(projections[layer, RESET, s] + total[:, s * half : (s + 1) * half])
            out_blocks[0, s] = (reset * states[layer, s]).astype(BF16)
        send()
        total = product(lambda p, s: blocks[p, s], layer, (REC_UPDATE,), range(places))
        for s in range(HALVES):
            updates[layer, s] = jax.nn.sigmoid(projections[layer, UPDATE, s] + total[:, s * half : (s + 1) * half])

    def next_half(layer, blocks, kind, emit):
        total = gathered(blocks, kind, layer, REC_CAND)
        for s in range(HALVES):
            candidate = jnp.tanh(projections[layer, CAND, s] + total[:, s * half : (s + 1) * half])
            update = updates[layer, s]
            state = (1.0 - update) * candidate + update * states[layer, s]
            emit(s, state.astype(BF16))
            states[layer, s] = state

    H1, R1, H2, R2 = range(4)

    def first_reset(t):
        slot = h1_blocks.at[lax.rem(t, 2)]
        reset_half(0, slot, H1, r1_blocks, lambda: spread(r1_blocks, R1))
        all_sent(slot, H1)

    def first_next(t):
        slot = h1_blocks.at[lax.rem(t + 1, 2)]

        def emit(s, value):
            slot[0, s] = value

        next_half(0, r1_blocks, R1, emit)
        spread(slot, H1)
        all_sent(r1_blocks, R1)

    def first_inputs(t):
        for n in range(chips):
            part = first_parts.at[t, n]
            pltpu.make_async_copy(part, part, parts_sem.at[t, n]).wait()
        for g in range(3):
            for s in range(HALVES):
                here = b1[pl.ds(g, 1), pl.ds(pl.multiple_of(xpos * chunk + s * half, half), half)]
                projections[0, g, s] = sum(first_parts[t, n, g, s] for n in range(chips)) + here

    def second_inputs(t):
        slot = h1_blocks.at[lax.rem(t, 2)]
        project(1, lambda p, s: slot[p, s], b2)

    def second_reset(t):
        slot = h2_blocks.at[lax.rem(t, 2)]
        reset_half(1, slot, H2, r2_blocks, lambda: spread(r2_blocks, R2))
        all_sent(slot, H2)

    def second_next(t, last):
        slot = h2_blocks.at[lax.rem(t + 1, 2)]

        def emit(s, value):
            seq_halves[s, t] = value
            if not last:
                slot[0, s] = value

        next_half(1, r2_blocks, R2, emit)
        if not last:
            spread(slot, H2)
        all_sent(r2_blocks, R2)

    @pl.when(core == 1)
    def _():
        for s in range(HALVES):
            part = state_in.at[:, s]
            pltpu.make_async_copy(part, part, state_sem.at[s]).wait()
        for layer in range(2):
            for s in range(HALVES):
                states[layer, s] = state_in[layer, s]
        for s in range(HALVES):
            h1_blocks[0, 0, s] = state_in[0, s].astype(BF16)
            h2_blocks[0, 0, s] = state_in[1, s].astype(BF16)
        spread(h1_blocks.at[0], H1)
        spread(h2_blocks.at[0], H2)
        split_pairs(0)
        weights_arrived(WN, 0)
        first_inputs(0)
        first_reset(0)
        first_next(0)
        first_inputs(1)
        split_pairs(1)
        weights_arrived(WX, 1)

        def let_go(t):
            def signal():
                pl.semaphore_signal(go_sem, inc=1, device_id=device(xpos, 0, col), device_id_type=MESH)

            pl.when(t + EARLY < steps)(signal)

        def step(t, first):
            first_reset(t)
            second_inputs(t)
            second_reset(t - 1)
            let_go(t)
            first_next(t)
            if first:
                weights_arrived(WN, 1)
            second_next(t - 1, False)
            let_go(t)
            pl.when(t + 1 < steps)(lambda: first_inputs(t + 1))

        def later_step(t, carry):
            step(t, False)
            return carry

        step(1, True)
        lax.fori_loop(2, steps, later_step, 0)
        last_slot = h1_blocks.at[steps % 2]
        for p in range(1, places):
            arrived(last_slot, H1, p)
        all_sent(last_slot, H1)
        second_inputs(steps)
        second_reset(steps - 1)
        second_next(steps - 1, True)
        for layer in range(2):
            for s in range(HALVES):
                last_halves[s, layer] = states[layer, s]
        seq_copy = remote(seq_halves.at[0], seq_out, out_sent.at[0], out_sem.at[0], device(xpos, 0, col))
        last_copy = remote(last_halves.at[0], last_out, out_sent.at[1], out_sem.at[1], device(xpos, 0, col))
        seq_copy.start()
        last_copy.start()
        seq_out[...] = seq_halves[1]
        last_out[...] = last_halves[1]
        seq_copy.wait_send()
        last_copy.wait_send()

    @pl.when(core == 0)
    def _():
        make_first(EARLY, True)

        def later_first(t, carry):
            for turns in ((2,), (1, chips - 1, 0)):
                pl.semaphore_wait(go_sem, 1)
                make_first(t, True, turns)
            return carry

        lax.fori_loop(EARLY + 1, steps, later_first, 0)
        pltpu.make_async_copy(seq_out, seq_out, out_sem.at[0]).wait()
        pltpu.make_async_copy(last_out, last_out, out_sem.at[1]).wait()

    drain_sends()


def solution(mesh):
    rows, cols = mesh.shape["row"], mesh.shape["col"]
    chips = rows // CORES
    places = chips * cols

    def device_body(x_rows, h_rows, wx_l1, whru_l1, whn_l1, bias_l1, wx_l2, whru_l2, whn_l2, bias_l2):
        steps, batch, row_block = x_rows.shape
        col_block = wx_l1.shape[2]
        half = col_block // rows
        chunk = HALVES * half
        anywhere = pl.BlockSpec(memory_space=pl.ANY)
        vmem = pl.BlockSpec(memory_space=pltpu.VMEM)
        dma = pltpu.SemaphoreType.DMA
        kinds = 4
        block = (HALVES, batch, half)
        scratch = [
            pltpu.VMEM((2, places, GATES, HALVES, chunk, half), BF16),
            pltpu.VMEM((2, places, HALVES, chunk, 2, half), BF16),
            pltpu.VMEM((2 * CORES, steps, *block), BF16),
            pltpu.VMEM((2, chips, 3, *block), F32),
            pltpu.VMEM((steps, chips, 3, *block), F32),
            pltpu.VMEM((2, *block), F32),
            pltpu.VMEM((2, places, *block), BF16),
            pltpu.VMEM((places, *block), BF16),
            pltpu.VMEM((2, places, *block), BF16),
            pltpu.VMEM((places, *block), BF16),
            pltpu.VMEM((2, *block), F32),
            pltpu.VMEM((2, *block), F32),
            pltpu.VMEM((2, 3, *block), F32),
            pltpu.VMEM((HALVES, steps, batch, half), BF16),
            pltpu.VMEM((HALVES, 2, batch, half), F32),
            dma((2, 3, places)),
            dma((3, chips, 2)),
            dma((2 * CORES,)),
            dma((chips, 2 * CORES)),
            dma((steps, chips)),
            dma((HALVES,)),
            dma((2, 3, chips, 2)),
            dma((3, chips, 2)),
            dma((2,)),
            dma((chips, 2)),
            dma((2, chips)),
            dma((2, HALVES)),
            dma((kinds, places)),
            dma((kinds,)),
            dma((2,)),
            dma((2,)),
            pltpu.SemaphoreType.REGULAR,
        ]
        return pl.pallas_call(
            functools.partial(gru_kernel, rows, cols),
            name="gru",
            out_shape=(
                jax.ShapeDtypeStruct((steps, batch, half), BF16),
                jax.ShapeDtypeStruct((2, batch, half), F32),
            ),
            in_specs=[anywhere, anywhere, anywhere, anywhere, anywhere, vmem, anywhere, anywhere, anywhere, vmem],
            out_specs=(vmem, vmem),
            scratch_shapes=scratch,
            compiler_params=pltpu.CompilerParams(
                collective_id=0, has_side_effects=True, vmem_limit_bytes=60 * 1024 * 1024
            ),
        )(
            x_rows, h_rows,
            jnp.transpose(wx_l1, (1, 0, 2)), whru_l1, whn_l1, bias_l1,
            jnp.transpose(wx_l2, (1, 0, 2)), whru_l2, whn_l2, bias_l2,
        )

    seq_spec = P(None, "data", "row")
    out_spec = P(None, "data", ("col", "row"))
    wide_spec = P("row", None, "col")
    square_spec = P("row", "col")
    bias_spec = P(None, "col")
    return jax.shard_map(
        device_body,
        mesh=mesh,
        in_specs=(seq_spec, seq_spec, wide_spec, wide_spec, square_spec, bias_spec, wide_spec, wide_spec, square_spec, bias_spec),
        out_specs=(out_spec, out_spec),
        check_vma=False,
    )
```

```python
import functools

import jax
import jax.numpy as jnp
from jax import lax
from jax.experimental import pallas as pl
from jax.experimental.pallas import tpu as pltpu
from jax.sharding import PartitionSpec as P

MESH = pl.DeviceIdType.MESH
F32 = jnp.float32
BF16 = jnp.bfloat16
HALVES = 2
CORES = 2
RESET, UPDATE, CAND, REC_CAND, REC_RESET, REC_UPDATE = range(6)
GATES = 6
PAIR, WX, WN = range(3)
EARLY = 2


def ring_distance(offset, count):
    return min(offset, count - offset)


def gru_kernel(
    rows, cols,
    x_ref, h_ref, wx1, wru1, wn1, b1_ref, wx2, wru2, wn2, b2_ref,
    seq_out, last_out,
    weights, pairs, x_here, first_made, first_parts, state_in,
    h1_blocks, r1_blocks, h2_blocks, r2_blocks,
    states, updates, projections, seq_halves, last_halves, b1, b2,
    weight_sem, hand_sem, x_sem, wide_sem, parts_sem, state_sem,
    weight_sent, handed_sent, x_sent, wide_sent, made_sent, state_sent,
    block_sem, block_sent, out_sem, out_sent, bias_sem,
):
    chips = rows // CORES
    steps, batch, half = seq_out.shape
    chunk = HALVES * half
    places = chips * cols
    row, col = lax.axis_index("row"), lax.axis_index("col")
    xpos, core = row // CORES, row % CORES
    layers = ((wx1, wru1, wn1), (wx2, wru2, wn2))

    def device(x, c, y):
        return {"row": CORES * x + c, "col": y}

    def wrap_x(v):
        return lax.rem(v + 2 * chips, chips)

    def wrap_y(v):
        return lax.rem(v + 2 * cols, cols)

    def place_of(x_from, y_from, x_to, y_to):
        return chips * wrap_y(y_from - y_to) + wrap_x(x_from - x_to)

    for n, (src, dst) in enumerate(((b1_ref, b1), (b2_ref, b2))):
        pltpu.make_async_copy(src, dst, bias_sem.at[n]).start()

    barrier = pltpu.get_barrier_semaphore()
    for k in range(1, rows * cols):
        other = {"row": lax.rem(row + k % rows, rows), "col": lax.rem(col + k // rows, cols)}
        pl.semaphore_signal(barrier, inc=1, device_id=other, device_id_type=MESH)
    pl.semaphore_wait(barrier, rows * cols - 1)

    def remote(src, dst, send, recv, to):
        return pltpu.make_async_remote_copy(
            src_ref=src, dst_ref=dst, send_sem=send, recv_sem=recv, device_id=to, device_id_type=MESH
        )

    def chunk_place(c, j, x_from, x_to, y_to):
        return place_of(HALVES * c + j, x_from, x_to, y_to)

    def room(part, layer, index):
        if part == PAIR:
            return pairs.at[layer, index]
        return weights.at[layer, index, pl.ds(0, 3)] if part == WX else weights.at[layer, index, REC_CAND]

    def pieces(part, layer, j, x_to, index):
        depth = pl.ds(j * chunk, chunk)
        dst = room(part, layer, index)
        wx, wru, wn = layers[layer]
        for s in range(HALVES):
            units = pl.ds(pl.multiple_of(x_to * chunk + s * half, half), half)
            if part == PAIR:
                yield wru.at[depth, :, units], dst.at[s]
            elif part == WX:
                yield wx.at[:, depth, units], dst.at[:, s]
            else:
                yield wn.at[depth, units], dst.at[s]

    moving = ((PAIR, WN), (PAIR, WX, WN))

    def send_part(part, layer, turns):
        for turn in turns:
            x_to = wrap_x(xpos + turn)
            for j in range(2):
                place = chunk_place(core, j, xpos, x_to, col)
                sent, sem = weight_sent.at[layer, part, turn, j], weight_sem.at[layer, part, place]
                for src, dst in pieces(part, layer, j, x_to, place):
                    remote(src, dst, sent, sem, device(x_to, 1, col)).start()

    def keep_weights(layer):
        for part in moving[layer]:
            for j in range(2):
                place = chunk_place(1, j, xpos, xpos, col)
                for src, dst in pieces(part, layer, j, xpos, place):
                    pltpu.make_async_copy(src, dst, weight_sem.at[layer, part, place]).start()

    def hand_over():
        for part in moving[1]:
            for turn in far_turns:
                x_to = wrap_x(xpos + turn)
                for j in range(2):
                    for src, dst in pieces(part, 1, j, x_to, 2 * turn + j):
                        to = device(xpos, 0, col)
                        remote(src, dst, weight_sent.at[1, part, turn, j], hand_sem.at[part, turn, j], to).start()

    def send_handed(part):
        for turn in far_turns:
            x_to = wrap_x(xpos + turn)
            for j in range(2):
                src = room(part, 1, 2 * turn + j)
                pltpu.make_async_copy(src, src, hand_sem.at[part, turn, j]).wait()
                place = chunk_place(1, j, xpos, x_to, col)
                sent, sem = handed_sent.at[part, turn, j], weight_sem.at[1, part, place]
                remote(src, room(part, 1, place), sent, sem, device(x_to, 1, col)).start()

    def weights_arrived(part, layer):
        for p in range(places):
            here = room(part, layer, p)
            pltpu.make_async_copy(here, here, weight_sem.at[layer, part, p]).wait()

    def split_pairs(layer):
        def split(p, carry):
            here = pairs.at[layer, p]
            pltpu.make_async_copy(here, here, weight_sem.at[layer, PAIR, p]).wait()
            for s in range(HALVES):
                both = jnp.swapaxes(here[s], 0, 1)
                weights[layer, p, REC_RESET, s] = both[0]
                weights[layer, p, REC_UPDATE, s] = both[1]
            return carry

        lax.fori_loop(0, places, split, 0)

    def input_copies():
        for j in range(2):
            n = 2 * core + j
            for s in range(HALVES):
                yield x_ref.at[:, :, pl.ds(j * chunk + s * half, half)], x_here.at[n, :, s], x_sent.at[j], x_sem.at[n]
            for turn in range(chips):
                for src, dst in pieces(WX, 0, j, wrap_x(xpos + turn), 2 * CORES * turn + n):
                    yield src, dst, wide_sent.at[turn, j], wide_sem.at[turn, n]

    def keep_inputs():
        for src, dst, _, sem in input_copies():
            pltpu.make_async_copy(src, dst, sem).start()

    def hand_inputs():
        for src, dst, sent, sem in input_copies():
            remote(src, dst, sent, sem, device(xpos, 0, col)).start()

    def inputs_here():
        for n in range(2 * CORES):
            pltpu.make_async_copy(x_here.at[n], x_here.at[n], x_sem.at[n]).wait()
            for turn in range(chips):
                kept = weights.at[0, 2 * CORES * turn + n, pl.ds(0, 3)]
                pltpu.make_async_copy(kept, kept, wide_sem.at[turn, n]).wait()

    def wide(parts):
        return jnp.concatenate(parts, axis=1)

    def make_first(t, again):
        slot = lax.rem(t, 2)
        for turn in (2, 1, chips - 1, 0):
            made = first_made.at[slot, turn]
            if again:
                pltpu.make_async_copy(made, made, made_sent.at[slot, turn]).wait()
            total = None
            for n in range(2 * CORES):
                rhs = wide([weights[0, 2 * CORES * turn + n, g, s] for g in range(3) for s in range(HALVES)])
                lhs = wide([x_here[n, t, s] for s in range(HALVES)])
                term = jnp.dot(lhs, rhs, preferred_element_type=F32)
                total = term if total is None else total + term
            for g in range(3):
                for s in range(HALVES):
                    n = g * HALVES + s
                    made[g, s] = total[:, n * half : (n + 1) * half]
            seen = (chips - turn) % chips
            to = device(wrap_x(xpos + turn), 1, col)
            remote(made, first_parts.at[t, seen], made_sent.at[slot, turn], parts_sem.at[t, seen], to).start()

    far_turns = (2, 1, chips - 1)

    @pl.when(xpos == col)
    def _():
        for j in range(2):
            x_to = HALVES * core + j
            for s in range(HALVES):
                src = h_ref.at[:, :, pl.ds(j * chunk + s * half, half)]
                dst = state_in.at[:, s]
                mine = (x_to == xpos) & (core == 1)

                @pl.when(mine)
                def _():
                    pltpu.make_async_copy(src, dst, state_sem.at[s]).start()

                @pl.when(jnp.logical_not(mine))
                def _():
                    copy = remote(src, dst, state_sent.at[j, s], state_sem.at[s], device(x_to, 1, col))
                    copy.start()
                    copy.wait_send()

    for part in moving[0]:
        send_part(part, 0, far_turns)

    @pl.when(core == 1)
    def _():
        hand_inputs()
        keep_weights(0)
        hand_over()
        keep_weights(1)

    @pl.when(core == 0)
    def _():
        keep_inputs()
        for part in moving[0]:
            send_part(part, 0, (0,))
        inputs_here()
        for t in range(EARLY):
            make_first(t, False)
        for part in moving[1]:
            send_part(part, 1, far_turns)
            send_part(part, 1, (0,))
            send_handed(part)

    for n, dst in enumerate((b1, b2)):
        pltpu.make_async_copy(dst, dst, bias_sem.at[n]).wait()

    def drain_sends():
        for layer in range(2):
            for part in moving[layer]:
                piece = room(part, layer, 0)
                for j in range(2):
                    for turn in far_turns:
                        pltpu.make_async_copy(piece, piece, weight_sent.at[layer, part, turn, j]).wait()

        @pl.when(core == 0)
        def _():
            for layer in range(2):
                for part in moving[layer]:
                    piece = room(part, layer, 0)
                    for j in range(2):
                        pltpu.make_async_copy(piece, piece, weight_sent.at[layer, part, 0, j]).wait()
            for part in moving[1]:
                piece = room(part, 1, 0)
                for j in range(2):
                    for turn in far_turns:
                        pltpu.make_async_copy(piece, piece, handed_sent.at[part, turn, j]).wait()
            for slot in range(2):
                for turn in range(chips):
                    made = first_made.at[slot, turn]
                    pltpu.make_async_copy(made, made, made_sent.at[slot, turn]).wait()

        @pl.when(core == 1)
        def _():
            piece = room(WX, 0, 0)
            for j in range(2):
                pltpu.make_async_copy(x_here.at[0], x_here.at[0], x_sent.at[j]).wait()
                for turn in range(chips):
                    pltpu.make_async_copy(piece, piece, wide_sent.at[turn, j]).wait()

    offsets = [(dx, dy) for dy in range(cols) for dx in range(chips)]
    distance = [ring_distance(dx, chips) + ring_distance(dy, cols) for dx, dy in offsets]
    far_first = sorted(range(1, places), key=lambda p: -distance[p])
    by_arrival = sorted(range(places), key=lambda p: (distance[p], ring_distance(offsets[p][0], chips)))
    groups = [by_arrival[:6], by_arrival[6:10], by_arrival[10:]]

    def spread(blocks, kind):
        for p in far_first:
            dx, dy = offsets[p]
            there = chips * ((cols - dy) % cols) + (chips - dx) % chips
            to = device(wrap_x(xpos + dx), 1, wrap_y(col + dy))
            remote(blocks.at[0], blocks.at[there], block_sent.at[kind], block_sem.at[kind, there], to).start()

    def arrived(blocks, kind, p):
        pltpu.make_async_copy(blocks.at[p], blocks.at[p], block_sem.at[kind, p]).wait()

    def all_sent(blocks, kind):
        sent = blocks.at[pl.ds(1, places - 1)]
        pltpu.make_async_copy(sent, sent, block_sent.at[kind]).wait()

    def product(lhs_of, layer, gates, order, total=None):
        for p in order:
            rhs = wide([weights[layer, p, g, s] for g in gates for s in range(HALVES)])
            lhs = wide([lhs_of(p, s) for s in range(HALVES)])
            term = jnp.dot(lhs, rhs, preferred_element_type=F32)
            total = term if total is None else total + term
        return total

    def gathered(blocks, kind, layer, gate):
        total = None
        for group in groups:
            for p in group:
                if p:
                    arrived(blocks, kind, p)
            total = product(lambda p, s: blocks[p, s], layer, (gate,), group, total)
        return total

    def project(layer, lhs_of, bias):
        total = product(lhs_of, layer, (RESET, UPDATE, CAND), range(places))
        for g in range(3):
            for s in range(HALVES):
                n = g * HALVES + s
                here = bias[pl.ds(g, 1), pl.ds(pl.multiple_of(xpos * chunk + s * half, half), half)]
                projections[layer, g, s] = total[:, n * half : (n + 1) * half] + here

    def reset_half(layer, blocks, kind, out_blocks, send):
        total = gathered(blocks, kind, layer, REC_RESET)
        for s in range(HALVES):
            reset = jax.nn.sigmoid(projections[layer, RESET, s] + total[:, s * half : (s + 1) * half])
            out_blocks[0, s] = (reset * states[layer, s]).astype(BF16)
        send()
        total = product(lambda p, s: blocks[p, s], layer, (REC_UPDATE,), range(places))
        for s in range(HALVES):
            updates[layer, s] = jax.nn.sigmoid(projections[layer, UPDATE, s] + total[:, s * half : (s + 1) * half])

    def next_half(layer, blocks, kind, emit):
        total = gathered(blocks, kind, layer, REC_CAND)
        for s in range(HALVES):
            candidate = jnp.tanh(projections[layer, CAND, s] + total[:, s * half : (s + 1) * half])
            update = updates[layer, s]
            state = (1.0 - update) * candidate + update * states[layer, s]
            emit(s, state.astype(BF16))
            states[layer, s] = state

    H1, R1, H2, R2 = range(4)

    def first_reset(t):
        slot = h1_blocks.at[lax.rem(t, 2)]
        reset_half(0, slot, H1, r1_blocks, lambda: spread(r1_blocks, R1))
        all_sent(slot, H1)

    def first_next(t):
        slot = h1_blocks.at[lax.rem(t + 1, 2)]

        def emit(s, value):
            slot[0, s] = value

        next_half(0, r1_blocks, R1, emit)
        spread(slot, H1)
        all_sent(r1_blocks, R1)

    def first_inputs(t):
        for n in range(chips):
            part = first_parts.at[t, n]
            pltpu.make_async_copy(part, part, parts_sem.at[t, n]).wait()
        for g in range(3):
            for s in range(HALVES):
                here = b1[pl.ds(g, 1), pl.ds(pl.multiple_of(xpos * chunk + s * half, half), half)]
                projections[0, g, s] = sum(first_parts[t, n, g, s] for n in range(chips)) + here

    def second_inputs(t):
        slot = h1_blocks.at[lax.rem(t, 2)]
        project(1, lambda p, s: slot[p, s], b2)

    def second_reset(t):
        slot = h2_blocks.at[lax.rem(t, 2)]
        reset_half(1, slot, H2, r2_blocks, lambda: spread(r2_blocks, R2))
        all_sent(slot, H2)

    def second_next(t, last):
        slot = h2_blocks.at[lax.rem(t + 1, 2)]

        def emit(s, value):
            seq_halves[s, t] = value
            if not last:
                slot[0, s] = value

        next_half(1, r2_blocks, R2, emit)
        if not last:
            spread(slot, H2)
        all_sent(r2_blocks, R2)

    @pl.when(core == 1)
    def _():
        for s in range(HALVES):
            part = state_in.at[:, s]
            pltpu.make_async_copy(part, part, state_sem.at[s]).wait()
        for layer in range(2):
            for s in range(HALVES):
                states[layer, s] = state_in[layer, s]
        for s in range(HALVES):
            h1_blocks[0, 0, s] = state_in[0, s].astype(BF16)
            h2_blocks[0, 0, s] = state_in[1, s].astype(BF16)
        spread(h1_blocks.at[0], H1)
        spread(h2_blocks.at[0], H2)
        split_pairs(0)
        weights_arrived(WN, 0)
        first_inputs(0)
        first_reset(0)
        first_next(0)
        first_inputs(1)
        split_pairs(1)
        weights_arrived(WX, 1)

        def step(t, first):
            first_reset(t)
            second_inputs(t)
            second_reset(t - 1)
            first_next(t)
            if first:
                weights_arrived(WN, 1)
            second_next(t - 1, False)
            pl.when(t + 1 < steps)(lambda: first_inputs(t + 1))

        def later_step(t, carry):
            step(t, False)
            return carry

        step(1, True)
        lax.fori_loop(2, steps, later_step, 0)
        last_slot = h1_blocks.at[steps % 2]
        for p in range(1, places):
            arrived(last_slot, H1, p)
        all_sent(last_slot, H1)
        second_inputs(steps)
        second_reset(steps - 1)
        before, at_end = pl.ds(0, steps - 1), steps - 1
        beside = device(xpos, 0, col)
        early_copy = remote(seq_halves.at[0, before], seq_out.at[before], out_sent.at[2], out_sem.at[2], beside)
        early_copy.start()
        seq_out[before] = seq_halves[1, before]
        second_next(at_end, True)
        for layer in range(2):
            for s in range(HALVES):
                last_halves[s, layer] = states[layer, s]
        seq_copy = remote(seq_halves.at[0, at_end], seq_out.at[at_end], out_sent.at[0], out_sem.at[0], beside)
        last_copy = remote(last_halves.at[0], last_out, out_sent.at[1], out_sem.at[1], beside)
        seq_copy.start()
        last_copy.start()
        seq_out[at_end] = seq_halves[1, at_end]
        last_out[...] = last_halves[1]
        early_copy.wait_send()
        seq_copy.wait_send()
        last_copy.wait_send()

    @pl.when(core == 0)
    def _():
        def later_first(t, carry):
            make_first(t, True)
            return carry

        lax.fori_loop(EARLY, steps, later_first, 0)
        for part, n in ((seq_out.at[pl.ds(0, steps - 1)], 2), (seq_out.at[steps - 1], 0)):
            pltpu.make_async_copy(part, part, out_sem.at[n]).wait()
        pltpu.make_async_copy(last_out, last_out, out_sem.at[1]).wait()

    drain_sends()


def pass_on(seq_ref, last_ref, seq_out, last_out):
    seq_out[...] = seq_ref[...]
    last_out[...] = last_ref[...]


def solution(mesh):
    rows, cols = mesh.shape["row"], mesh.shape["col"]
    chips = rows // CORES
    places = chips * cols

    def device_body(x_rows, h_rows, wx_l1, whru_l1, whn_l1, bias_l1, wx_l2, whru_l2, whn_l2, bias_l2):
        steps, batch, row_block = x_rows.shape
        col_block = wx_l1.shape[2]
        half = col_block // rows
        chunk = HALVES * half
        anywhere = pl.BlockSpec(memory_space=pl.ANY)
        vmem = pl.BlockSpec(memory_space=pltpu.VMEM)
        dma = pltpu.SemaphoreType.DMA
        kinds = 4
        block = (HALVES, batch, half)
        scratch = [
            pltpu.VMEM((2, places, GATES, HALVES, chunk, half), BF16),
            pltpu.VMEM((2, places, HALVES, chunk, 2, half), BF16),
            pltpu.VMEM((2 * CORES, steps, *block), BF16),
            pltpu.VMEM((2, chips, 3, *block), F32),
            pltpu.VMEM((steps, chips, 3, *block), F32),
            pltpu.VMEM((2, *block), F32),
            pltpu.VMEM((2, places, *block), BF16),
            pltpu.VMEM((places, *block), BF16),
            pltpu.VMEM((2, places, *block), BF16),
            pltpu.VMEM((places, *block), BF16),
            pltpu.VMEM((2, *block), F32),
            pltpu.VMEM((2, *block), F32),
            pltpu.VMEM((2, 3, *block), F32),
            pltpu.VMEM((HALVES, steps, batch, half), BF16),
            pltpu.VMEM((HALVES, 2, batch, half), F32),
            pltpu.VMEM((3, col_block), F32),
            pltpu.VMEM((3, col_block), F32),
            dma((2, 3, places)),
            dma((3, chips, 2)),
            dma((2 * CORES,)),
            dma((chips, 2 * CORES)),
            dma((steps, chips)),
            dma((HALVES,)),
            dma((2, 3, chips, 2)),
            dma((3, chips, 2)),
            dma((2,)),
            dma((chips, 2)),
            dma((2, chips)),
            dma((2, HALVES)),
            dma((kinds, places)),
            dma((kinds,)),
            dma((3,)),
            dma((3,)),
            dma((2,)),
        ]
        out_shape = (
            jax.ShapeDtypeStruct((steps, batch, half), BF16),
            jax.ShapeDtypeStruct((2, batch, half), F32),
        )
        results = pl.pallas_call(
            functools.partial(gru_kernel, rows, cols),
            name="gru",
            out_shape=out_shape,
            in_specs=[anywhere] * 10,
            out_specs=(vmem, vmem),
            scratch_shapes=scratch,
            compiler_params=pltpu.CompilerParams(
                collective_id=0, has_side_effects=True, vmem_limit_bytes=60 * 1024 * 1024
            ),
        )(
            x_rows, h_rows,
            jnp.transpose(wx_l1, (1, 0, 2)), whru_l1, whn_l1, bias_l1,
            jnp.transpose(wx_l2, (1, 0, 2)), whru_l2, whn_l2, bias_l2,
        )
        return pl.pallas_call(pass_on, name="results", out_shape=out_shape, in_specs=[vmem] * 2, out_specs=(vmem, vmem))(*results)

    seq_spec = P(None, "data", "row")
    out_spec = P(None, "data", ("col", "row"))
    wide_spec = P("row", None, "col")
    square_spec = P("row", "col")
    bias_spec = P(None, "col")
    return jax.shard_map(
        device_body,
        mesh=mesh,
        in_specs=(seq_spec, seq_spec, wide_spec, wide_spec, square_spec, bias_spec, wide_spec, wide_spec, square_spec, bias_spec),
        out_specs=(out_spec, out_spec),
        check_vma=False,
    )
```

```python
import functools

import jax
import jax.numpy as jnp
from jax import lax
from jax.experimental import pallas as pl
from jax.experimental.pallas import tpu as pltpu
from jax.sharding import PartitionSpec as P

MESH = pl.DeviceIdType.MESH
F32 = jnp.float32
BF16 = jnp.bfloat16
HALVES = 2
CORES = 2
RESET, UPDATE, CAND, REC_CAND, REC_RESET, REC_UPDATE = range(6)
GATES = 6
PAIR, WX, WN = range(3)
EARLY = 2


def ring_distance(offset, count):
    return min(offset, count - offset)


def gru_kernel(
    rows, cols,
    x_ref, h_ref, wx1, wru1, wn1, b1_ref, wx2, wru2, wn2, b2_ref,
    seq_out, last_out,
    weights, pairs, x_here, first_made, first_parts, state_in,
    h1_blocks, r1_blocks, h2_blocks, r2_blocks,
    states, updates, projections, seq_halves, last_halves, b1, b2,
    weight_sem, hand_sem, x_sem, wide_sem, parts_sem, state_sem,
    weight_sent, handed_sent, x_sent, wide_sent, made_sent, state_sent,
    block_sem, block_sent, out_sem, out_sent, bias_sem,
):
    chips = rows // CORES
    steps, batch, half = seq_out.shape
    chunk = HALVES * half
    places = chips * cols
    row, col = lax.axis_index("row"), lax.axis_index("col")
    xpos, core = row // CORES, row % CORES
    layers = ((wx1, wru1, wn1), (wx2, wru2, wn2))

    def device(x, c, y):
        return {"row": CORES * x + c, "col": y}

    def wrap_x(v):
        return lax.rem(v + 2 * chips, chips)

    def wrap_y(v):
        return lax.rem(v + 2 * cols, cols)

    def place_of(x_from, y_from, x_to, y_to):
        return chips * wrap_y(y_from - y_to) + wrap_x(x_from - x_to)

    for n, (src, dst) in enumerate(((b1_ref, b1), (b2_ref, b2))):
        pltpu.make_async_copy(src, dst, bias_sem.at[n]).start()

    barrier = pltpu.get_barrier_semaphore()
    for k in range(1, rows * cols):
        other = {"row": lax.rem(row + k % rows, rows), "col": lax.rem(col + k // rows, cols)}
        pl.semaphore_signal(barrier, inc=1, device_id=other, device_id_type=MESH)
    pl.semaphore_wait(barrier, rows * cols - 1)

    def remote(src, dst, send, recv, to):
        return pltpu.make_async_remote_copy(
            src_ref=src, dst_ref=dst, send_sem=send, recv_sem=recv, device_id=to, device_id_type=MESH
        )

    def chunk_place(c, j, x_from, x_to, y_to):
        return place_of(HALVES * c + j, x_from, x_to, y_to)

    def room(part, layer, index):
        if part == PAIR:
            return pairs.at[layer, index]
        return weights.at[layer, index, pl.ds(0, 3)] if part == WX else weights.at[layer, index, REC_CAND]

    def pieces(part, layer, j, x_to, index):
        depth = pl.ds(j * chunk, chunk)
        dst = room(part, layer, index)
        wx, wru, wn = layers[layer]
        for s in range(HALVES):
            units = pl.ds(pl.multiple_of(x_to * chunk + s * half, half), half)
            if part == PAIR:
                yield wru.at[depth, :, units], dst.at[s]
            elif part == WX:
                yield wx.at[:, depth, units], dst.at[:, s]
            else:
                yield wn.at[depth, units], dst.at[s]

    moving = ((PAIR, WN), (PAIR, WX, WN))

    def send_part(part, layer, turns):
        for turn in turns:
            x_to = wrap_x(xpos + turn)
            for j in range(2):
                place = chunk_place(core, j, xpos, x_to, col)
                sent, sem = weight_sent.at[layer, part, turn, j], weight_sem.at[layer, part, place]
                for src, dst in pieces(part, layer, j, x_to, place):
                    remote(src, dst, sent, sem, device(x_to, 1, col)).start()

    def keep_weights(layer):
        for part in moving[layer]:
            for j in range(2):
                place = chunk_place(1, j, xpos, xpos, col)
                for src, dst in pieces(part, layer, j, xpos, place):
                    pltpu.make_async_copy(src, dst, weight_sem.at[layer, part, place]).start()

    def hand_over():
        for part in moving[1]:
            for turn in far_turns:
                x_to = wrap_x(xpos + turn)
                for j in range(2):
                    for src, dst in pieces(part, 1, j, x_to, 2 * turn + j):
                        to = device(xpos, 0, col)
                        remote(src, dst, weight_sent.at[1, part, turn, j], hand_sem.at[part, turn, j], to).start()

    def send_handed(part):
        for turn in far_turns:
            x_to = wrap_x(xpos + turn)
            for j in range(2):
                src = room(part, 1, 2 * turn + j)
                pltpu.make_async_copy(src, src, hand_sem.at[part, turn, j]).wait()
                place = chunk_place(1, j, xpos, x_to, col)
                sent, sem = handed_sent.at[part, turn, j], weight_sem.at[1, part, place]
                remote(src, room(part, 1, place), sent, sem, device(x_to, 1, col)).start()

    def weights_arrived(part, layer):
        for p in range(places):
            here = room(part, layer, p)
            pltpu.make_async_copy(here, here, weight_sem.at[layer, part, p]).wait()

    def split_pairs(layer):
        def split(p, carry):
            here = pairs.at[layer, p]
            pltpu.make_async_copy(here, here, weight_sem.at[layer, PAIR, p]).wait()
            for s in range(HALVES):
                both = jnp.swapaxes(here[s], 0, 1)
                weights[layer, p, REC_RESET, s] = both[0]
                weights[layer, p, REC_UPDATE, s] = both[1]
            return carry

        lax.fori_loop(0, places, split, 0)

    def input_copies():
        for j in range(2):
            n = 2 * core + j
            for s in range(HALVES):
                yield x_ref.at[:, :, pl.ds(j * chunk + s * half, half)], x_here.at[n, :, s], x_sent.at[j], x_sem.at[n]
            for turn in range(chips):
                for src, dst in pieces(WX, 0, j, wrap_x(xpos + turn), 2 * CORES * turn + n):
                    yield src, dst, wide_sent.at[turn, j], wide_sem.at[turn, n]

    def keep_inputs():
        for src, dst, _, sem in input_copies():
            pltpu.make_async_copy(src, dst, sem).start()

    def hand_inputs():
        for src, dst, sent, sem in input_copies():
            remote(src, dst, sent, sem, device(xpos, 0, col)).start()

    def inputs_here():
        for n in range(2 * CORES):
            pltpu.make_async_copy(x_here.at[n], x_here.at[n], x_sem.at[n]).wait()
            for turn in range(chips):
                kept = weights.at[0, 2 * CORES * turn + n, pl.ds(0, 3)]
                pltpu.make_async_copy(kept, kept, wide_sem.at[turn, n]).wait()

    def wide(parts):
        return jnp.concatenate(parts, axis=1)

    def make_first(t, again):
        slot = lax.rem(t, 2)
        for turn in (2, 1, chips - 1, 0):
            made = first_made.at[slot, turn]
            if again:
                pltpu.make_async_copy(made, made, made_sent.at[slot, turn]).wait()
            total = None
            for n in range(2 * CORES):
                rhs = wide([weights[0, 2 * CORES * turn + n, g, s] for g in range(3) for s in range(HALVES)])
                lhs = wide([x_here[n, t, s] for s in range(HALVES)])
                term = jnp.dot(lhs, rhs, preferred_element_type=F32)
                total = term if total is None else total + term
            for g in range(3):
                for s in range(HALVES):
                    n = g * HALVES + s
                    made[g, s] = total[:, n * half : (n + 1) * half]
            seen = (chips - turn) % chips
            to = device(wrap_x(xpos + turn), 1, col)
            remote(made, first_parts.at[t, seen], made_sent.at[slot, turn], parts_sem.at[t, seen], to).start()

    far_turns = (2, 1, chips - 1)

    @pl.when(xpos == col)
    def _():
        for j in range(2):
            x_to = HALVES * core + j
            for s in range(HALVES):
                src = h_ref.at[:, :, pl.ds(j * chunk + s * half, half)]
                dst = state_in.at[:, s]
                mine = (x_to == xpos) & (core == 1)

                @pl.when(mine)
                def _():
                    pltpu.make_async_copy(src, dst, state_sem.at[s]).start()

                @pl.when(jnp.logical_not(mine))
                def _():
                    copy = remote(src, dst, state_sent.at[j, s], state_sem.at[s], device(x_to, 1, col))
                    copy.start()
                    copy.wait_send()

    for part in moving[0]:
        send_part(part, 0, far_turns)

    @pl.when(core == 1)
    def _():
        hand_inputs()
        keep_weights(0)
        hand_over()
        keep_weights(1)

    @pl.when(core == 0)
    def _():
        keep_inputs()
        for part in moving[0]:
            send_part(part, 0, (0,))
        inputs_here()
        for t in range(EARLY):
            make_first(t, False)
        for part in moving[1]:
            send_part(part, 1, far_turns)
            send_part(part, 1, (0,))
            send_handed(part)

    for n, dst in enumerate((b1, b2)):
        pltpu.make_async_copy(dst, dst, bias_sem.at[n]).wait()

    def drain_sends():
        for layer in range(2):
            for part in moving[layer]:
                piece = room(part, layer, 0)
                for j in range(2):
                    for turn in far_turns:
                        pltpu.make_async_copy(piece, piece, weight_sent.at[layer, part, turn, j]).wait()

        @pl.when(core == 0)
        def _():
            for layer in range(2):
                for part in moving[layer]:
                    piece = room(part, layer, 0)
                    for j in range(2):
                        pltpu.make_async_copy(piece, piece, weight_sent.at[layer, part, 0, j]).wait()
            for part in moving[1]:
                piece = room(part, 1, 0)
                for j in range(2):
                    for turn in far_turns:
                        pltpu.make_async_copy(piece, piece, handed_sent.at[part, turn, j]).wait()
            for slot in range(2):
                for turn in range(chips):
                    made = first_made.at[slot, turn]
                    pltpu.make_async_copy(made, made, made_sent.at[slot, turn]).wait()

        @pl.when(core == 1)
        def _():
            piece = room(WX, 0, 0)
            for j in range(2):
                pltpu.make_async_copy(x_here.at[0], x_here.at[0], x_sent.at[j]).wait()
                for turn in range(chips):
                    pltpu.make_async_copy(piece, piece, wide_sent.at[turn, j]).wait()

    offsets = [(dx, dy) for dy in range(cols) for dx in range(chips)]
    distance = [ring_distance(dx, chips) + ring_distance(dy, cols) for dx, dy in offsets]
    far_first = sorted(range(1, places), key=lambda p: -distance[p])
    by_arrival = sorted(range(places), key=lambda p: (distance[p], ring_distance(offsets[p][0], chips)))
    groups = [by_arrival[:6], by_arrival[6:10], by_arrival[10:14], by_arrival[14:]]

    def spread(blocks, kind):
        for p in far_first:
            dx, dy = offsets[p]
            there = chips * ((cols - dy) % cols) + (chips - dx) % chips
            to = device(wrap_x(xpos + dx), 1, wrap_y(col + dy))
            remote(blocks.at[0], blocks.at[there], block_sent.at[kind], block_sem.at[kind, there], to).start()

    def arrived(blocks, kind, p):
        pltpu.make_async_copy(blocks.at[p], blocks.at[p], block_sem.at[kind, p]).wait()

    def all_sent(blocks, kind):
        sent = blocks.at[pl.ds(1, places - 1)]
        pltpu.make_async_copy(sent, sent, block_sent.at[kind]).wait()

    def product(lhs_of, layer, gates, order, total=None):
        for p in order:
            rhs = wide([weights[layer, p, g, s] for g in gates for s in range(HALVES)])
            lhs = wide([lhs_of(p, s) for s in range(HALVES)])
            term = jnp.dot(lhs, rhs, preferred_element_type=F32)
            total = term if total is None else total + term
        return total

    def gathered(blocks, kind, layer, gate):
        total = None
        for group in groups:
            for p in group:
                if p:
                    arrived(blocks, kind, p)
            total = product(lambda p, s: blocks[p, s], layer, (gate,), group, total)
        return total

    def project(layer, lhs_of, bias):
        total = product(lhs_of, layer, (RESET, UPDATE, CAND), range(places))
        for g in range(3):
            for s in range(HALVES):
                n = g * HALVES + s
                here = bias[pl.ds(g, 1), pl.ds(pl.multiple_of(xpos * chunk + s * half, half), half)]
                projections[layer, g, s] = total[:, n * half : (n + 1) * half] + here

    def reset_half(layer, blocks, kind, out_blocks, send):
        total = gathered(blocks, kind, layer, REC_RESET)
        for s in range(HALVES):
            reset = jax.nn.sigmoid(projections[layer, RESET, s] + total[:, s * half : (s + 1) * half])
            out_blocks[0, s] = (reset * states[layer, s]).astype(BF16)
        send()
        total = product(lambda p, s: blocks[p, s], layer, (REC_UPDATE,), range(places))
        for s in range(HALVES):
            updates[layer, s] = jax.nn.sigmoid(projections[layer, UPDATE, s] + total[:, s * half : (s + 1) * half])

    def next_half(layer, blocks, kind, emit):
        total = gathered(blocks, kind, layer, REC_CAND)
        for s in range(HALVES):
            candidate = jnp.tanh(projections[layer, CAND, s] + total[:, s * half : (s + 1) * half])
            update = updates[layer, s]
            state = (1.0 - update) * candidate + update * states[layer, s]
            emit(s, state.astype(BF16))
            states[layer, s] = state

    H1, R1, H2, R2 = range(4)

    def first_reset(t):
        slot = h1_blocks.at[lax.rem(t, 2)]
        reset_half(0, slot, H1, r1_blocks, lambda: spread(r1_blocks, R1))
        all_sent(slot, H1)

    def first_next(t):
        slot = h1_blocks.at[lax.rem(t + 1, 2)]

        def emit(s, value):
            slot[0, s] = value

        next_half(0, r1_blocks, R1, emit)
        spread(slot, H1)
        all_sent(r1_blocks, R1)

    def first_inputs(t):
        for n in range(chips):
            part = first_parts.at[t, n]
            pltpu.make_async_copy(part, part, parts_sem.at[t, n]).wait()
        for g in range(3):
            for s in range(HALVES):
                here = b1[pl.ds(g, 1), pl.ds(pl.multiple_of(xpos * chunk + s * half, half), half)]
                projections[0, g, s] = sum(first_parts[t, n, g, s] for n in range(chips)) + here

    def second_inputs(t):
        slot = h1_blocks.at[lax.rem(t, 2)]
        project(1, lambda p, s: slot[p, s], b2)

    def second_reset(t):
        slot = h2_blocks.at[lax.rem(t, 2)]
        reset_half(1, slot, H2, r2_blocks, lambda: spread(r2_blocks, R2))
        all_sent(slot, H2)

    def second_next(t, last):
        slot = h2_blocks.at[lax.rem(t + 1, 2)]

        def emit(s, value):
            seq_halves[s, t] = value
            if not last:
                slot[0, s] = value

        next_half(1, r2_blocks, R2, emit)
        if not last:
            spread(slot, H2)
        all_sent(r2_blocks, R2)

    @pl.when(core == 1)
    def _():
        for s in range(HALVES):
            part = state_in.at[:, s]
            pltpu.make_async_copy(part, part, state_sem.at[s]).wait()
        for layer in range(2):
            for s in range(HALVES):
                states[layer, s] = state_in[layer, s]
        for s in range(HALVES):
            h1_blocks[0, 0, s] = state_in[0, s].astype(BF16)
            h2_blocks[0, 0, s] = state_in[1, s].astype(BF16)
        spread(h1_blocks.at[0], H1)
        spread(h2_blocks.at[0], H2)
        split_pairs(0)
        weights_arrived(WN, 0)
        first_inputs(0)
        first_reset(0)
        first_next(0)
        first_inputs(1)
        def step(t, first):
            first_reset(t)
            if first:
                split_pairs(1)
                weights_arrived(WX, 1)
            second_inputs(t)
            second_reset(t - 1)
            first_next(t)
            if first:
                weights_arrived(WN, 1)
            second_next(t - 1, False)
            pl.when(t + 1 < steps)(lambda: first_inputs(t + 1))

        def later_step(t, carry):
            step(t, False)
            return carry

        step(1, True)
        lax.fori_loop(2, steps, later_step, 0)
        last_slot = h1_blocks.at[steps % 2]
        for p in range(1, places):
            arrived(last_slot, H1, p)
        all_sent(last_slot, H1)
        second_inputs(steps)
        second_reset(steps - 1)
        before, at_end = pl.ds(0, steps - 1), steps - 1
        beside = device(xpos, 0, col)
        early_copy = remote(seq_halves.at[0, before], seq_out.at[before], out_sent.at[2], out_sem.at[2], beside)
        early_copy.start()
        seq_out[before] = seq_halves[1, before]
        second_next(at_end, True)
        for layer in range(2):
            for s in range(HALVES):
                last_halves[s, layer] = states[layer, s]
        seq_copy = remote(seq_halves.at[0, at_end], seq_out.at[at_end], out_sent.at[0], out_sem.at[0], beside)
        last_copy = remote(last_halves.at[0], last_out, out_sent.at[1], out_sem.at[1], beside)
        seq_copy.start()
        last_copy.start()
        seq_out[at_end] = seq_halves[1, at_end]
        last_out[...] = last_halves[1]
        early_copy.wait_send()
        seq_copy.wait_send()
        last_copy.wait_send()

    @pl.when(core == 0)
    def _():
        def later_first(t, carry):
            make_first(t, True)
            return carry

        lax.fori_loop(EARLY, steps, later_first, 0)
        for part, n in ((seq_out.at[pl.ds(0, steps - 1)], 2), (seq_out.at[steps - 1], 0)):
            pltpu.make_async_copy(part, part, out_sem.at[n]).wait()
        pltpu.make_async_copy(last_out, last_out, out_sem.at[1]).wait()

    drain_sends()


def pass_on(seq_ref, last_ref, seq_out, last_out):
    seq_out[...] = seq_ref[...]
    last_out[...] = last_ref[...]


def solution(mesh):
    rows, cols = mesh.shape["row"], mesh.shape["col"]
    chips = rows // CORES
    places = chips * cols

    def device_body(x_rows, h_rows, wx_l1, whru_l1, whn_l1, bias_l1, wx_l2, whru_l2, whn_l2, bias_l2):
        steps, batch, row_block = x_rows.shape
        col_block = wx_l1.shape[2]
        half = col_block // rows
        chunk = HALVES * half
        anywhere = pl.BlockSpec(memory_space=pl.ANY)
        vmem = pl.BlockSpec(memory_space=pltpu.VMEM)
        dma = pltpu.SemaphoreType.DMA
        kinds = 4
        block = (HALVES, batch, half)
        scratch = [
            pltpu.VMEM((2, places, GATES, HALVES, chunk, half), BF16),
            pltpu.VMEM((2, places, HALVES, chunk, 2, half), BF16),
            pltpu.VMEM((2 * CORES, steps, *block), BF16),
            pltpu.VMEM((2, chips, 3, *block), F32),
            pltpu.VMEM((steps, chips, 3, *block), F32),
            pltpu.VMEM((2, *block), F32),
            pltpu.VMEM((2, places, *block), BF16),
            pltpu.VMEM((places, *block), BF16),
            pltpu.VMEM((2, places, *block), BF16),
            pltpu.VMEM((places, *block), BF16),
            pltpu.VMEM((2, *block), F32),
            pltpu.VMEM((2, *block), F32),
            pltpu.VMEM((2, 3, *block), F32),
            pltpu.VMEM((HALVES, steps, batch, half), BF16),
            pltpu.VMEM((HALVES, 2, batch, half), F32),
            pltpu.VMEM((3, col_block), F32),
            pltpu.VMEM((3, col_block), F32),
            dma((2, 3, places)),
            dma((3, chips, 2)),
            dma((2 * CORES,)),
            dma((chips, 2 * CORES)),
            dma((steps, chips)),
            dma((HALVES,)),
            dma((2, 3, chips, 2)),
            dma((3, chips, 2)),
            dma((2,)),
            dma((chips, 2)),
            dma((2, chips)),
            dma((2, HALVES)),
            dma((kinds, places)),
            dma((kinds,)),
            dma((3,)),
            dma((3,)),
            dma((2,)),
        ]
        out_shape = (
            jax.ShapeDtypeStruct((steps, batch, half), BF16),
            jax.ShapeDtypeStruct((2, batch, half), F32),
        )
        results = pl.pallas_call(
            functools.partial(gru_kernel, rows, cols),
            name="gru",
            out_shape=out_shape,
            in_specs=[anywhere] * 10,
            out_specs=(vmem, vmem),
            scratch_shapes=scratch,
            compiler_params=pltpu.CompilerParams(
                collective_id=0, has_side_effects=True, vmem_limit_bytes=60 * 1024 * 1024
            ),
        )(
            x_rows, h_rows,
            jnp.transpose(wx_l1, (1, 0, 2)), whru_l1, whn_l1, bias_l1,
            jnp.transpose(wx_l2, (1, 0, 2)), whru_l2, whn_l2, bias_l2,
        )
        return pl.pallas_call(pass_on, name="results", out_shape=out_shape, in_specs=[vmem] * 2, out_specs=(vmem, vmem))(*results)

    seq_spec = P(None, "data", "row")
    out_spec = P(None, "data", ("col", "row"))
    wide_spec = P("row", None, "col")
    square_spec = P("row", "col")
    bias_spec = P(None, "col")
    return jax.shard_map(
        device_body,
        mesh=mesh,
        in_specs=(seq_spec, seq_spec, wide_spec, wide_spec, square_spec, bias_spec, wide_spec, wide_spec, square_spec, bias_spec),
        out_specs=(out_spec, out_spec),
        check_vma=False,
    )
```

```python
import functools

import jax
import jax.numpy as jnp
from jax import lax
from jax.experimental import pallas as pl
from jax.experimental.pallas import tpu as pltpu
from jax.sharding import PartitionSpec as P

MESH = pl.DeviceIdType.MESH
F32 = jnp.float32
BF16 = jnp.bfloat16
HALVES = 2
CORES = 2
RESET, UPDATE, CAND, REC_CAND, REC_RESET, REC_UPDATE = range(6)
GATES = 6
PAIR, WX, WN = range(3)
EARLY = 2


def ring_distance(offset, count):
    return min(offset, count - offset)


def gru_kernel(
    rows, cols,
    x_ref, h_ref, wx1, wru1, wn1, b1_ref, wx2, wru2, wn2, b2_ref,
    seq_out, last_out,
    weights, pairs, x_here, first_made, first_passed, first_parts, state_in,
    h1_blocks, r1_blocks, h2_blocks, r2_blocks,
    states, updates, projections, seq_halves, last_halves, b1, b2,
    weight_sem, hand_sem, x_sem, wide_sem, passed_sem, parts_sem, state_sem,
    weight_sent, handed_sent, x_sent, wide_sent, made_sent, state_sent,
    block_sem, block_sent, out_sem, out_sent, bias_sem,
):
    chips = rows // CORES
    steps, batch, half = seq_out.shape
    chunk = HALVES * half
    places = chips * cols
    row, col = lax.axis_index("row"), lax.axis_index("col")
    xpos, core = row // CORES, row % CORES
    layers = ((wx1, wru1, wn1), (wx2, wru2, wn2))

    def device(x, c, y):
        return {"row": CORES * x + c, "col": y}

    def wrap_x(v):
        return lax.rem(v + 2 * chips, chips)

    def wrap_y(v):
        return lax.rem(v + 2 * cols, cols)

    def place_of(x_from, y_from, x_to, y_to):
        return chips * wrap_y(y_from - y_to) + wrap_x(x_from - x_to)

    for n, (src, dst) in enumerate(((b1_ref, b1), (b2_ref, b2))):
        pltpu.make_async_copy(src, dst, bias_sem.at[n]).start()

    barrier = pltpu.get_barrier_semaphore()
    for k in range(1, rows * cols):
        other = {"row": lax.rem(row + k % rows, rows), "col": lax.rem(col + k // rows, cols)}
        pl.semaphore_signal(barrier, inc=1, device_id=other, device_id_type=MESH)
    pl.semaphore_wait(barrier, rows * cols - 1)

    def remote(src, dst, send, recv, to):
        return pltpu.make_async_remote_copy(
            src_ref=src, dst_ref=dst, send_sem=send, recv_sem=recv, device_id=to, device_id_type=MESH
        )

    def chunk_place(c, j, x_from, x_to, y_to):
        return place_of(HALVES * c + j, x_from, x_to, y_to)

    def room(part, layer, index):
        if part == PAIR:
            return pairs.at[layer, index]
        return weights.at[layer, index, pl.ds(0, 3)] if part == WX else weights.at[layer, index, REC_CAND]

    def pieces(part, layer, j, x_to, index):
        depth = pl.ds(j * chunk, chunk)
        dst = room(part, layer, index)
        wx, wru, wn = layers[layer]
        for s in range(HALVES):
            units = pl.ds(pl.multiple_of(x_to * chunk + s * half, half), half)
            if part == PAIR:
                yield wru.at[depth, :, units], dst.at[s]
            elif part == WX:
                yield wx.at[:, depth, units], dst.at[:, s]
            else:
                yield wn.at[depth, units], dst.at[s]

    moving = ((PAIR, WN), (PAIR, WX, WN))

    def send_part(part, layer, turns):
        for turn in turns:
            x_to = wrap_x(xpos + turn)
            for j in range(2):
                place = chunk_place(core, j, xpos, x_to, col)
                sent, sem = weight_sent.at[layer, part, turn, j], weight_sem.at[layer, part, place]
                for src, dst in pieces(part, layer, j, x_to, place):
                    remote(src, dst, sent, sem, device(x_to, 1, col)).start()

    def keep_weights(layer):
        for part in moving[layer]:
            for j in range(2):
                place = chunk_place(1, j, xpos, xpos, col)
                for src, dst in pieces(part, layer, j, xpos, place):
                    pltpu.make_async_copy(src, dst, weight_sem.at[layer, part, place]).start()

    def hand_over():
        for part in moving[1]:
            for turn in far_turns:
                x_to = wrap_x(xpos + turn)
                for j in range(2):
                    for src, dst in pieces(part, 1, j, x_to, 2 * turn + j):
                        to = device(xpos, 0, col)
                        remote(src, dst, weight_sent.at[1, part, turn, j], hand_sem.at[part, turn, j], to).start()

    def send_handed(part):
        for turn in far_turns:
            x_to = wrap_x(xpos + turn)
            for j in range(2):
                src = room(part, 1, 2 * turn + j)
                pltpu.make_async_copy(src, src, hand_sem.at[part, turn, j]).wait()
                place = chunk_place(1, j, xpos, x_to, col)
                sent, sem = handed_sent.at[part, turn, j], weight_sem.at[1, part, place]
                remote(src, room(part, 1, place), sent, sem, device(x_to, 1, col)).start()

    def weights_arrived(part, layer):
        for p in range(places):
            here = room(part, layer, p)
            pltpu.make_async_copy(here, here, weight_sem.at[layer, part, p]).wait()

    def split_pairs(layer):
        def split(p, carry):
            here = pairs.at[layer, p]
            pltpu.make_async_copy(here, here, weight_sem.at[layer, PAIR, p]).wait()
            for s in range(HALVES):
                both = jnp.swapaxes(here[s], 0, 1)
                weights[layer, p, REC_RESET, s] = both[0]
                weights[layer, p, REC_UPDATE, s] = both[1]
            return carry

        lax.fori_loop(0, places, split, 0)

    def input_copies():
        for j in range(2):
            n = 2 * core + j
            for s in range(HALVES):
                yield x_ref.at[:, :, pl.ds(j * chunk + s * half, half)], x_here.at[n, :, s], x_sent.at[j], x_sem.at[n]
            for turn in range(chips):
                for src, dst in pieces(WX, 0, j, wrap_x(xpos + turn), 2 * CORES * turn + n):
                    yield src, dst, wide_sent.at[turn, j], wide_sem.at[turn, n]

    def keep_inputs():
        for src, dst, _, sem in input_copies():
            pltpu.make_async_copy(src, dst, sem).start()

    def hand_inputs():
        for src, dst, sent, sem in input_copies():
            remote(src, dst, sent, sem, device(xpos, 0, col)).start()

    def inputs_here():
        for n in range(2 * CORES):
            pltpu.make_async_copy(x_here.at[n], x_here.at[n], x_sem.at[n]).wait()
            for turn in range(chips):
                kept = weights.at[0, 2 * CORES * turn + n, pl.ds(0, 3)]
                pltpu.make_async_copy(kept, kept, wide_sem.at[turn, n]).wait()

    def wide(parts):
        return jnp.concatenate(parts, axis=1)

    def make_first(t, way, again):
        onward, other = ((1, chips - 1), (chips - 1, 1))[way]

        def part_of(turn):
            total = None
            for n in range(2 * CORES):
                rhs = wide([weights[0, 2 * CORES * turn + n, g, s] for g in range(3) for s in range(HALVES)])
                lhs = wide([x_here[n, t, s] for s in range(HALVES)])
                term = jnp.dot(lhs, rhs, preferred_element_type=F32)
                total = term if total is None else total + term
            return total

        def emit(turn, passed, dst, sem, to):
            made = first_made.at[way, turn]
            if again:
                pltpu.make_async_copy(made, made, made_sent.at[way, turn]).wait()
            total = part_of(turn)
            if passed is not None:
                pltpu.make_async_copy(passed, passed, passed_sem.at[way]).wait()
            for g in range(3):
                for s in range(HALVES):
                    n = g * HALVES + s
                    value = total[:, n * half : (n + 1) * half]
                    made[g, s] = value if passed is None else value + passed[g, s]
            remote(made, dst, made_sent.at[way, turn], sem, to).start()

        def parts(seen):
            return first_parts.at[t, seen], parts_sem.at[t, seen]

        emit(2, None, first_passed.at[way], passed_sem.at[way], device(wrap_x(xpos + onward), 0, col))
        emit(other, None, *parts(1 - way), device(wrap_x(xpos + other), 1, col))
        emit(onward, first_passed.at[way], *parts(way), device(wrap_x(xpos + onward), 1, col))
        emit(0, None, *parts(2), device(xpos, 1, col))

    far_turns = (2, 1, chips - 1)

    @pl.when(xpos == col)
    def _():
        for j in range(2):
            x_to = HALVES * core + j
            for s in range(HALVES):
                src = h_ref.at[:, :, pl.ds(j * chunk + s * half, half)]
                dst = state_in.at[:, s]
                mine = (x_to == xpos) & (core == 1)

                @pl.when(mine)
                def _():
                    pltpu.make_async_copy(src, dst, state_sem.at[s]).start()

                @pl.when(jnp.logical_not(mine))
                def _():
                    copy = remote(src, dst, state_sent.at[j, s], state_sem.at[s], device(x_to, 1, col))
                    copy.start()
                    copy.wait_send()

    for part in moving[0]:
        send_part(part, 0, far_turns)

    @pl.when(core == 1)
    def _():
        hand_inputs()
        keep_weights(0)
        hand_over()
        keep_weights(1)

    @pl.when(core == 0)
    def _():
        keep_inputs()
        for part in moving[0]:
            send_part(part, 0, (0,))
        inputs_here()
        for t in range(EARLY):
            make_first(t, t % 2, False)
        for part in moving[1]:
            send_part(part, 1, far_turns)
            send_part(part, 1, (0,))
            send_handed(part)

    for n, dst in enumerate((b1, b2)):
        pltpu.make_async_copy(dst, dst, bias_sem.at[n]).wait()

    def drain_sends():
        for layer in range(2):
            for part in moving[layer]:
                piece = room(part, layer, 0)
                for j in range(2):
                    for turn in far_turns:
                        pltpu.make_async_copy(piece, piece, weight_sent.at[layer, part, turn, j]).wait()

        @pl.when(core == 0)
        def _():
            for layer in range(2):
                for part in moving[layer]:
                    piece = room(part, layer, 0)
                    for j in range(2):
                        pltpu.make_async_copy(piece, piece, weight_sent.at[layer, part, 0, j]).wait()
            for part in moving[1]:
                piece = room(part, 1, 0)
                for j in range(2):
                    for turn in far_turns:
                        pltpu.make_async_copy(piece, piece, handed_sent.at[part, turn, j]).wait()
            for slot in range(2):
                for turn in range(chips):
                    made = first_made.at[slot, turn]
                    pltpu.make_async_copy(made, made, made_sent.at[slot, turn]).wait()

        @pl.when(core == 1)
        def _():
            piece = room(WX, 0, 0)
            for j in range(2):
                pltpu.make_async_copy(x_here.at[0], x_here.at[0], x_sent.at[j]).wait()
                for turn in range(chips):
                    pltpu.make_async_copy(piece, piece, wide_sent.at[turn, j]).wait()

    offsets = [(dx, dy) for dy in range(cols) for dx in range(chips)]
    distance = [ring_distance(dx, chips) + ring_distance(dy, cols) for dx, dy in offsets]
    far_first = sorted(range(1, places), key=lambda p: -distance[p])
    by_arrival = sorted(range(places), key=lambda p: (distance[p], ring_distance(offsets[p][0], chips)))
    groups = [by_arrival[:6], by_arrival[6:10], by_arrival[10:]]

    def spread(blocks, kind):
        for p in far_first:
            dx, dy = offsets[p]
            there = chips * ((cols - dy) % cols) + (chips - dx) % chips
            to = device(wrap_x(xpos + dx), 1, wrap_y(col + dy))
            remote(blocks.at[0], blocks.at[there], block_sent.at[kind], block_sem.at[kind, there], to).start()

    def arrived(blocks, kind, p):
        pltpu.make_async_copy(blocks.at[p], blocks.at[p], block_sem.at[kind, p]).wait()

    def all_sent(blocks, kind):
        sent = blocks.at[pl.ds(1, places - 1)]
        pltpu.make_async_copy(sent, sent, block_sent.at[kind]).wait()

    def product(lhs_of, layer, gates, order, total=None):
        for p in order:
            rhs = wide([weights[layer, p, g, s] for g in gates for s in range(HALVES)])
            lhs = wide([lhs_of(p, s) for s in range(HALVES)])
            term = jnp.dot(lhs, rhs, preferred_element_type=F32)
            total = term if total is None else total + term
        return total

    def gathered(blocks, kind, layer, gate):
        total = None
        for group in groups:
            for p in group:
                if p:
                    arrived(blocks, kind, p)
            total = product(lambda p, s: blocks[p, s], layer, (gate,), group, total)
        return total

    def project(layer, lhs_of, bias):
        total = product(lhs_of, layer, (RESET, UPDATE, CAND), range(places))
        for g in range(3):
            for s in range(HALVES):
                n = g * HALVES + s
                here = bias[pl.ds(g, 1), pl.ds(pl.multiple_of(xpos * chunk + s * half, half), half)]
                projections[layer, g, s] = total[:, n * half : (n + 1) * half] + here

    def reset_half(layer, blocks, kind, out_blocks, send):
        total = gathered(blocks, kind, layer, REC_RESET)
        for s in range(HALVES):
            reset = jax.nn.sigmoid(projections[layer, RESET, s] + total[:, s * half : (s + 1) * half])
            out_blocks[0, s] = (reset * states[layer, s]).astype(BF16)
        send()
        total = product(lambda p, s: blocks[p, s], layer, (REC_UPDATE,), range(places))
        for s in range(HALVES):
            updates[layer, s] = jax.nn.sigmoid(projections[layer, UPDATE, s] + total[:, s * half : (s + 1) * half])

    def next_half(layer, blocks, kind, emit):
        total = gathered(blocks, kind, layer, REC_CAND)
        for s in range(HALVES):
            candidate = jnp.tanh(projections[layer, CAND, s] + total[:, s * half : (s + 1) * half])
            update = updates[layer, s]
            state = (1.0 - update) * candidate + update * states[layer, s]
            emit(s, state.astype(BF16))
            states[layer, s] = state

    H1, R1, H2, R2 = range(4)

    def first_reset(t):
        slot = h1_blocks.at[lax.rem(t, 2)]
        reset_half(0, slot, H1, r1_blocks, lambda: spread(r1_blocks, R1))
        all_sent(slot, H1)

    def first_next(t):
        slot = h1_blocks.at[lax.rem(t + 1, 2)]

        def emit(s, value):
            slot[0, s] = value

        next_half(0, r1_blocks, R1, emit)
        spread(slot, H1)
        all_sent(r1_blocks, R1)

    def first_inputs(t):
        for n in range(3):
            part = first_parts.at[t, n]
            pltpu.make_async_copy(part, part, parts_sem.at[t, n]).wait()
        for g in range(3):
            for s in range(HALVES):
                here = b1[pl.ds(g, 1), pl.ds(pl.multiple_of(xpos * chunk + s * half, half), half)]
                projections[0, g, s] = sum(first_parts[t, n, g, s] for n in range(3)) + here

    def second_inputs(t):
        slot = h1_blocks.at[lax.rem(t, 2)]
        project(1, lambda p, s: slot[p, s], b2)

    def second_reset(t):
        slot = h2_blocks.at[lax.rem(t, 2)]
        reset_half(1, slot, H2, r2_blocks, lambda: spread(r2_blocks, R2))
        all_sent(slot, H2)

    def second_next(t, last):
        slot = h2_blocks.at[lax.rem(t + 1, 2)]

        def emit(s, value):
            seq_halves[s, t] = value
            if not last:
                slot[0, s] = value

        next_half(1, r2_blocks, R2, emit)
        if not last:
            spread(slot, H2)
        all_sent(r2_blocks, R2)

    @pl.when(core == 1)
    def _():
        for s in range(HALVES):
            part = state_in.at[:, s]
            pltpu.make_async_copy(part, part, state_sem.at[s]).wait()
        for layer in range(2):
            for s in range(HALVES):
                states[layer, s] = state_in[layer, s]
        for s in range(HALVES):
            h1_blocks[0, 0, s] = state_in[0, s].astype(BF16)
            h2_blocks[0, 0, s] = state_in[1, s].astype(BF16)
        spread(h1_blocks.at[0], H1)
        spread(h2_blocks.at[0], H2)
        split_pairs(0)
        weights_arrived(WN, 0)
        first_inputs(0)
        first_reset(0)
        first_next(0)
        first_inputs(1)
        split_pairs(1)
        weights_arrived(WX, 1)

        def step(t, first):
            first_reset(t)
            second_inputs(t)
            second_reset(t - 1)
            first_next(t)
            if first:
                weights_arrived(WN, 1)
            second_next(t - 1, False)
            pl.when(t + 1 < steps)(lambda: first_inputs(t + 1))

        def later_step(t, carry):
            step(t, False)
            return carry

        step(1, True)
        lax.fori_loop(2, steps, later_step, 0)
        last_slot = h1_blocks.at[steps % 2]
        for p in range(1, places):
            arrived(last_slot, H1, p)
        all_sent(last_slot, H1)
        second_inputs(steps)
        second_reset(steps - 1)
        before, at_end = pl.ds(0, steps - 1), steps - 1
        beside = device(xpos, 0, col)
        early_copy = remote(seq_halves.at[0, before], seq_out.at[before], out_sent.at[2], out_sem.at[2], beside)
        early_copy.start()
        seq_out[before] = seq_halves[1, before]
        second_next(at_end, True)
        for layer in range(2):
            for s in range(HALVES):
                last_halves[s, layer] = states[layer, s]
        seq_copy = remote(seq_halves.at[0, at_end], seq_out.at[at_end], out_sent.at[0], out_sem.at[0], beside)
        last_copy = remote(last_halves.at[0], last_out, out_sent.at[1], out_sem.at[1], beside)
        seq_copy.start()
        last_copy.start()
        seq_out[at_end] = seq_halves[1, at_end]
        last_out[...] = last_halves[1]
        early_copy.wait_send()
        seq_copy.wait_send()
        last_copy.wait_send()

    @pl.when(core == 0)
    def _():
        def later_first(pair, carry):
            for way in range(2):
                make_first(2 * pair + way, way, True)
            return carry

        lax.fori_loop(EARLY // 2, steps // 2, later_first, 0)
        for part, n in ((seq_out.at[pl.ds(0, steps - 1)], 2), (seq_out.at[steps - 1], 0)):
            pltpu.make_async_copy(part, part, out_sem.at[n]).wait()
        pltpu.make_async_copy(last_out, last_out, out_sem.at[1]).wait()

    drain_sends()


def pass_on(seq_ref, last_ref, seq_out, last_out):
    seq_out[...] = seq_ref[...]
    last_out[...] = last_ref[...]


def solution(mesh):
    rows, cols = mesh.shape["row"], mesh.shape["col"]
    chips = rows // CORES
    places = chips * cols

    def device_body(x_rows, h_rows, wx_l1, whru_l1, whn_l1, bias_l1, wx_l2, whru_l2, whn_l2, bias_l2):
        steps, batch, row_block = x_rows.shape
        col_block = wx_l1.shape[2]
        half = col_block // rows
        chunk = HALVES * half
        anywhere = pl.BlockSpec(memory_space=pl.ANY)
        vmem = pl.BlockSpec(memory_space=pltpu.VMEM)
        dma = pltpu.SemaphoreType.DMA
        kinds = 4
        block = (HALVES, batch, half)
        scratch = [
            pltpu.VMEM((2, places, GATES, HALVES, chunk, half), BF16),
            pltpu.VMEM((2, places, HALVES, chunk, 2, half), BF16),
            pltpu.VMEM((2 * CORES, steps, *block), BF16),
            pltpu.VMEM((2, chips, 3, *block), F32),
            pltpu.VMEM((2, 3, *block), F32),
            pltpu.VMEM((steps, 3, 3, *block), F32),
            pltpu.VMEM((2, *block), F32),
            pltpu.VMEM((2, places, *block), BF16),
            pltpu.VMEM((places, *block), BF16),
            pltpu.VMEM((2, places, *block), BF16),
            pltpu.VMEM((places, *block), BF16),
            pltpu.VMEM((2, *block), F32),
            pltpu.VMEM((2, *block), F32),
            pltpu.VMEM((2, 3, *block), F32),
            pltpu.VMEM((HALVES, steps, batch, half), BF16),
            pltpu.VMEM((HALVES, 2, batch, half), F32),
            pltpu.VMEM((3, col_block), F32),
            pltpu.VMEM((3, col_block), F32),
            dma((2, 3, places)),
            dma((3, chips, 2)),
            dma((2 * CORES,)),
            dma((chips, 2 * CORES)),
            dma((2,)),
            dma((steps, 3)),
            dma((HALVES,)),
            dma((2, 3, chips, 2)),
            dma((3, chips, 2)),
            dma((2,)),
            dma((chips, 2)),
            dma((2, chips)),
            dma((2, HALVES)),
            dma((kinds, places)),
            dma((kinds,)),
            dma((3,)),
            dma((3,)),
            dma((2,)),
        ]
        out_shape = (
            jax.ShapeDtypeStruct((steps, batch, half), BF16),
            jax.ShapeDtypeStruct((2, batch, half), F32),
        )
        results = pl.pallas_call(
            functools.partial(gru_kernel, rows, cols),
            name="gru",
            out_shape=out_shape,
            in_specs=[anywhere] * 10,
            out_specs=(vmem, vmem),
            scratch_shapes=scratch,
            compiler_params=pltpu.CompilerParams(
                collective_id=0, has_side_effects=True, vmem_limit_bytes=60 * 1024 * 1024
            ),
        )(
            x_rows, h_rows,
            jnp.transpose(wx_l1, (1, 0, 2)), whru_l1, whn_l1, bias_l1,
            jnp.transpose(wx_l2, (1, 0, 2)), whru_l2, whn_l2, bias_l2,
        )
        return pl.pallas_call(pass_on, name="results", out_shape=out_shape, in_specs=[vmem] * 2, out_specs=(vmem, vmem))(*results)

    seq_spec = P(None, "data", "row")
    out_spec = P(None, "data", ("col", "row"))
    wide_spec = P("row", None, "col")
    square_spec = P("row", "col")
    bias_spec = P(None, "col")
    return jax.shard_map(
        device_body,
        mesh=mesh,
        in_specs=(seq_spec, seq_spec, wide_spec, wide_spec, square_spec, bias_spec, wide_spec, wide_spec, square_spec, bias_spec),
        out_specs=(out_spec, out_spec),
        check_vma=False,
    )
```

```python
import functools

import jax
import jax.numpy as jnp
from jax import lax
from jax.experimental import pallas as pl
from jax.experimental.pallas import tpu as pltpu
from jax.sharding import PartitionSpec as P

MESH = pl.DeviceIdType.MESH
F32 = jnp.float32
BF16 = jnp.bfloat16
HALVES = 2
CORES = 2
RESET, UPDATE, CAND, REC_CAND, REC_RESET, REC_UPDATE = range(6)
GATES = 6
PAIR, WX, WN = range(3)
EARLY = 2


def ring_distance(offset, count):
    return min(offset, count - offset)


def gru_kernel(
    rows, cols,
    x_ref, h_ref, wx1, wru1, wn1, b1_ref, wx2, wru2, wn2, b2_ref,
    seq_out, last_out,
    weights, pairs, x_here, first_made, first_passed, first_parts, state_in,
    h1_blocks, r1_blocks, h2_blocks, r2_blocks,
    states, updates, projections, seq_halves, last_halves, b1, b2,
    weight_sem, hand_sem, x_sem, wide_sem, passed_sem, parts_sem, state_sem,
    weight_sent, handed_sent, x_sent, wide_sent, made_sent, state_sent,
    block_sem, block_sent, out_sem, out_sent, bias_sem,
):
    chips = rows // CORES
    steps, batch, half = seq_out.shape
    chunk = HALVES * half
    places = chips * cols
    row, col = lax.axis_index("row"), lax.axis_index("col")
    xpos, core = row // CORES, row % CORES
    layers = ((wx1, wru1, wn1), (wx2, wru2, wn2))

    def device(x, c, y):
        return {"row": CORES * x + c, "col": y}

    def wrap_x(v):
        return lax.rem(v + 2 * chips, chips)

    def wrap_y(v):
        return lax.rem(v + 2 * cols, cols)

    def place_of(x_from, y_from, x_to, y_to):
        return chips * wrap_y(y_from - y_to) + wrap_x(x_from - x_to)

    for n, (src, dst) in enumerate(((b1_ref, b1), (b2_ref, b2))):
        pltpu.make_async_copy(src, dst, bias_sem.at[n]).start()

    barrier = pltpu.get_barrier_semaphore()
    for k in range(1, rows * cols):
        other = {"row": lax.rem(row + k % rows, rows), "col": lax.rem(col + k // rows, cols)}
        pl.semaphore_signal(barrier, inc=1, device_id=other, device_id_type=MESH)
    pl.semaphore_wait(barrier, rows * cols - 1)

    def remote(src, dst, send, recv, to):
        return pltpu.make_async_remote_copy(
            src_ref=src, dst_ref=dst, send_sem=send, recv_sem=recv, device_id=to, device_id_type=MESH
        )

    def chunk_place(c, j, x_from, x_to, y_to):
        return place_of(HALVES * c + j, x_from, x_to, y_to)

    def room(part, layer, index):
        if part == PAIR:
            return pairs.at[layer, index]
        return weights.at[layer, index, pl.ds(0, 3)] if part == WX else weights.at[layer, index, REC_CAND]

    def pieces(part, layer, j, x_to, index):
        depth = pl.ds(j * chunk, chunk)
        dst = room(part, layer, index)
        wx, wru, wn = layers[layer]
        for s in range(HALVES):
            units = pl.ds(pl.multiple_of(x_to * chunk + s * half, half), half)
            if part == PAIR:
                yield wru.at[depth, :, units], dst.at[s]
            elif part == WX:
                yield wx.at[:, depth, units], dst.at[:, s]
            else:
                yield wn.at[depth, units], dst.at[s]

    moving = ((PAIR, WN), (PAIR, WX, WN))

    def send_part(part, layer, turns):
        for turn in turns:
            x_to = wrap_x(xpos + turn)
            for j in range(2):
                place = chunk_place(core, j, xpos, x_to, col)
                sent, sem = weight_sent.at[layer, part, turn, j], weight_sem.at[layer, part, place]
                for src, dst in pieces(part, layer, j, x_to, place):
                    remote(src, dst, sent, sem, device(x_to, 1, col)).start()

    def keep_weights(layer):
        for part in moving[layer]:
            for j in range(2):
                place = chunk_place(1, j, xpos, xpos, col)
                for src, dst in pieces(part, layer, j, xpos, place):
                    pltpu.make_async_copy(src, dst, weight_sem.at[layer, part, place]).start()

    def hand_over():
        for part in moving[1]:
            for turn in far_turns:
                x_to = wrap_x(xpos + turn)
                for j in range(2):
                    for src, dst in pieces(part, 1, j, x_to, 2 * turn + j):
                        to = device(xpos, 0, col)
                        remote(src, dst, weight_sent.at[1, part, turn, j], hand_sem.at[part, turn, j], to).start()

    def send_handed(part):
        for turn in far_turns:
            x_to = wrap_x(xpos + turn)
            for j in range(2):
                src = room(part, 1, 2 * turn + j)
                pltpu.make_async_copy(src, src, hand_sem.at[part, turn, j]).wait()
                place = chunk_place(1, j, xpos, x_to, col)
                sent, sem = handed_sent.at[part, turn, j], weight_sem.at[1, part, place]
                remote(src, room(part, 1, place), sent, sem, device(x_to, 1, col)).start()

    def weights_arrived(part, layer):
        for p in range(places):
            here = room(part, layer, p)
            pltpu.make_async_copy(here, here, weight_sem.at[layer, part, p]).wait()

    def split_pairs(layer):
        def split(p, carry):
            here = pairs.at[layer, p]
            pltpu.make_async_copy(here, here, weight_sem.at[layer, PAIR, p]).wait()
            for s in range(HALVES):
                both = jnp.swapaxes(here[s], 0, 1)
                weights[layer, p, REC_RESET, s] = both[0]
                weights[layer, p, REC_UPDATE, s] = both[1]
            return carry

        lax.fori_loop(0, places, split, 0)

    def input_copies():
        for j in range(2):
            n = 2 * core + j
            for s in range(HALVES):
                yield x_ref.at[:, :, pl.ds(j * chunk + s * half, half)], x_here.at[n, :, s], x_sent.at[j], x_sem.at[n]
            for turn in range(chips):
                for src, dst in pieces(WX, 0, j, wrap_x(xpos + turn), 2 * CORES * turn + n):
                    yield src, dst, wide_sent.at[turn, j], wide_sem.at[turn, n]

    def keep_inputs():
        for src, dst, _, sem in input_copies():
            pltpu.make_async_copy(src, dst, sem).start()

    def hand_inputs():
        for src, dst, sent, sem in input_copies():
            remote(src, dst, sent, sem, device(xpos, 0, col)).start()

    def inputs_here():
        for n in range(2 * CORES):
            pltpu.make_async_copy(x_here.at[n], x_here.at[n], x_sem.at[n]).wait()
            for turn in range(chips):
                kept = weights.at[0, 2 * CORES * turn + n, pl.ds(0, 3)]
                pltpu.make_async_copy(kept, kept, wide_sem.at[turn, n]).wait()

    def wide(parts):
        return jnp.concatenate(parts, axis=1)

    def make_first(t, way, again):
        onward, other = ((1, chips - 1), (chips - 1, 1))[way]

        def part_of(turn):
            total = None
            for n in range(2 * CORES):
                rhs = wide([weights[0, 2 * CORES * turn + n, g, s] for g in range(3) for s in range(HALVES)])
                lhs = wide([x_here[n, t, s] for s in range(HALVES)])
                term = jnp.dot(lhs, rhs, preferred_element_type=F32)
                total = term if total is None else total + term
            return total

        def emit(turn, passed, dst, sem, to):
            made = first_made.at[way, turn]
            if again:
                pltpu.make_async_copy(made, made, made_sent.at[way, turn]).wait()
            total = part_of(turn)
            if passed is not None:
                pltpu.make_async_copy(passed, passed, passed_sem.at[way]).wait()
            for g in range(3):
                for s in range(HALVES):
                    n = g * HALVES + s
                    value = total[:, n * half : (n + 1) * half]
                    made[g, s] = value if passed is None else value + passed[g, s]
            remote(made, dst, made_sent.at[way, turn], sem, to).start()

        def parts(seen):
            return first_parts.at[t, seen], parts_sem.at[t, seen]

        emit(2, None, first_passed.at[way], passed_sem.at[way], device(wrap_x(xpos + onward), 0, col))
        emit(other, None, *parts(1 - way), device(wrap_x(xpos + other), 1, col))
        emit(onward, first_passed.at[way], *parts(way), device(wrap_x(xpos + onward), 1, col))
        emit(0, None, *parts(2), device(xpos, 1, col))

    far_turns = (2, 1, chips - 1)

    @pl.when(xpos == col)
    def _():
        for j in range(2):
            x_to = HALVES * core + j
            for s in range(HALVES):
                src = h_ref.at[:, :, pl.ds(j * chunk + s * half, half)]
                dst = state_in.at[:, s]
                mine = (x_to == xpos) & (core == 1)

                @pl.when(mine)
                def _():
                    pltpu.make_async_copy(src, dst, state_sem.at[s]).start()

                @pl.when(jnp.logical_not(mine))
                def _():
                    copy = remote(src, dst, state_sent.at[j, s], state_sem.at[s], device(x_to, 1, col))
                    copy.start()
                    copy.wait_send()

    for part in moving[0]:
        send_part(part, 0, far_turns)

    @pl.when(core == 1)
    def _():
        hand_inputs()
        keep_weights(0)
        hand_over()
        keep_weights(1)

    @pl.when(core == 0)
    def _():
        keep_inputs()
        for part in moving[0]:
            send_part(part, 0, (0,))
        inputs_here()
        for t in range(EARLY):
            make_first(t, t % 2, False)
        for part in moving[1]:
            send_part(part, 1, far_turns)
            send_part(part, 1, (0,))
            send_handed(part)

    for n, dst in enumerate((b1, b2)):
        pltpu.make_async_copy(dst, dst, bias_sem.at[n]).wait()

    def drain_sends():
        for layer in range(2):
            for part in moving[layer]:
                piece = room(part, layer, 0)
                for j in range(2):
                    for turn in far_turns:
                        pltpu.make_async_copy(piece, piece, weight_sent.at[layer, part, turn, j]).wait()

        @pl.when(core == 0)
        def _():
            for layer in range(2):
                for part in moving[layer]:
                    piece = room(part, layer, 0)
                    for j in range(2):
                        pltpu.make_async_copy(piece, piece, weight_sent.at[layer, part, 0, j]).wait()
            for part in moving[1]:
                piece = room(part, 1, 0)
                for j in range(2):
                    for turn in far_turns:
                        pltpu.make_async_copy(piece, piece, handed_sent.at[part, turn, j]).wait()
            for slot in range(2):
                for turn in range(chips):
                    made = first_made.at[slot, turn]
                    pltpu.make_async_copy(made, made, made_sent.at[slot, turn]).wait()

        @pl.when(core == 1)
        def _():
            piece = room(WX, 0, 0)
            for j in range(2):
                pltpu.make_async_copy(x_here.at[0], x_here.at[0], x_sent.at[j]).wait()
                for turn in range(chips):
                    pltpu.make_async_copy(piece, piece, wide_sent.at[turn, j]).wait()

    offsets = [(dx, dy) for dy in range(cols) for dx in range(chips)]
    distance = [ring_distance(dx, chips) + ring_distance(dy, cols) for dx, dy in offsets]
    def weight_of(p):
        in_x, in_y = ring_distance(offsets[p][0], chips), ring_distance(offsets[p][1], cols)
        return -distance[p], -in_y if distance[p] > 1 else -in_x

    far_first = sorted(range(1, places), key=weight_of)
    by_arrival = sorted(range(places), key=lambda p: (distance[p], ring_distance(offsets[p][0], chips)))
    groups = [by_arrival[:6], by_arrival[6:10], by_arrival[10:]]

    def spread(blocks, kind):
        for p in far_first:
            dx, dy = offsets[p]
            there = chips * ((cols - dy) % cols) + (chips - dx) % chips
            to = device(wrap_x(xpos + dx), 1, wrap_y(col + dy))
            remote(blocks.at[0], blocks.at[there], block_sent.at[kind], block_sem.at[kind, there], to).start()

    def arrived(blocks, kind, p):
        pltpu.make_async_copy(blocks.at[p], blocks.at[p], block_sem.at[kind, p]).wait()

    def all_sent(blocks, kind):
        sent = blocks.at[pl.ds(1, places - 1)]
        pltpu.make_async_copy(sent, sent, block_sent.at[kind]).wait()

    def product(lhs_of, layer, gates, order, total=None):
        for p in order:
            rhs = wide([weights[layer, p, g, s] for g in gates for s in range(HALVES)])
            lhs = wide([lhs_of(p, s) for s in range(HALVES)])
            term = jnp.dot(lhs, rhs, preferred_element_type=F32)
            total = term if total is None else total + term
        return total

    def gathered(blocks, kind, layer, gate):
        total = None
        for group in groups:
            for p in group:
                if p:
                    arrived(blocks, kind, p)
            total = product(lambda p, s: blocks[p, s], layer, (gate,), group, total)
        return total

    def project(layer, lhs_of, bias):
        total = product(lhs_of, layer, (RESET, UPDATE, CAND), range(places))
        for g in range(3):
            for s in range(HALVES):
                n = g * HALVES + s
                here = bias[pl.ds(g, 1), pl.ds(pl.multiple_of(xpos * chunk + s * half, half), half)]
                projections[layer, g, s] = total[:, n * half : (n + 1) * half] + here

    def reset_half(layer, blocks, kind, out_blocks, send):
        total = gathered(blocks, kind, layer, REC_RESET)
        for s in range(HALVES):
            reset = jax.nn.sigmoid(projections[layer, RESET, s] + total[:, s * half : (s + 1) * half])
            out_blocks[0, s] = (reset * states[layer, s]).astype(BF16)
        send()
        total = product(lambda p, s: blocks[p, s], layer, (REC_UPDATE,), range(places))
        for s in range(HALVES):
            updates[layer, s] = jax.nn.sigmoid(projections[layer, UPDATE, s] + total[:, s * half : (s + 1) * half])

    def next_half(layer, blocks, kind, emit):
        total = gathered(blocks, kind, layer, REC_CAND)
        for s in range(HALVES):
            candidate = jnp.tanh(projections[layer, CAND, s] + total[:, s * half : (s + 1) * half])
            update = updates[layer, s]
            state = (1.0 - update) * candidate + update * states[layer, s]
            emit(s, state.astype(BF16))
            states[layer, s] = state

    H1, R1, H2, R2 = range(4)

    def first_reset(t):
        slot = h1_blocks.at[lax.rem(t, 2)]
        reset_half(0, slot, H1, r1_blocks, lambda: spread(r1_blocks, R1))
        all_sent(slot, H1)

    def first_next(t):
        slot = h1_blocks.at[lax.rem(t + 1, 2)]

        def emit(s, value):
            slot[0, s] = value

        next_half(0, r1_blocks, R1, emit)
        spread(slot, H1)
        all_sent(r1_blocks, R1)

    def first_inputs(t):
        for n in range(3):
            part = first_parts.at[t, n]
            pltpu.make_async_copy(part, part, parts_sem.at[t, n]).wait()
        for g in range(3):
            for s in range(HALVES):
                here = b1[pl.ds(g, 1), pl.ds(pl.multiple_of(xpos * chunk + s * half, half), half)]
                projections[0, g, s] = sum(first_parts[t, n, g, s] for n in range(3)) + here

    def second_inputs(t):
        slot = h1_blocks.at[lax.rem(t, 2)]
        project(1, lambda p, s: slot[p, s], b2)

    def second_reset(t):
        slot = h2_blocks.at[lax.rem(t, 2)]
        reset_half(1, slot, H2, r2_blocks, lambda: spread(r2_blocks, R2))
        all_sent(slot, H2)

    def second_next(t, last):
        slot = h2_blocks.at[lax.rem(t + 1, 2)]

        def emit(s, value):
            seq_halves[s, t] = value
            if not last:
                slot[0, s] = value

        next_half(1, r2_blocks, R2, emit)
        if not last:
            spread(slot, H2)
        all_sent(r2_blocks, R2)

    @pl.when(core == 1)
    def _():
        for s in range(HALVES):
            part = state_in.at[:, s]
            pltpu.make_async_copy(part, part, state_sem.at[s]).wait()
        for layer in range(2):
            for s in range(HALVES):
                states[layer, s] = state_in[layer, s]
        for s in range(HALVES):
            h1_blocks[0, 0, s] = state_in[0, s].astype(BF16)
            h2_blocks[0, 0, s] = state_in[1, s].astype(BF16)
        spread(h1_blocks.at[0], H1)
        spread(h2_blocks.at[0], H2)
        split_pairs(0)
        weights_arrived(WN, 0)
        first_inputs(0)
        first_reset(0)
        first_next(0)
        first_inputs(1)
        split_pairs(1)
        weights_arrived(WX, 1)

        def step(t, first):
            first_reset(t)
            second_inputs(t)
            second_reset(t - 1)
            first_next(t)
            if first:
                weights_arrived(WN, 1)
            second_next(t - 1, False)
            pl.when(t + 1 < steps)(lambda: first_inputs(t + 1))

        def later_step(t, carry):
            step(t, False)
            return carry

        step(1, True)
        lax.fori_loop(2, steps, later_step, 0)
        last_slot = h1_blocks.at[steps % 2]
        for p in range(1, places):
            arrived(last_slot, H1, p)
        all_sent(last_slot, H1)
        second_inputs(steps)
        second_reset(steps - 1)
        before, at_end = pl.ds(0, steps - 1), steps - 1
        beside = device(xpos, 0, col)
        early_copy = remote(seq_halves.at[0, before], seq_out.at[before], out_sent.at[2], out_sem.at[2], beside)
        early_copy.start()
        seq_out[before] = seq_halves[1, before]
        second_next(at_end, True)
        for layer in range(2):
            for s in range(HALVES):
                last_halves[s, layer] = states[layer, s]
        seq_copy = remote(seq_halves.at[0, at_end], seq_out.at[at_end], out_sent.at[0], out_sem.at[0], beside)
        last_copy = remote(last_halves.at[0], last_out, out_sent.at[1], out_sem.at[1], beside)
        seq_copy.start()
        last_copy.start()
        seq_out[at_end] = seq_halves[1, at_end]
        last_out[...] = last_halves[1]
        early_copy.wait_send()
        seq_copy.wait_send()
        last_copy.wait_send()

    @pl.when(core == 0)
    def _():
        def later_first(pair, carry):
            for way in range(2):
                make_first(2 * pair + way, way, True)
            return carry

        lax.fori_loop(EARLY // 2, steps // 2, later_first, 0)
        for part, n in ((seq_out.at[pl.ds(0, steps - 1)], 2), (seq_out.at[steps - 1], 0)):
            pltpu.make_async_copy(part, part, out_sem.at[n]).wait()
        pltpu.make_async_copy(last_out, last_out, out_sem.at[1]).wait()

    drain_sends()


def pass_on(seq_ref, last_ref, seq_out, last_out):
    seq_out[...] = seq_ref[...]
    last_out[...] = last_ref[...]


def solution(mesh):
    rows, cols = mesh.shape["row"], mesh.shape["col"]
    chips = rows // CORES
    places = chips * cols

    def device_body(x_rows, h_rows, wx_l1, whru_l1, whn_l1, bias_l1, wx_l2, whru_l2, whn_l2, bias_l2):
        steps, batch, row_block = x_rows.shape
        col_block = wx_l1.shape[2]
        half = col_block // rows
        chunk = HALVES * half
        anywhere = pl.BlockSpec(memory_space=pl.ANY)
        vmem = pl.BlockSpec(memory_space=pltpu.VMEM)
        dma = pltpu.SemaphoreType.DMA
        kinds = 4
        block = (HALVES, batch, half)
        scratch = [
            pltpu.VMEM((2, places, GATES, HALVES, chunk, half), BF16),
            pltpu.VMEM((2, places, HALVES, chunk, 2, half), BF16),
            pltpu.VMEM((2 * CORES, steps, *block), BF16),
            pltpu.VMEM((2, chips, 3, *block), F32),
            pltpu.VMEM((2, 3, *block), F32),
            pltpu.VMEM((steps, 3, 3, *block), F32),
            pltpu.VMEM((2, *block), F32),
            pltpu.VMEM((2, places, *block), BF16),
            pltpu.VMEM((places, *block), BF16),
            pltpu.VMEM((2, places, *block), BF16),
            pltpu.VMEM((places, *block), BF16),
            pltpu.VMEM((2, *block), F32),
            pltpu.VMEM((2, *block), F32),
            pltpu.VMEM((2, 3, *block), F32),
            pltpu.VMEM((HALVES, steps, batch, half), BF16),
            pltpu.VMEM((HALVES, 2, batch, half), F32),
            pltpu.VMEM((3, col_block), F32),
            pltpu.VMEM((3, col_block), F32),
            dma((2, 3, places)),
            dma((3, chips, 2)),
            dma((2 * CORES,)),
            dma((chips, 2 * CORES)),
            dma((2,)),
            dma((steps, 3)),
            dma((HALVES,)),
            dma((2, 3, chips, 2)),
            dma((3, chips, 2)),
            dma((2,)),
            dma((chips, 2)),
            dma((2, chips)),
            dma((2, HALVES)),
            dma((kinds, places)),
            dma((kinds,)),
            dma((3,)),
            dma((3,)),
            dma((2,)),
        ]
        out_shape = (
            jax.ShapeDtypeStruct((steps, batch, half), BF16),
            jax.ShapeDtypeStruct((2, batch, half), F32),
        )
        results = pl.pallas_call(
            functools.partial(gru_kernel, rows, cols),
            name="gru",
            out_shape=out_shape,
            in_specs=[anywhere] * 10,
            out_specs=(vmem, vmem),
            scratch_shapes=scratch,
            compiler_params=pltpu.CompilerParams(
                collective_id=0, has_side_effects=True, vmem_limit_bytes=60 * 1024 * 1024
            ),
        )(
            x_rows, h_rows,
            jnp.transpose(wx_l1, (1, 0, 2)), whru_l1, whn_l1, bias_l1,
            jnp.transpose(wx_l2, (1, 0, 2)), whru_l2, whn_l2, bias_l2,
        )
        return pl.pallas_call(pass_on, name="results", out_shape=out_shape, in_specs=[vmem] * 2, out_specs=(vmem, vmem))(*results)

    seq_spec = P(None, "data", "row")
    out_spec = P(None, "data", ("col", "row"))
    wide_spec = P("row", None, "col")
    square_spec = P("row", "col")
    bias_spec = P(None, "col")
    return jax.shard_map(
        device_body,
        mesh=mesh,
        in_specs=(seq_spec, seq_spec, wide_spec, wide_spec, square_spec, bias_spec, wide_spec, wide_spec, square_spec, bias_spec),
        out_specs=(out_spec, out_spec),
        check_vma=False,
    )
```

```python
import functools

import jax
import jax.numpy as jnp
from jax import lax
from jax.experimental import pallas as pl
from jax.experimental.pallas import tpu as pltpu
from jax.sharding import PartitionSpec as P

MESH = pl.DeviceIdType.MESH
F32 = jnp.float32
BF16 = jnp.bfloat16
HALVES = 2
CORES = 2
RESET, UPDATE, CAND, REC_CAND, REC_RESET, REC_UPDATE = range(6)
GATES = 6
PAIR, WX, WN = range(3)
EARLY = 2


def ring_distance(offset, count):
    return min(offset, count - offset)


def gru_kernel(
    rows, cols,
    x_ref, h_ref, wx1, wru1, wn1, b1_ref, wx2, wru2, wn2, b2_ref,
    seq_out, last_out,
    weights, pairs, x_here, first_made, first_passed, first_parts, state_in,
    h1_blocks, r1_blocks, h2_blocks, r2_blocks,
    states, updates, projections, seq_halves, last_halves, b1, b2,
    weight_sem, hand_sem, x_sem, wide_sem, passed_sem, parts_sem, state_sem,
    weight_sent, handed_sent, x_sent, wide_sent, made_sent, state_sent,
    block_sem, block_sent, out_sem, out_sent, bias_sem,
):
    chips = rows // CORES
    steps, batch, half = seq_out.shape
    chunk = HALVES * half
    places = chips * cols
    row, col = lax.axis_index("row"), lax.axis_index("col")
    xpos, core = row // CORES, row % CORES
    layers = ((wx1, wru1, wn1), (wx2, wru2, wn2))

    def device(x, c, y):
        return {"row": CORES * x + c, "col": y}

    def wrap_x(v):
        return lax.rem(v + 2 * chips, chips)

    def wrap_y(v):
        return lax.rem(v + 2 * cols, cols)

    def place_of(x_from, y_from, x_to, y_to):
        return chips * wrap_y(y_from - y_to) + wrap_x(x_from - x_to)

    for n, (src, dst) in enumerate(((b1_ref, b1), (b2_ref, b2))):
        pltpu.make_async_copy(src, dst, bias_sem.at[n]).start()

    barrier = pltpu.get_barrier_semaphore()
    for k in range(1, rows * cols):
        other = {"row": lax.rem(row + k % rows, rows), "col": lax.rem(col + k // rows, cols)}
        pl.semaphore_signal(barrier, inc=1, device_id=other, device_id_type=MESH)
    pl.semaphore_wait(barrier, rows * cols - 1)

    def remote(src, dst, send, recv, to):
        return pltpu.make_async_remote_copy(
            src_ref=src, dst_ref=dst, send_sem=send, recv_sem=recv, device_id=to, device_id_type=MESH
        )

    def chunk_place(c, j, x_from, x_to, y_to):
        return place_of(HALVES * c + j, x_from, x_to, y_to)

    def room(part, layer, index):
        if part == PAIR:
            return pairs.at[layer, index]
        return weights.at[layer, index, pl.ds(0, 3)] if part == WX else weights.at[layer, index, REC_CAND]

    def pieces(part, layer, j, x_to, index):
        depth = pl.ds(j * chunk, chunk)
        dst = room(part, layer, index)
        wx, wru, wn = layers[layer]
        for s in range(HALVES):
            units = pl.ds(pl.multiple_of(x_to * chunk + s * half, half), half)
            if part == PAIR:
                yield wru.at[depth, :, units], dst.at[s]
            elif part == WX:
                yield wx.at[:, depth, units], dst.at[:, s]
            else:
                yield wn.at[depth, units], dst.at[s]

    moving = ((PAIR, WN), (PAIR, WX, WN))

    def send_part(part, layer, turns):
        for turn in turns:
            x_to = wrap_x(xpos + turn)
            for j in range(2):
                place = chunk_place(core, j, xpos, x_to, col)
                sent, sem = weight_sent.at[layer, part, turn, j], weight_sem.at[layer, part, place]
                for src, dst in pieces(part, layer, j, x_to, place):
                    remote(src, dst, sent, sem, device(x_to, 1, col)).start()

    def keep_weights(layer):
        for part in moving[layer]:
            for j in range(2):
                place = chunk_place(1, j, xpos, xpos, col)
                for src, dst in pieces(part, layer, j, xpos, place):
                    pltpu.make_async_copy(src, dst, weight_sem.at[layer, part, place]).start()

    def hand_over():
        for part in moving[1]:
            for turn in far_turns:
                x_to = wrap_x(xpos + turn)
                for j in range(2):
                    for src, dst in pieces(part, 1, j, x_to, 2 * turn + j):
                        to = device(xpos, 0, col)
                        remote(src, dst, weight_sent.at[1, part, turn, j], hand_sem.at[part, turn, j], to).start()

    def send_handed(part):
        for turn in far_turns:
            x_to = wrap_x(xpos + turn)
            for j in range(2):
                src = room(part, 1, 2 * turn + j)
                pltpu.make_async_copy(src, src, hand_sem.at[part, turn, j]).wait()
                place = chunk_place(1, j, xpos, x_to, col)
                sent, sem = handed_sent.at[part, turn, j], weight_sem.at[1, part, place]
                remote(src, room(part, 1, place), sent, sem, device(x_to, 1, col)).start()

    def weights_arrived(part, layer):
        for p in range(places):
            here = room(part, layer, p)
            pltpu.make_async_copy(here, here, weight_sem.at[layer, part, p]).wait()

    def split_pairs(layer):
        def split(p, carry):
            here = pairs.at[layer, p]
            pltpu.make_async_copy(here, here, weight_sem.at[layer, PAIR, p]).wait()
            for s in range(HALVES):
                both = jnp.swapaxes(here[s], 0, 1)
                weights[layer, p, REC_RESET, s] = both[0]
                weights[layer, p, REC_UPDATE, s] = both[1]
            return carry

        lax.fori_loop(0, places, split, 0)

    def input_copies():
        for j in range(2):
            n = 2 * core + j
            for s in range(HALVES):
                yield x_ref.at[:, :, pl.ds(j * chunk + s * half, half)], x_here.at[n, :, s], x_sent.at[j], x_sem.at[n]
            for turn in range(chips):
                for src, dst in pieces(WX, 0, j, wrap_x(xpos + turn), 2 * CORES * turn + n):
                    yield src, dst, wide_sent.at[turn, j], wide_sem.at[turn, n]

    def keep_inputs():
        for src, dst, _, sem in input_copies():
            pltpu.make_async_copy(src, dst, sem).start()

    def hand_inputs():
        for src, dst, sent, sem in input_copies():
            remote(src, dst, sent, sem, device(xpos, 0, col)).start()

    def inputs_here():
        for n in range(2 * CORES):
            pltpu.make_async_copy(x_here.at[n], x_here.at[n], x_sem.at[n]).wait()
            for turn in range(chips):
                kept = weights.at[0, 2 * CORES * turn + n, pl.ds(0, 3)]
                pltpu.make_async_copy(kept, kept, wide_sem.at[turn, n]).wait()

    def wide(parts):
        return jnp.concatenate(parts, axis=1)

    def make_first(t, way, again):
        onward, other = ((1, chips - 1), (chips - 1, 1))[way]

        def part_of(turn):
            total = None
            for n in range(2 * CORES):
                rhs = wide([weights[0, 2 * CORES * turn + n, g, s] for g in range(3) for s in range(HALVES)])
                lhs = wide([x_here[n, t, s] for s in range(HALVES)])
                term = jnp.dot(lhs, rhs, preferred_element_type=F32)
                total = term if total is None else total + term
            return total

        def emit(turn, passed, dst, sem, to):
            made = first_made.at[way, turn]
            if again:
                pltpu.make_async_copy(made, made, made_sent.at[way, turn]).wait()
            total = part_of(turn)
            if passed is not None:
                pltpu.make_async_copy(passed, passed, passed_sem.at[way]).wait()
            for g in range(3):
                for s in range(HALVES):
                    n = g * HALVES + s
                    value = total[:, n * half : (n + 1) * half]
                    made[g, s] = value if passed is None else value + passed[g, s]
            remote(made, dst, made_sent.at[way, turn], sem, to).start()

        def parts(seen):
            return first_parts.at[t, seen], parts_sem.at[t, seen]

        emit(2, None, first_passed.at[way], passed_sem.at[way], device(wrap_x(xpos + onward), 0, col))
        emit(other, None, *parts(1 - way), device(wrap_x(xpos + other), 1, col))
        emit(onward, first_passed.at[way], *parts(way), device(wrap_x(xpos + onward), 1, col))
        emit(0, None, *parts(2), device(xpos, 1, col))

    far_turns = (2, 1, chips - 1)

    @pl.when(xpos == col)
    def _():
        for j in range(2):
            x_to = HALVES * core + j
            for s in range(HALVES):
                src = h_ref.at[:, :, pl.ds(j * chunk + s * half, half)]
                dst = state_in.at[:, s]
                mine = (x_to == xpos) & (core == 1)

                @pl.when(mine)
                def _():
                    pltpu.make_async_copy(src, dst, state_sem.at[s]).start()

                @pl.when(jnp.logical_not(mine))
                def _():
                    copy = remote(src, dst, state_sent.at[j, s], state_sem.at[s], device(x_to, 1, col))
                    copy.start()
                    copy.wait_send()

    for part in moving[0]:
        send_part(part, 0, far_turns)

    @pl.when(core == 1)
    def _():
        hand_inputs()
        keep_weights(0)
        hand_over()
        keep_weights(1)

    @pl.when(core == 0)
    def _():
        keep_inputs()
        for part in moving[0]:
            send_part(part, 0, (0,))
        inputs_here()
        for t in range(EARLY):
            make_first(t, t % 2, False)
        for part in moving[1]:
            send_part(part, 1, far_turns)
            send_part(part, 1, (0,))
            send_handed(part)

    for n, dst in enumerate((b1, b2)):
        pltpu.make_async_copy(dst, dst, bias_sem.at[n]).wait()

    def drain_sends():
        for layer in range(2):
            for part in moving[layer]:
                piece = room(part, layer, 0)
                for j in range(2):
                    for turn in far_turns:
                        pltpu.make_async_copy(piece, piece, weight_sent.at[layer, part, turn, j]).wait()

        @pl.when(core == 0)
        def _():
            for layer in range(2):
                for part in moving[layer]:
                    piece = room(part, layer, 0)
                    for j in range(2):
                        pltpu.make_async_copy(piece, piece, weight_sent.at[layer, part, 0, j]).wait()
            for part in moving[1]:
                piece = room(part, 1, 0)
                for j in range(2):
                    for turn in far_turns:
                        pltpu.make_async_copy(piece, piece, handed_sent.at[part, turn, j]).wait()
            for slot in range(2):
                for turn in range(chips):
                    made = first_made.at[slot, turn]
                    pltpu.make_async_copy(made, made, made_sent.at[slot, turn]).wait()

        @pl.when(core == 1)
        def _():
            piece = room(WX, 0, 0)
            for j in range(2):
                pltpu.make_async_copy(x_here.at[0], x_here.at[0], x_sent.at[j]).wait()
                for turn in range(chips):
                    pltpu.make_async_copy(piece, piece, wide_sent.at[turn, j]).wait()

    offsets = [(dx, dy) for dy in range(cols) for dx in range(chips)]
    distance = [ring_distance(dx, chips) + ring_distance(dy, cols) for dx, dy in offsets]
    far_first = sorted(range(1, places), key=lambda p: -distance[p])
    by_arrival = sorted(range(places), key=lambda p: (distance[p], ring_distance(offsets[p][0], chips)))
    groups = [by_arrival[:6], by_arrival[6:10], by_arrival[10:]]

    def spread(blocks, kind):
        for p in far_first:
            dx, dy = offsets[p]
            there = chips * ((cols - dy) % cols) + (chips - dx) % chips
            to = device(wrap_x(xpos + dx), 1, wrap_y(col + dy))
            remote(blocks.at[0], blocks.at[there], block_sent.at[kind], block_sem.at[kind, there], to).start()

    def arrived(blocks, kind, p):
        pltpu.make_async_copy(blocks.at[p], blocks.at[p], block_sem.at[kind, p]).wait()

    def all_sent(blocks, kind):
        sent = blocks.at[pl.ds(1, places - 1)]
        pltpu.make_async_copy(sent, sent, block_sent.at[kind]).wait()

    def product(lhs_of, layer, gates, order, total=None):
        for p in order:
            rhs = wide([weights[layer, p, g, s] for g in gates for s in range(HALVES)])
            lhs = wide([lhs_of(p, s) for s in range(HALVES)])
            term = jnp.dot(lhs, rhs, preferred_element_type=F32)
            total = term if total is None else total + term
        return total

    def gathered(blocks, kind, layer, gate):
        total = None
        for group in groups:
            for p in group:
                if p:
                    arrived(blocks, kind, p)
            total = product(lambda p, s: blocks[p, s], layer, (gate,), group, total)
        return total

    def project(layer, lhs_of, bias, gates):
        total = product(lhs_of, layer, gates, range(places))
        for k, g in enumerate(gates):
            for s in range(HALVES):
                n = k * HALVES + s
                here = bias[pl.ds(g, 1), pl.ds(pl.multiple_of(xpos * chunk + s * half, half), half)]
                projections[layer, g, s] = total[:, n * half : (n + 1) * half] + here

    def reset_half(layer, blocks, kind, out_blocks):
        total = gathered(blocks, kind, layer, REC_RESET)
        for s in range(HALVES):
            reset = jax.nn.sigmoid(projections[layer, RESET, s] + total[:, s * half : (s + 1) * half])
            out_blocks[0, s] = (reset * states[layer, s]).astype(BF16)

    def update_half(layer, blocks, kind):
        total = product(lambda p, s: blocks[p, s], layer, (REC_UPDATE,), range(places))
        for s in range(HALVES):
            updates[layer, s] = jax.nn.sigmoid(projections[layer, UPDATE, s] + total[:, s * half : (s + 1) * half])
        all_sent(blocks, kind)

    def next_half(layer, blocks, kind, emit):
        total = gathered(blocks, kind, layer, REC_CAND)
        for s in range(HALVES):
            candidate = jnp.tanh(projections[layer, CAND, s] + total[:, s * half : (s + 1) * half])
            update = updates[layer, s]
            state = (1.0 - update) * candidate + update * states[layer, s]
            emit(s, state.astype(BF16))
            states[layer, s] = state

    H1, R1, H2, R2 = range(4)

    def first_reset(t):
        reset_half(0, h1_blocks.at[lax.rem(t, 2)], H1, r1_blocks)
        spread(r1_blocks, R1)

    def first_update(t):
        update_half(0, h1_blocks.at[lax.rem(t, 2)], H1)

    def first_next(t):
        slot = h1_blocks.at[lax.rem(t + 1, 2)]

        def emit(s, value):
            slot[0, s] = value

        next_half(0, r1_blocks, R1, emit)
        spread(slot, H1)
        all_sent(r1_blocks, R1)

    def first_inputs(t):
        for n in range(3):
            part = first_parts.at[t, n]
            pltpu.make_async_copy(part, part, parts_sem.at[t, n]).wait()
        for g in range(3):
            for s in range(HALVES):
                here = b1[pl.ds(g, 1), pl.ds(pl.multiple_of(xpos * chunk + s * half, half), half)]
                projections[0, g, s] = sum(first_parts[t, n, g, s] for n in range(3)) + here

    def second_inputs(t, gates):
        slot = h1_blocks.at[lax.rem(t, 2)]
        project(1, lambda p, s: slot[p, s], b2, gates)

    def second_reset(t):
        reset_half(1, h2_blocks.at[lax.rem(t, 2)], H2, r2_blocks)
        spread(r2_blocks, R2)

    def second_update(t):
        update_half(1, h2_blocks.at[lax.rem(t, 2)], H2)

    def second_next(t, last):
        slot = h2_blocks.at[lax.rem(t + 1, 2)]

        def emit(s, value):
            seq_halves[s, t] = value
            if not last:
                slot[0, s] = value

        next_half(1, r2_blocks, R2, emit)
        if not last:
            spread(slot, H2)
        all_sent(r2_blocks, R2)

    @pl.when(core == 1)
    def _():
        for s in range(HALVES):
            part = state_in.at[:, s]
            pltpu.make_async_copy(part, part, state_sem.at[s]).wait()
        for layer in range(2):
            for s in range(HALVES):
                states[layer, s] = state_in[layer, s]
        for s in range(HALVES):
            h1_blocks[0, 0, s] = state_in[0, s].astype(BF16)
            h2_blocks[0, 0, s] = state_in[1, s].astype(BF16)
        spread(h1_blocks.at[0], H1)
        spread(h2_blocks.at[0], H2)
        split_pairs(0)
        weights_arrived(WN, 0)
        first_inputs(0)
        first_reset(0)
        first_update(0)
        first_next(0)
        first_inputs(1)
        split_pairs(1)
        weights_arrived(WX, 1)

        def step(t, first):
            first_reset(t)
            second_inputs(t, (RESET,))
            second_reset(t - 1)
            first_update(t)
            second_inputs(t, (UPDATE, CAND))
            second_update(t - 1)
            first_next(t)
            if first:
                weights_arrived(WN, 1)
            second_next(t - 1, False)
            pl.when(t + 1 < steps)(lambda: first_inputs(t + 1))

        def later_step(t, carry):
            step(t, False)
            return carry

        step(1, True)
        lax.fori_loop(2, steps, later_step, 0)
        last_slot = h1_blocks.at[steps % 2]
        for p in range(1, places):
            arrived(last_slot, H1, p)
        all_sent(last_slot, H1)
        second_inputs(steps, (RESET,))
        second_reset(steps - 1)
        second_inputs(steps, (UPDATE, CAND))
        second_update(steps - 1)
        before, at_end = pl.ds(0, steps - 1), steps - 1
        beside = device(xpos, 0, col)
        early_copy = remote(seq_halves.at[0, before], seq_out.at[before], out_sent.at[2], out_sem.at[2], beside)
        early_copy.start()
        seq_out[before] = seq_halves[1, before]
        second_next(at_end, True)
        for layer in range(2):
            for s in range(HALVES):
                last_halves[s, layer] = states[layer, s]
        seq_copy = remote(seq_halves.at[0, at_end], seq_out.at[at_end], out_sent.at[0], out_sem.at[0], beside)
        last_copy = remote(last_halves.at[0], last_out, out_sent.at[1], out_sem.at[1], beside)
        seq_copy.start()
        last_copy.start()
        seq_out[at_end] = seq_halves[1, at_end]
        last_out[...] = last_halves[1]
        early_copy.wait_send()
        seq_copy.wait_send()
        last_copy.wait_send()

    @pl.when(core == 0)
    def _():
        def later_first(pair, carry):
            for way in range(2):
                make_first(2 * pair + way, way, True)
            return carry

        lax.fori_loop(EARLY // 2, steps // 2, later_first, 0)
        for part, n in ((seq_out.at[pl.ds(0, steps - 1)], 2), (seq_out.at[steps - 1], 0)):
            pltpu.make_async_copy(part, part, out_sem.at[n]).wait()
        pltpu.make_async_copy(last_out, last_out, out_sem.at[1]).wait()

    drain_sends()


def pass_on(seq_ref, last_ref, seq_out, last_out):
    seq_out[...] = seq_ref[...]
    last_out[...] = last_ref[...]


def solution(mesh):
    rows, cols = mesh.shape["row"], mesh.shape["col"]
    chips = rows // CORES
    places = chips * cols

    def device_body(x_rows, h_rows, wx_l1, whru_l1, whn_l1, bias_l1, wx_l2, whru_l2, whn_l2, bias_l2):
        steps, batch, row_block = x_rows.shape
        col_block = wx_l1.shape[2]
        half = col_block // rows
        chunk = HALVES * half
        anywhere = pl.BlockSpec(memory_space=pl.ANY)
        vmem = pl.BlockSpec(memory_space=pltpu.VMEM)
        dma = pltpu.SemaphoreType.DMA
        kinds = 4
        block = (HALVES, batch, half)
        scratch = [
            pltpu.VMEM((2, places, GATES, HALVES, chunk, half), BF16),
            pltpu.VMEM((2, places, HALVES, chunk, 2, half), BF16),
            pltpu.VMEM((2 * CORES, steps, *block), BF16),
            pltpu.VMEM((2, chips, 3, *block), F32),
            pltpu.VMEM((2, 3, *block), F32),
            pltpu.VMEM((steps, 3, 3, *block), F32),
            pltpu.VMEM((2, *block), F32),
            pltpu.VMEM((2, places, *block), BF16),
            pltpu.VMEM((places, *block), BF16),
            pltpu.VMEM((2, places, *block), BF16),
            pltpu.VMEM((places, *block), BF16),
            pltpu.VMEM((2, *block), F32),
            pltpu.VMEM((2, *block), F32),
            pltpu.VMEM((2, 3, *block), F32),
            pltpu.VMEM((HALVES, steps, batch, half), BF16),
            pltpu.VMEM((HALVES, 2, batch, half), F32),
            pltpu.VMEM((3, col_block), F32),
            pltpu.VMEM((3, col_block), F32),
            dma((2, 3, places)),
            dma((3, chips, 2)),
            dma((2 * CORES,)),
            dma((chips, 2 * CORES)),
            dma((2,)),
            dma((steps, 3)),
            dma((HALVES,)),
            dma((2, 3, chips, 2)),
            dma((3, chips, 2)),
            dma((2,)),
            dma((chips, 2)),
            dma((2, chips)),
            dma((2, HALVES)),
            dma((kinds, places)),
            dma((kinds,)),
            dma((3,)),
            dma((3,)),
            dma((2,)),
        ]
        out_shape = (
            jax.ShapeDtypeStruct((steps, batch, half), BF16),
            jax.ShapeDtypeStruct((2, batch, half), F32),
        )
        results = pl.pallas_call(
            functools.partial(gru_kernel, rows, cols),
            name="gru",
            out_shape=out_shape,
            in_specs=[anywhere] * 10,
            out_specs=(vmem, vmem),
            scratch_shapes=scratch,
            compiler_params=pltpu.CompilerParams(
                collective_id=0, has_side_effects=True, vmem_limit_bytes=60 * 1024 * 1024
            ),
        )(
            x_rows, h_rows,
            jnp.transpose(wx_l1, (1, 0, 2)), whru_l1, whn_l1, bias_l1,
            jnp.transpose(wx_l2, (1, 0, 2)), whru_l2, whn_l2, bias_l2,
        )
        return pl.pallas_call(pass_on, name="results", out_shape=out_shape, in_specs=[vmem] * 2, out_specs=(vmem, vmem))(*results)

    seq_spec = P(None, "data", "row")
    out_spec = P(None, "data", ("col", "row"))
    wide_spec = P("row", None, "col")
    square_spec = P("row", "col")
    bias_spec = P(None, "col")
    return jax.shard_map(
        device_body,
        mesh=mesh,
        in_specs=(seq_spec, seq_spec, wide_spec, wide_spec, square_spec, bias_spec, wide_spec, wide_spec, square_spec, bias_spec),
        out_specs=(out_spec, out_spec),
        check_vma=False,
    )
```

```python
import functools

import jax
import jax.numpy as jnp
from jax import lax
from jax.experimental import pallas as pl
from jax.experimental.pallas import tpu as pltpu
from jax.sharding import PartitionSpec as P

MESH = pl.DeviceIdType.MESH
F32 = jnp.float32
BF16 = jnp.bfloat16
HALVES = 2
CORES = 2
RESET, UPDATE, CAND, REC_CAND, REC_RESET, REC_UPDATE = range(6)
GATES = 6
PAIR, WX, WN = range(3)
EARLY = 2


def ring_distance(offset, count):
    return min(offset, count - offset)


def gru_kernel(
    rows, cols,
    x_ref, h_ref, wx1, wru1, wn1, b1_ref, wx2, wru2, wn2, b2_ref,
    seq_out, last_out,
    weights, pairs, x_here, first_made, first_passed, first_parts, state_in,
    h1_blocks, r1_blocks, h2_blocks, r2_blocks,
    states, updates, projections, seq_halves, last_halves, b1, b2,
    weight_sem, hand_sem, x_sem, wide_sem, passed_sem, parts_sem, state_sem,
    weight_sent, handed_sent, x_sent, wide_sent, made_sent, state_sent,
    block_sem, block_sent, out_sem, out_sent, bias_sem,
):
    chips = rows // CORES
    steps, batch, half = seq_out.shape
    chunk = HALVES * half
    places = chips * cols
    row, col = lax.axis_index("row"), lax.axis_index("col")
    xpos, core = row // CORES, row % CORES
    layers = ((wx1, wru1, wn1), (wx2, wru2, wn2))

    def device(x, c, y):
        return {"row": CORES * x + c, "col": y}

    def wrap_x(v):
        return lax.rem(v + 2 * chips, chips)

    def wrap_y(v):
        return lax.rem(v + 2 * cols, cols)

    def place_of(x_from, y_from, x_to, y_to):
        return chips * wrap_y(y_from - y_to) + wrap_x(x_from - x_to)

    for n, (src, dst) in enumerate(((b1_ref, b1), (b2_ref, b2))):
        pltpu.make_async_copy(src, dst, bias_sem.at[n]).start()

    barrier = pltpu.get_barrier_semaphore()
    for k in range(1, rows * cols):
        other = {"row": lax.rem(row + k % rows, rows), "col": lax.rem(col + k // rows, cols)}
        pl.semaphore_signal(barrier, inc=1, device_id=other, device_id_type=MESH)
    pl.semaphore_wait(barrier, rows * cols - 1)

    def remote(src, dst, send, recv, to):
        return pltpu.make_async_remote_copy(
            src_ref=src, dst_ref=dst, send_sem=send, recv_sem=recv, device_id=to, device_id_type=MESH
        )

    def chunk_place(c, j, x_from, x_to, y_to):
        return place_of(HALVES * c + j, x_from, x_to, y_to)

    def room(part, layer, index):
        if part == PAIR:
            return pairs.at[layer, index]
        return weights.at[layer, index, pl.ds(0, 3)] if part == WX else weights.at[layer, index, REC_CAND]

    def pieces(part, layer, j, x_to, index):
        depth = pl.ds(j * chunk, chunk)
        dst = room(part, layer, index)
        wx, wru, wn = layers[layer]
        for s in range(HALVES):
            units = pl.ds(pl.multiple_of(x_to * chunk + s * half, half), half)
            if part == PAIR:
                yield wru.at[depth, :, units], dst.at[s]
            elif part == WX:
                yield wx.at[:, depth, units], dst.at[:, s]
            else:
                yield wn.at[depth, units], dst.at[s]

    moving = ((PAIR, WN), (PAIR, WX, WN))

    def send_part(part, layer, turns):
        for turn in turns:
            x_to = wrap_x(xpos + turn)
            for j in range(2):
                place = chunk_place(core, j, xpos, x_to, col)
                sent, sem = weight_sent.at[layer, part, turn, j], weight_sem.at[layer, part, place]
                for src, dst in pieces(part, layer, j, x_to, place):
                    remote(src, dst, sent, sem, device(x_to, 1, col)).start()

    def keep_weights(layer):
        for part in moving[layer]:
            for j in range(2):
                place = chunk_place(1, j, xpos, xpos, col)
                for src, dst in pieces(part, layer, j, xpos, place):
                    pltpu.make_async_copy(src, dst, weight_sem.at[layer, part, place]).start()

    def hand_over():
        for part in moving[1]:
            for turn in far_turns:
                x_to = wrap_x(xpos + turn)
                for j in range(2):
                    for src, dst in pieces(part, 1, j, x_to, 2 * turn + j):
                        to = device(xpos, 0, col)
                        remote(src, dst, weight_sent.at[1, part, turn, j], hand_sem.at[part, turn, j], to).start()

    def send_handed(part):
        for turn in far_turns:
            x_to = wrap_x(xpos + turn)
            for j in range(2):
                src = room(part, 1, 2 * turn + j)
                pltpu.make_async_copy(src, src, hand_sem.at[part, turn, j]).wait()
                place = chunk_place(1, j, xpos, x_to, col)
                sent, sem = handed_sent.at[part, turn, j], weight_sem.at[1, part, place]
                remote(src, room(part, 1, place), sent, sem, device(x_to, 1, col)).start()

    def weights_arrived(part, layer):
        for p in range(places):
            here = room(part, layer, p)
            pltpu.make_async_copy(here, here, weight_sem.at[layer, part, p]).wait()

    def split_pairs(layer):
        def split(p, carry):
            here = pairs.at[layer, p]
            pltpu.make_async_copy(here, here, weight_sem.at[layer, PAIR, p]).wait()
            for s in range(HALVES):
                both = jnp.swapaxes(here[s], 0, 1)
                weights[layer, p, REC_RESET, s] = both[0]
                weights[layer, p, REC_UPDATE, s] = both[1]
            return carry

        lax.fori_loop(0, places, split, 0)

    def input_copies():
        for j in range(2):
            n = 2 * core + j
            for s in range(HALVES):
                yield x_ref.at[:, :, pl.ds(j * chunk + s * half, half)], x_here.at[n, :, s], x_sent.at[j], x_sem.at[n]
            for turn in range(chips):
                for src, dst in pieces(WX, 0, j, wrap_x(xpos + turn), 2 * CORES * turn + n):
                    yield src, dst, wide_sent.at[turn, j], wide_sem.at[turn, n]

    def keep_inputs():
        for src, dst, _, sem in input_copies():
            pltpu.make_async_copy(src, dst, sem).start()

    def hand_inputs():
        for src, dst, sent, sem in input_copies():
            remote(src, dst, sent, sem, device(xpos, 0, col)).start()

    def inputs_here():
        for n in range(2 * CORES):
            pltpu.make_async_copy(x_here.at[n], x_here.at[n], x_sem.at[n]).wait()
            for turn in range(chips):
                kept = weights.at[0, 2 * CORES * turn + n, pl.ds(0, 3)]
                pltpu.make_async_copy(kept, kept, wide_sem.at[turn, n]).wait()

    def wide(parts):
        return jnp.concatenate(parts, axis=1)

    def make_first(t, way, again):
        onward, other = ((1, chips - 1), (chips - 1, 1))[way]

        def part_of(turn):
            total = None
            for n in range(2 * CORES):
                rhs = wide([weights[0, 2 * CORES * turn + n, g, s] for g in range(3) for s in range(HALVES)])
                lhs = wide([x_here[n, t, s] for s in range(HALVES)])
                term = jnp.dot(lhs, rhs, preferred_element_type=F32)
                total = term if total is None else total + term
            return total

        def emit(turn, passed, dst, sem, to):
            made = first_made.at[way, turn]
            if again:
                pltpu.make_async_copy(made, made, made_sent.at[way, turn]).wait()
            total = part_of(turn)
            if passed is not None:
                pltpu.make_async_copy(passed, passed, passed_sem.at[way]).wait()
            for g in range(3):
                for s in range(HALVES):
                    n = g * HALVES + s
                    value = total[:, n * half : (n + 1) * half]
                    made[g, s] = value if passed is None else value + passed[g, s]
            remote(made, dst, made_sent.at[way, turn], sem, to).start()

        def parts(seen):
            return first_parts.at[t, seen], parts_sem.at[t, seen]

        emit(2, None, first_passed.at[way], passed_sem.at[way], device(wrap_x(xpos + onward), 0, col))
        emit(other, None, *parts(1 - way), device(wrap_x(xpos + other), 1, col))
        emit(onward, first_passed.at[way], *parts(way), device(wrap_x(xpos + onward), 1, col))
        emit(0, None, *parts(2), device(xpos, 1, col))

    far_turns = (2, 1, chips - 1)

    @pl.when(xpos == col)
    def _():
        for j in range(2):
            x_to = HALVES * core + j
            for s in range(HALVES):
                src = h_ref.at[:, :, pl.ds(j * chunk + s * half, half)]
                dst = state_in.at[:, s]
                mine = (x_to == xpos) & (core == 1)

                @pl.when(mine)
                def _():
                    pltpu.make_async_copy(src, dst, state_sem.at[s]).start()

                @pl.when(jnp.logical_not(mine))
                def _():
                    copy = remote(src, dst, state_sent.at[j, s], state_sem.at[s], device(x_to, 1, col))
                    copy.start()
                    copy.wait_send()

    for part in moving[0]:
        send_part(part, 0, far_turns)

    @pl.when(core == 1)
    def _():
        hand_inputs()
        keep_weights(0)
        hand_over()
        keep_weights(1)

    @pl.when(core == 0)
    def _():
        keep_inputs()
        for part in moving[0]:
            send_part(part, 0, (0,))
        inputs_here()
        for t in range(EARLY):
            make_first(t, t % 2, False)
        for part in moving[1]:
            send_part(part, 1, far_turns)
            send_part(part, 1, (0,))
            send_handed(part)

    for n, dst in enumerate((b1, b2)):
        pltpu.make_async_copy(dst, dst, bias_sem.at[n]).wait()

    def drain_sends():
        for layer in range(2):
            for part in moving[layer]:
                piece = room(part, layer, 0)
                for j in range(2):
                    for turn in far_turns:
                        pltpu.make_async_copy(piece, piece, weight_sent.at[layer, part, turn, j]).wait()

        @pl.when(core == 0)
        def _():
            for layer in range(2):
                for part in moving[layer]:
                    piece = room(part, layer, 0)
                    for j in range(2):
                        pltpu.make_async_copy(piece, piece, weight_sent.at[layer, part, 0, j]).wait()
            for part in moving[1]:
                piece = room(part, 1, 0)
                for j in range(2):
                    for turn in far_turns:
                        pltpu.make_async_copy(piece, piece, handed_sent.at[part, turn, j]).wait()
            for slot in range(2):
                for turn in range(chips):
                    made = first_made.at[slot, turn]
                    pltpu.make_async_copy(made, made, made_sent.at[slot, turn]).wait()

        @pl.when(core == 1)
        def _():
            piece = room(WX, 0, 0)
            for j in range(2):
                pltpu.make_async_copy(x_here.at[0], x_here.at[0], x_sent.at[j]).wait()
                for turn in range(chips):
                    pltpu.make_async_copy(piece, piece, wide_sent.at[turn, j]).wait()

    offsets = [(dx, dy) for dy in range(cols) for dx in range(chips)]
    distance = [ring_distance(dx, chips) + ring_distance(dy, cols) for dx, dy in offsets]
    far_first = sorted(range(1, places), key=lambda p: -distance[p])
    by_arrival = sorted(range(places), key=lambda p: (distance[p], ring_distance(offsets[p][0], chips)))
    groups = [by_arrival[:6], by_arrival[6:10], by_arrival[10:]]

    def spread(blocks, kind):
        for p in far_first:
            dx, dy = offsets[p]
            there = chips * ((cols - dy) % cols) + (chips - dx) % chips
            to = device(wrap_x(xpos + dx), 1, wrap_y(col + dy))
            remote(blocks.at[0], blocks.at[there], block_sent.at[kind], block_sem.at[kind, there], to).start()

    def arrived(blocks, kind, p):
        pltpu.make_async_copy(blocks.at[p], blocks.at[p], block_sem.at[kind, p]).wait()

    def all_sent(blocks, kind):
        sent = blocks.at[pl.ds(1, places - 1)]
        pltpu.make_async_copy(sent, sent, block_sent.at[kind]).wait()

    def product(lhs_of, layer, gates, order, total=None):
        for p in order:
            rhs = wide([weights[layer, p, g, s] for g in gates for s in range(HALVES)])
            lhs = wide([lhs_of(p, s) for s in range(HALVES)])
            term = jnp.dot(lhs, rhs, preferred_element_type=F32)
            total = term if total is None else total + term
        return total

    def gathered(blocks, kind, layer, gate):
        total = None
        for group in groups:
            for p in group:
                if p:
                    arrived(blocks, kind, p)
            total = product(lambda p, s: blocks[p, s], layer, (gate,), group, total)
        return total

    def project(layer, lhs_of, bias):
        total = product(lhs_of, layer, (RESET, UPDATE, CAND), range(places))
        for g in range(3):
            for s in range(HALVES):
                n = g * HALVES + s
                here = bias[pl.ds(g, 1), pl.ds(pl.multiple_of(xpos * chunk + s * half, half), half)]
                projections[layer, g, s] = total[:, n * half : (n + 1) * half] + here

    def reset_half(layer, blocks, kind, out_blocks, send):
        total = gathered(blocks, kind, layer, REC_RESET)
        for s in range(HALVES):
            reset = jax.nn.sigmoid(projections[layer, RESET, s] + total[:, s * half : (s + 1) * half])
            out_blocks[0, s] = (reset * states[layer, s]).astype(BF16)
        send()
        total = product(lambda p, s: blocks[p, s], layer, (REC_UPDATE,), range(places))
        for s in range(HALVES):
            updates[layer, s] = jax.nn.sigmoid(projections[layer, UPDATE, s] + total[:, s * half : (s + 1) * half])

    def next_half(layer, blocks, kind, emit):
        total = gathered(blocks, kind, layer, REC_CAND)
        for s in range(HALVES):
            candidate = jnp.tanh(projections[layer, CAND, s] + total[:, s * half : (s + 1) * half])
            update = updates[layer, s]
            state = (1.0 - update) * candidate + update * states[layer, s]
            emit(s, state.astype(BF16))
            states[layer, s] = state

    H1, R1, H2, R2 = range(4)

    def first_reset(t):
        slot = h1_blocks.at[lax.rem(t, 2)]
        reset_half(0, slot, H1, r1_blocks, lambda: spread(r1_blocks, R1))
        all_sent(slot, H1)

    def first_next(t):
        slot = h1_blocks.at[lax.rem(t + 1, 2)]

        def emit(s, value):
            slot[0, s] = value

        next_half(0, r1_blocks, R1, emit)
        spread(slot, H1)
        all_sent(r1_blocks, R1)

    def first_inputs(t):
        for n in range(3):
            part = first_parts.at[t, n]
            pltpu.make_async_copy(part, part, parts_sem.at[t, n]).wait()
        for g in range(3):
            for s in range(HALVES):
                here = b1[pl.ds(g, 1), pl.ds(pl.multiple_of(xpos * chunk + s * half, half), half)]
                projections[0, g, s] = sum(first_parts[t, n, g, s] for n in range(3)) + here

    def second_inputs(t):
        slot = h1_blocks.at[lax.rem(t, 2)]
        project(1, lambda p, s: slot[p, s], b2)

    def second_reset(t):
        slot = h2_blocks.at[lax.rem(t, 2)]
        reset_half(1, slot, H2, r2_blocks, lambda: spread(r2_blocks, R2))
        all_sent(slot, H2)

    def second_next(t, last):
        slot = h2_blocks.at[lax.rem(t + 1, 2)]

        def emit(s, value):
            seq_halves[s, t] = value
            if not last:
                slot[0, s] = value

        next_half(1, r2_blocks, R2, emit)
        if not last:
            spread(slot, H2)
        all_sent(r2_blocks, R2)

    @pl.when(core == 1)
    def _():
        for s in range(HALVES):
            part = state_in.at[:, s]
            pltpu.make_async_copy(part, part, state_sem.at[s]).wait()
        for layer in range(2):
            for s in range(HALVES):
                states[layer, s] = state_in[layer, s]
        for s in range(HALVES):
            h1_blocks[0, 0, s] = state_in[0, s].astype(BF16)
            h2_blocks[0, 0, s] = state_in[1, s].astype(BF16)
        spread(h1_blocks.at[0], H1)
        spread(h2_blocks.at[0], H2)
        split_pairs(0)
        weights_arrived(WN, 0)
        first_inputs(0)
        first_reset(0)
        first_next(0)
        first_inputs(1)
        first_reset(1)
        first_next(1)
        split_pairs(1)
        weights_arrived(WX, 1)
        second_inputs(1)
        second_reset(0)

        first_inputs(2)

        def step(t, carry):
            first_reset(t)
            pl.when(t == 2)(lambda: weights_arrived(WN, 1))
            second_next(t - 2, False)
            first_next(t)
            second_inputs(t)
            second_reset(t - 1)
            pl.when(t + 1 < steps)(lambda: first_inputs(t + 1))
            return carry

        lax.fori_loop(2, steps, step, 0)
        last_slot = h1_blocks.at[steps % 2]
        for p in range(1, places):
            arrived(last_slot, H1, p)
        all_sent(last_slot, H1)
        second_next(steps - 2, False)
        second_inputs(steps)
        second_reset(steps - 1)
        before, at_end = pl.ds(0, steps - 1), steps - 1
        beside = device(xpos, 0, col)
        early_copy = remote(seq_halves.at[0, before], seq_out.at[before], out_sent.at[2], out_sem.at[2], beside)
        early_copy.start()
        seq_out[before] = seq_halves[1, before]
        second_next(at_end, True)
        for layer in range(2):
            for s in range(HALVES):
                last_halves[s, layer] = states[layer, s]
        seq_copy = remote(seq_halves.at[0, at_end], seq_out.at[at_end], out_sent.at[0], out_sem.at[0], beside)
        last_copy = remote(last_halves.at[0], last_out, out_sent.at[1], out_sem.at[1], beside)
        seq_copy.start()
        last_copy.start()
        seq_out[at_end] = seq_halves[1, at_end]
        last_out[...] = last_halves[1]
        early_copy.wait_send()
        seq_copy.wait_send()
        last_copy.wait_send()

    @pl.when(core == 0)
    def _():
        def later_first(pair, carry):
            for way in range(2):
                make_first(2 * pair + way, way, True)
            return carry

        lax.fori_loop(EARLY // 2, steps // 2, later_first, 0)
        for part, n in ((seq_out.at[pl.ds(0, steps - 1)], 2), (seq_out.at[steps - 1], 0)):
            pltpu.make_async_copy(part, part, out_sem.at[n]).wait()
        pltpu.make_async_copy(last_out, last_out, out_sem.at[1]).wait()

    drain_sends()


def pass_on(seq_ref, last_ref, seq_out, last_out):
    seq_out[...] = seq_ref[...]
    last_out[...] = last_ref[...]


def solution(mesh):
    rows, cols = mesh.shape["row"], mesh.shape["col"]
    chips = rows // CORES
    places = chips * cols

    def device_body(x_rows, h_rows, wx_l1, whru_l1, whn_l1, bias_l1, wx_l2, whru_l2, whn_l2, bias_l2):
        steps, batch, row_block = x_rows.shape
        col_block = wx_l1.shape[2]
        half = col_block // rows
        chunk = HALVES * half
        anywhere = pl.BlockSpec(memory_space=pl.ANY)
        vmem = pl.BlockSpec(memory_space=pltpu.VMEM)
        dma = pltpu.SemaphoreType.DMA
        kinds = 4
        block = (HALVES, batch, half)
        scratch = [
            pltpu.VMEM((2, places, GATES, HALVES, chunk, half), BF16),
            pltpu.VMEM((2, places, HALVES, chunk, 2, half), BF16),
            pltpu.VMEM((2 * CORES, steps, *block), BF16),
            pltpu.VMEM((2, chips, 3, *block), F32),
            pltpu.VMEM((2, 3, *block), F32),
            pltpu.VMEM((steps, 3, 3, *block), F32),
            pltpu.VMEM((2, *block), F32),
            pltpu.VMEM((2, places, *block), BF16),
            pltpu.VMEM((places, *block), BF16),
            pltpu.VMEM((2, places, *block), BF16),
            pltpu.VMEM((places, *block), BF16),
            pltpu.VMEM((2, *block), F32),
            pltpu.VMEM((2, *block), F32),
            pltpu.VMEM((2, 3, *block), F32),
            pltpu.VMEM((HALVES, steps, batch, half), BF16),
            pltpu.VMEM((HALVES, 2, batch, half), F32),
            pltpu.VMEM((3, col_block), F32),
            pltpu.VMEM((3, col_block), F32),
            dma((2, 3, places)),
            dma((3, chips, 2)),
            dma((2 * CORES,)),
            dma((chips, 2 * CORES)),
            dma((2,)),
            dma((steps, 3)),
            dma((HALVES,)),
            dma((2, 3, chips, 2)),
            dma((3, chips, 2)),
            dma((2,)),
            dma((chips, 2)),
            dma((2, chips)),
            dma((2, HALVES)),
            dma((kinds, places)),
            dma((kinds,)),
            dma((3,)),
            dma((3,)),
            dma((2,)),
        ]
        out_shape = (
            jax.ShapeDtypeStruct((steps, batch, half), BF16),
            jax.ShapeDtypeStruct((2, batch, half), F32),
        )
        results = pl.pallas_call(
            functools.partial(gru_kernel, rows, cols),
            name="gru",
            out_shape=out_shape,
            in_specs=[anywhere] * 10,
            out_specs=(vmem, vmem),
            scratch_shapes=scratch,
            compiler_params=pltpu.CompilerParams(
                collective_id=0, has_side_effects=True, vmem_limit_bytes=60 * 1024 * 1024
            ),
        )(
            x_rows, h_rows,
            jnp.transpose(wx_l1, (1, 0, 2)), whru_l1, whn_l1, bias_l1,
            jnp.transpose(wx_l2, (1, 0, 2)), whru_l2, whn_l2, bias_l2,
        )
        return pl.pallas_call(pass_on, name="results", out_shape=out_shape, in_specs=[vmem] * 2, out_specs=(vmem, vmem))(*results)

    seq_spec = P(None, "data", "row")
    out_spec = P(None, "data", ("col", "row"))
    wide_spec = P("row", None, "col")
    square_spec = P("row", "col")
    bias_spec = P(None, "col")
    return jax.shard_map(
        device_body,
        mesh=mesh,
        in_specs=(seq_spec, seq_spec, wide_spec, wide_spec, square_spec, bias_spec, wide_spec, wide_spec, square_spec, bias_spec),
        out_specs=(out_spec, out_spec),
        check_vma=False,
    )
```
